8 devices in a mesh: dp: 2 (over z, y), cp: 4 (over x, core).
Axes of the slice: x: 2, y: 2, z: 1, core: 2. Of those that a mesh axis runs over, the one named last changes fastest.
Arguments:
- x_in: bfloat16 [512, 5120], P(('dp', 'cp')), parts along dimension 0
- cache_k1: bfloat16 [2048, 40, 128], P(('dp', 'cp')), parts along dimension 0
- cache_v1: bfloat16 [2048, 40, 128], P(('dp', 'cp')), parts along dimension 0
- w_q1: bfloat16 [5120, 5120], replicated
- b_q1: bfloat16 [5120], replicated
- w_k1: bfloat16 [5120, 5120], replicated
- b_k1: bfloat16 [5120], replicated
- w_v1: bfloat16 [5120, 5120], replicated
- w_o1: bfloat16 [5120, 5120], replicated
- w_gate: bfloat16 [5120, 13824], replicated
- w_up: bfloat16 [5120, 13824], replicated
- w_down: bfloat16 [13824, 5120], replicated
- cache_k2: bfloat16 [2048, 40, 128], P(('dp', 'cp')), parts along dimension 0
- cache_v2: bfloat16 [2048, 40, 128], P(('dp', 'cp')), parts along dimension 0
- w_q2: bfloat16 [5120, 5120], replicated
- b_q2: bfloat16 [5120], replicated
- w_k2: bfloat16 [5120, 5120], replicated
- b_k2: bfloat16 [5120], replicated
- w_v2: bfloat16 [5120, 5120], replicated
- w_o2: bfloat16 [5120, 5120], replicated
Outputs:
- output 1: bfloat16 [512, 5120], P(('dp', 'cp')), parts along dimension 0
- output 2: bfloat16 [512, 5120], P(('dp', 'cp')), parts along dimension 0
- output 3: bfloat16 [512, 40, 128], P(('dp', 'cp')), parts along dimension 0
- output 4: bfloat16 [512, 40, 128], P(('dp', 'cp')), parts along dimension 0
- output 5: bfloat16 [512, 40, 128], P(('dp', 'cp')), parts along dimension 0
- output 6: bfloat16 [512, 40, 128], P(('dp', 'cp')), parts along dimension 0
There are 2 independent parts. The reference program is written for one: setup_inputs(seed, part) draws one part's arguments, and reference() takes and returns one part's arrays. A program takes and returns all parts, laid end to end along the dimension named above; an argument that names none is the same for every part.
All inputs are finite; a program needn't handle non-finite values.
Results may differ from the reference program's by a relative error of at most 0.0145851.
Values are sent between devices in bfloat16 or wider.
A program may use at most 3.25 GiB of HBM per device.

```python
import math
import jax
import jax.numpy as jnp
from jax import lax

D_MODEL = 5120
HEADS = 40
KV_HEADS = 40
HEAD = 128
FF = 13824
CHUNK = 256
CACHE = 1024
SHARDS = 4
QBLK = 64

GROUP = HEADS // KV_HEADS
SHARD_LEN = CACHE // SHARDS


def draw_matrix(key, rows, cols):
    return (jax.random.normal(key, (rows, cols), jnp.float32) * rows ** -0.5).astype(jnp.bfloat16)


def draw_cache(key_k, key_s, key_v, key_m):
    shard_scale = jax.random.uniform(key_s, (SHARDS, 1, 1, 1), jnp.float32, 0.6, 1.6)
    cache_keys = jax.random.normal(key_k, (SHARDS, SHARD_LEN, KV_HEADS, HEAD), jnp.float32) * shard_scale
    shard_mean = jax.random.normal(key_m, (SHARDS, 1, KV_HEADS, HEAD), jnp.float32)
    cache_vals = 0.5 * jax.random.normal(key_v, (SHARDS, SHARD_LEN, KV_HEADS, HEAD), jnp.float32) + shard_mean
    return (cache_keys.reshape(CACHE, KV_HEADS, HEAD).astype(jnp.bfloat16),
            cache_vals.reshape(CACHE, KV_HEADS, HEAD).astype(jnp.bfloat16))


def draw_bias(key_dir, key_q, key_k):
    half_dim = HEAD // 2
    lane_idx = jnp.arange(HEAD) % half_dim
    low_mask = (lane_idx >= (7 * half_dim) // 8).astype(jnp.float32)
    raw_dir = jax.random.normal(key_dir, (KV_HEADS, HEAD), jnp.float32) * low_mask
    unit_dir = raw_dir / jnp.sqrt(jnp.sum(raw_dir * raw_dir, axis=-1, keepdims=True))
    mean_score = max(math.log(CACHE / CHUNK) + 0.5, 0.5)
    bias_amp = math.sqrt(mean_score * math.sqrt(HEAD))
    jitter_q = jax.random.uniform(key_q, (HEADS, 1), jnp.float32, 0.9, 1.1)
    jitter_k = jax.random.uniform(key_k, (KV_HEADS, 1), jnp.float32, 0.9, 1.1)
    bias_q = bias_amp * jnp.repeat(unit_dir, GROUP, axis=0) * jitter_q
    bias_k = bias_amp * unit_dir * jitter_k
    return (bias_q.reshape(HEADS * HEAD).astype(jnp.bfloat16),
            bias_k.reshape(KV_HEADS * HEAD).astype(jnp.bfloat16))


def setup_inputs(seed: int = 0, part: int = 0) -> dict:
    shared_root, part_root = jax.random.split(jax.random.key(seed))
    part_keys = jax.random.split(jax.random.fold_in(part_root, part), 9)
    weight_keys = jax.random.split(shared_root, 17)
    x_in = jax.random.normal(part_keys[0], (CHUNK, D_MODEL), jnp.float32).astype(jnp.bfloat16)
    cache_k1, cache_v1 = draw_cache(part_keys[1], part_keys[2], part_keys[3], part_keys[4])
    cache_k2, cache_v2 = draw_cache(part_keys[5], part_keys[6], part_keys[7], part_keys[8])
    b_q1, b_k1 = draw_bias(weight_keys[0], weight_keys[1], weight_keys[2])
    b_q2, b_k2 = draw_bias(weight_keys[3], weight_keys[4], weight_keys[5])
    return {
        'x_in': x_in,
        'cache_k1': cache_k1,
        'cache_v1': cache_v1,
        'w_q1': draw_matrix(weight_keys[6], D_MODEL, HEADS * HEAD),
        'b_q1': b_q1,
        'w_k1': draw_matrix(weight_keys[7], D_MODEL, KV_HEADS * HEAD),
        'b_k1': b_k1,
        'w_v1': draw_matrix(weight_keys[8], D_MODEL, KV_HEADS * HEAD),
        'w_o1': draw_matrix(weight_keys[9], HEADS * HEAD, D_MODEL),
        'w_gate': draw_matrix(weight_keys[10], D_MODEL, FF),
        'w_up': draw_matrix(weight_keys[11], D_MODEL, FF),
        'w_down': draw_matrix(weight_keys[12], FF, D_MODEL),
        'cache_k2': cache_k2,
        'cache_v2': cache_v2,
        'w_q2': draw_matrix(weight_keys[13], D_MODEL, HEADS * HEAD),
        'b_q2': b_q2,
        'w_k2': draw_matrix(weight_keys[14], D_MODEL, KV_HEADS * HEAD),
        'b_k2': b_k2,
        'w_v2': draw_matrix(weight_keys[15], D_MODEL, KV_HEADS * HEAD),
        'w_o2': draw_matrix(weight_keys[16], HEADS * HEAD, D_MODEL),
    }


def rms_norm(vals):
    wide = vals.astype(jnp.float32)
    return (wide * lax.rsqrt(jnp.mean(wide * wide, axis=-1, keepdims=True) + 1e-5)).astype(jnp.bfloat16)


def rope_tables(positions):
    half_dim = HEAD // 2
    inv_freq = 1.0 / (500000.0 ** (jnp.arange(half_dim, dtype=jnp.float32) * (2.0 / HEAD)))
    angles = positions.astype(jnp.float32)[:, None] * inv_freq[None, :]
    return jnp.cos(angles)[:, None, :], jnp.sin(angles)[:, None, :]


def apply_rope(vals, cos_t, sin_t):
    half_dim = HEAD // 2
    first = vals[..., :half_dim]
    second = vals[..., half_dim:]
    return jnp.concatenate([first * cos_t - second * sin_t, second * cos_t + first * sin_t], axis=-1)


def attention_layer(layer_in, cache_k, cache_v, w_q, b_q, w_k, b_k, w_v, w_o):
    cos_t, sin_t = rope_tables(CACHE + jnp.arange(CHUNK))
    q_pre = (jnp.dot(layer_in, w_q, preferred_element_type=jnp.float32) + b_q.astype(jnp.float32)).astype(jnp.bfloat16)
    k_pre = (jnp.dot(layer_in, w_k, preferred_element_type=jnp.float32) + b_k.astype(jnp.float32)).astype(jnp.bfloat16)
    v_new = jnp.dot(layer_in, w_v, preferred_element_type=jnp.float32).astype(jnp.bfloat16).reshape(CHUNK, KV_HEADS, HEAD)
    q_rot = apply_rope(q_pre.reshape(CHUNK, HEADS, HEAD).astype(jnp.float32), cos_t, sin_t).astype(jnp.bfloat16)
    k_new = apply_rope(k_pre.reshape(CHUNK, KV_HEADS, HEAD).astype(jnp.float32), cos_t, sin_t).astype(jnp.bfloat16)
    keys_all = jnp.concatenate([cache_k, k_new], axis=0).astype(jnp.float32)
    vals_all = jnp.concatenate([cache_v, v_new], axis=0).astype(jnp.float32)
    key_pos = jnp.arange(CACHE + CHUNK)
    scale = HEAD ** -0.5
    q_blocks = q_rot.reshape(CHUNK // QBLK, QBLK, KV_HEADS, GROUP, HEAD)
    starts = jnp.arange(CHUNK // QBLK) * QBLK

    def one_block(blk_in):
        q_blk, start = blk_in
        scores = jnp.einsum('tkgd,skd->tkgs', q_blk.astype(jnp.float32), keys_all) * scale
        q_pos = CACHE + start + jnp.arange(QBLK)
        visible = key_pos[None, :] <= q_pos[:, None]
        scores = jnp.where(visible[:, None, None, :], scores, -jnp.inf)
        peak = jnp.max(scores, axis=-1, keepdims=True)
        prob_w = jnp.exp(scores - peak)
        total = jnp.sum(prob_w, axis=-1, keepdims=True)
        summed = jnp.einsum('tkgs,skd->tkgd', prob_w.astype(jnp.bfloat16).astype(jnp.float32), vals_all)
        return summed / total

    o_all = lax.map(one_block, (q_blocks, starts))
    o_half = o_all.reshape(CHUNK, HEADS * HEAD).astype(jnp.bfloat16)
    y_out = jnp.dot(o_half, w_o, preferred_element_type=jnp.float32).astype(jnp.bfloat16)
    return y_out, k_new, v_new


def reference(x_in, cache_k1, cache_v1, w_q1, b_q1, w_k1, b_k1, w_v1, w_o1, w_gate, w_up, w_down, cache_k2, cache_v2, w_q2, b_q2, w_k2, b_k2, w_v2, w_o2):
    y_one, k_one, v_one = attention_layer(x_in, cache_k1, cache_v1, w_q1, b_q1, w_k1, b_k1, w_v1, w_o1)
    resid_h = (x_in.astype(jnp.float32) + y_one.astype(jnp.float32)).astype(jnp.bfloat16)
    normed = rms_norm(resid_h)
    gate_act = jnp.dot(normed, w_gate, preferred_element_type=jnp.float32).astype(jnp.bfloat16)
    up_proj = jnp.dot(normed, w_up, preferred_element_type=jnp.float32).astype(jnp.bfloat16)
    mixed = (jax.nn.silu(gate_act.astype(jnp.float32)) * up_proj.astype(jnp.float32)).astype(jnp.bfloat16)
    hidden = (resid_h.astype(jnp.float32) + jnp.dot(mixed, w_down, preferred_element_type=jnp.float32)).astype(jnp.bfloat16)
    y_two, k_two, v_two = attention_layer(rms_norm(hidden), cache_k2, cache_v2, w_q2, b_q2, w_k2, b_k2, w_v2, w_o2)
    return (hidden, y_two, k_one, v_one, k_two, v_two)
```

```python
import functools

import jax
import jax.numpy as jnp
from jax import lax
from jax.experimental import pallas as pl
from jax.experimental.pallas import tpu as pltpu
from jax.sharding import PartitionSpec as P

ROPE_THETA = 500000.0
NORM_EPS = 1e-5
MESH = pl.DeviceIdType.MESH
F32 = jnp.float32
BF16 = jnp.bfloat16

TILE = 512
HEAD = 128
PER_BLOCK = TILE // HEAD
SLOTS = 7


def rope_tables(positions, head_dim):
    half_dim = head_dim // 2
    inv_freq = 1.0 / (ROPE_THETA ** (jnp.arange(half_dim, dtype=F32) * (2.0 / head_dim)))
    angles = positions.astype(F32)[:, None] * inv_freq[None, :]
    cos_t, sin_t = jnp.cos(angles), jnp.sin(angles)
    return jnp.concatenate([cos_t, cos_t], axis=1), jnp.concatenate([-sin_t, sin_t], axis=1)


def body(dims, cos_ref, sin_ref, bias_ref, x_hbm, ck1, cv1, ck2, cv2, wq1, wk1, wv1, wo1, w_gate, w_up, w_down,
         wq2, wk2, wv2, wo2, g_out, y_out, k1_out, v1_out, k2_out, v2_out,
         wring, xin, hbuf, nbuf, gbuf, ebuf, qcat, knew, vnew, kc, vc, o_loc, o_send, o_recv, obuf, ybuf,
         st_loc, st_send, st_recv,
         wsem, xsem, csem, qsend, qrecv, osend, orecv, ssend, srecv, dsend, drecv, asem, gsem):
    d_model, ff, rows, cache_rows = dims
    half = d_model // 2
    ffh = ff // 2
    ffc = ff // 3
    blocks = half // TILE
    ffn = ffh // (TILE // 2)
    crows = 2 * rows
    me = lax.axis_index("cp")
    core = lax.rem(me, 2)
    chip = me // 2
    partner = me + 1 - 2 * core
    peer = lax.rem(me + 2, 4)
    my_cols = pl.multiple_of(core * half, 128)
    my_rows = pl.multiple_of(core * rows, 16)
    other_rows = pl.multiple_of((1 - core) * rows, 16)
    other_cols = pl.multiple_of((1 - core) * half, 128)

    def col(b):
        return pl.multiple_of(core * half + b * TILE, 128)

    attn_tiles = 4 * blocks
    base1 = 0
    base_up = attn_tiles
    base_down = base_up + ffn
    base2 = base_down + 3 * blocks
    total = base2 + attn_tiles

    def start_full(w, b, slot):
        pltpu.make_async_copy(w.at[:, pl.ds(col(b), TILE)], wring.at[slot], wsem.at[slot]).start()

    def start_mlp(n, slot):
        at = pl.ds(pl.multiple_of(core * ffh + n * (TILE // 2), 128), TILE // 2)
        pltpu.make_async_copy(w_gate.at[:, at], wring.at[slot, :, pl.ds(0, TILE // 2)], wsem.at[slot]).start()
        pltpu.make_async_copy(w_up.at[:, at], wring.at[slot, :, pl.ds(TILE // 2, TILE // 2)], wsem.at[slot]).start()

    def start_down(i, slot):
        pltpu.make_async_copy(
            w_down.at[pl.ds(pl.multiple_of(lax.rem(i, 3) * ffc, 16), ffc), pl.ds(col(i // 3), TILE)],
            wring.at[slot, pl.ds(0, ffc), :], wsem.at[slot]).start()

    loop_end = 3 * (blocks - 1) + 1

    def attn_segments(base, wq, wk, wv, wo):
        return [
            (base, base + 1, lambda r, slot: start_full(wq, 0, slot), None),
            (base + 1, base + loop_end, lambda r, slot: start_full(wq, r // 3 + 1, slot), 0),
            (base + 1, base + loop_end, lambda r, slot: start_full(wk, r // 3, slot), 1),
            (base + 1, base + loop_end, lambda r, slot: start_full(wv, r // 3, slot), 2),
            (base + loop_end, base + loop_end + 1, lambda r, slot: start_full(wk, blocks - 1, slot), None),
            (base + loop_end + 1, base + loop_end + 2, lambda r, slot: start_full(wv, blocks - 1, slot), None),
            (base + loop_end + 2, base + attn_tiles, lambda r, slot: start_full(wo, r, slot), None),
        ]

    segments = attn_segments(base1, wq1, wk1, wv1, wo1) + [
        (base_up, base_down, start_mlp, None),
        (base_down, base2, start_down, None),
    ] + attn_segments(base2, wq2, wk2, wv2, wo2)

    def start_tile(s, lo, hi):
        slot = lax.rem(s, SLOTS) if not isinstance(s, int) else s % SLOTS
        for a, b, fn, phase in segments:
            if b <= lo or a >= hi:
                continue
            if isinstance(s, int):
                if a <= s < b and (phase is None or (s - a) % 3 == phase):
                    fn(s - a, slot)
                continue
            cond = (s >= a) & (s < b)
            if phase is not None:
                cond = cond & (lax.rem(s - a + 3, 3) == phase)

            @pl.when(cond)
            def _(a=a, fn=fn):
                fn(s - a, slot)

    def wait_tile(s, depth=None):
        slot = lax.rem(s, SLOTS) if not isinstance(s, int) else s % SLOTS
        ref = wring.at[slot] if depth is None else wring.at[slot, pl.ds(0, depth), :]
        pltpu.make_async_copy(ref, ref, wsem.at[slot]).wait()
        return slot

    def remote(src, dst, send, recv, who):
        return pltpu.make_async_remote_copy(src_ref=src, dst_ref=dst, send_sem=send, recv_sem=recv,
                                            device_id={"cp": who}, device_id_type=MESH)

    for s in range(SLOTS):
        start_tile(s, s, s + 1)

    barrier = pltpu.get_barrier_semaphore()
    for who in (partner, peer):
        pl.semaphore_signal(barrier, inc=1, device_id={"cp": who}, device_id_type=MESH)
    pl.semaphore_wait(barrier, 2)

    x_loc = pltpu.make_async_copy(x_hbm, xin.at[pl.ds(my_rows, rows)], xsem.at[0])
    x_rem = remote(x_hbm, xin.at[pl.ds(my_rows, rows)], xsem.at[1], xsem.at[2], partner)
    x_rem.start()
    x_loc.start()

    def cache_copies(ck, cv):
        crow = pl.ds(pl.multiple_of(core * cache_rows, 16), cache_rows)
        out = []
        for i, (src, dst) in enumerate(((ck, kc), (cv, vc))):
            out.append(pltpu.make_async_copy(src.at[:, pl.ds(my_cols, half)], dst.at[crow], csem.at[3 * i]))
            out.append(remote(src.at[:, pl.ds(other_cols, half)], dst.at[crow], csem.at[3 * i + 1], csem.at[3 * i + 2],
                              partner))
        return out

    cache1 = cache_copies(ck1, cv1)
    for c in cache1:
        c.start()
    x_loc.wait()
    x_rem.wait()

    def rope(vals):
        parts = []
        for i in range(PER_BLOCK):
            seg = vals[:, i * HEAD:(i + 1) * HEAD]
            parts.append(seg * cos_ref[...] + pltpu.roll(seg, HEAD // 2, 1) * sin_ref[...])
        return jnp.concatenate(parts, axis=1)

    def norm(src):
        step = 16

        @pl.loop(0, crows // step)
        def _(i):
            at = pl.ds(pl.multiple_of(i * step, step), step)
            wide = src[at, :].astype(F32)
            nbuf[at, :] = (wide * lax.rsqrt(jnp.mean(wide * wide, axis=-1, keepdims=True) + NORM_EPS)).astype(BF16)

    row_i = lax.broadcasted_iota(jnp.int32, (2 * crows, crows), 0)
    col_i = lax.broadcasted_iota(jnp.int32, (2 * crows, crows), 1)
    far_lim = jnp.where(chip == 0, crows, -1)
    scale = HEAD ** -0.5

    def attend(b):
        lane = lax.broadcasted_iota(jnp.int32, (2 * crows, HEAD), 1)
        visible = col_i <= jnp.where(row_i < crows, row_i, far_lim)
        stats = jnp.zeros((2 * crows, HEAD), F32)
        dims_t = (((1,), (1,)), ((), ()))
        for i in range(PER_BLOCK):
            at = pl.ds(i * HEAD, HEAD)
            cat = pl.ds(pl.multiple_of(b * TILE + i * HEAD, 128), HEAD)
            q = qcat[b, :, at]
            s_old = lax.dot_general(q, kc[:, cat], dims_t, preferred_element_type=F32) * scale
            s_new = lax.dot_general(q, knew[b, :, at], dims_t, preferred_element_type=F32) * scale
            s_new = jnp.where(visible, s_new, -jnp.inf)
            peak = jnp.maximum(jnp.max(s_old, axis=1, keepdims=True), jnp.max(s_new, axis=1, keepdims=True))
            p_old = jnp.exp(s_old - peak)
            p_new = jnp.exp(s_new - peak)
            total_p = jnp.sum(p_old, axis=1, keepdims=True) + jnp.sum(p_new, axis=1, keepdims=True)
            acc = jnp.dot(p_old.astype(BF16), vc[:, cat], preferred_element_type=F32)
            acc = acc + jnp.dot(p_new.astype(BF16), vnew[b, :, at], preferred_element_type=F32)
            o_loc[b, :, at] = acc[:crows]
            o_send[b, :, at] = acc[crows:]
            stats = jnp.where(lane == 2 * i, peak, stats)
            stats = jnp.where(lane == 2 * i + 1, total_p, stats)
        st_loc[b] = stats[:crows]
        st_send[b] = stats[crows:].T[:8, :]

    def q_copy(b):
        return remote(qcat.at[b, pl.ds(0, crows), :], qcat.at[b, pl.ds(crows, crows), :], qsend.at[b], qrecv.at[b], peer)

    def o_copy(b):
        return remote(o_send.at[b], o_recv.at[b], osend.at[b], orecv.at[b], peer)

    def s_copy(b):
        return remote(st_send.at[b], st_recv.at[b], ssend.at[b], srecv.at[b], peer)

    def attention(layer_in, base, bias_row, caches, k_out, v_out):
        def q_step(b, s, lo, hi):
            slot = wait_tile(s)
            pre = (jnp.dot(layer_in[...], wring[slot], preferred_element_type=F32)
                   + bias_ref[pl.ds(bias_row, 1), pl.ds(col(b), TILE)]).astype(BF16)
            start_tile(s + SLOTS, lo + SLOTS, hi + SLOTS)
            qcat[b, pl.ds(0, crows), :] = rope(pre.astype(F32)).astype(BF16)
            q_copy(b).start()

        q_step(0, base, base, base + 1)

        @pl.loop(0, blocks)
        def _(b):
            has_q = (2 * blocks - 3 - b) // (blocks - 1)
            s = base + 1 + 3 * b

            @pl.when(b < blocks - 1)
            def _():
                q_step(b + 1, s, base + 1, base + loop_end)

            s = s + has_q
            slot = wait_tile(s)
            pre = (jnp.dot(layer_in[...], wring[slot], preferred_element_type=F32)
                   + bias_ref[pl.ds(bias_row + 1, 1), pl.ds(col(b), TILE)]).astype(BF16)
            start_tile(s + SLOTS, base + 2 + SLOTS, base + loop_end + 2 + SLOTS)
            knew[b] = rope(pre.astype(F32)).astype(BF16)
            s = s + 1
            slot = wait_tile(s)
            vals = jnp.dot(layer_in[...], wring[slot], preferred_element_type=F32).astype(BF16)
            start_tile(s + SLOTS, base + 3 + SLOTS, base + loop_end + 2 + SLOTS)
            vnew[b] = vals

            @pl.when(b == 0)
            def _():
                for c in caches:
                    c.wait()

            q_copy(b).wait_recv()
            attend(b)
            for src, dst, k in ((knew, k_out, 0), (vnew, v_out, 3)):
                pltpu.make_async_copy(src.at[b, pl.ds(my_rows, rows), :], dst.at[:, pl.ds(col(b), TILE)], asem.at[k]).start()
                remote(src.at[b, pl.ds(other_rows, rows), :], dst.at[:, pl.ds(col(b), TILE)], asem.at[k + 1],
                       asem.at[k + 2], partner).start()
            o_copy(b).start()
            s_copy(b).start()

        @pl.loop(0, blocks)
        def _(b):
            o_copy(b).wait_recv()
            s_copy(b).wait_recv()
            far = jnp.concatenate([st_recv[b], jnp.zeros((HEAD - 8, HEAD), F32)], axis=0).T
            near = st_loc[b]
            for i in range(PER_BLOCK):
                at = pl.ds(i * HEAD, HEAD)
                m_a, l_a = near[:, 2 * i:2 * i + 1], near[:, 2 * i + 1:2 * i + 2]
                m_b, l_b = far[:, 2 * i:2 * i + 1], far[:, 2 * i + 1:2 * i + 2]
                peak = jnp.maximum(m_a, m_b)
                w_a, w_b = jnp.exp(m_a - peak), jnp.exp(m_b - peak)
                norm_l = 1.0 / (l_a * w_a + l_b * w_b)
                o = o_loc[b, :, at] * (w_a * norm_l) + o_recv[b, :, at] * (w_b * norm_l)
                obuf[:, pl.ds(pl.multiple_of(core * half + b * TILE + i * HEAD, 128), HEAD)] = o.astype(BF16)
            piece = obuf.at[:, pl.ds(col(b), TILE)]
            remote(piece, piece, dsend.at[0], drecv.at[0], partner).start()

        mine = obuf.at[:, pl.ds(my_cols, half)]
        theirs = obuf.at[:, pl.ds(other_cols, half)]
        remote(mine, theirs, dsend.at[0], drecv.at[0], partner).wait_send()
        remote(mine, theirs, dsend.at[0], drecv.at[0], partner).wait_recv()

        @pl.loop(0, blocks)
        def _(b):
            q_copy(b).wait_send()
            o_copy(b).wait_send()
            s_copy(b).wait_send()

        for dst, k in ((k_out, 0), (v_out, 3)):
            to_me = dst.at[:, pl.ds(my_cols, half)]
            to_me2 = dst.at[:, pl.ds(other_cols, half)]
            pltpu.make_async_copy(to_me, to_me, asem.at[k]).wait()
            remote(to_me, to_me2, asem.at[k + 1], asem.at[k + 2], partner).wait_send()
            remote(to_me, to_me2, asem.at[k + 1], asem.at[k + 2], partner).wait_recv()

    def both_wait(buf, sem, width, my_at, other_at):
        mine = buf.at[:, pl.ds(my_at, width)]
        theirs = buf.at[:, pl.ds(other_at, width)]
        remote(mine, theirs, dsend.at[sem], drecv.at[sem], partner).wait_send()
        remote(mine, theirs, dsend.at[sem], drecv.at[sem], partner).wait_recv()

    attention(xin, base1, 0, cache1, k1_out, v1_out)
    cache2 = cache_copies(ck2, cv2)
    for c in cache2:
        c.start()

    @pl.loop(0, blocks)
    def _(b):
        s = base1 + 3 * blocks + b
        slot = wait_tile(s)
        y = jnp.dot(obuf[...], wring[slot], preferred_element_type=F32).astype(BF16)
        start_tile(s + SLOTS, base1 + 3 * blocks + SLOTS, base_up + SLOTS)
        at = pl.ds(col(b), TILE)
        hbuf[:, at] = (xin[:, at].astype(F32) + y.astype(F32)).astype(BF16)
        remote(hbuf.at[:, at], hbuf.at[:, at], dsend.at[1], drecv.at[1], partner).start()

    both_wait(hbuf, 1, half, my_cols, other_cols)
    norm(hbuf)

    @pl.loop(0, ffn)
    def _(n):
        s = base_up + n
        slot = wait_tile(s)
        both = jnp.dot(nbuf[...], wring[slot], preferred_element_type=F32)
        start_tile(s + SLOTS, base_up + SLOTS, base_down + SLOTS)
        gate = both[:, :TILE // 2].astype(BF16).astype(F32)
        up = both[:, TILE // 2:].astype(BF16).astype(F32)
        at = pl.ds(pl.multiple_of(core * ffh + n * (TILE // 2), 128), TILE // 2)
        ebuf[:, at] = (jax.nn.silu(gate) * up).astype(BF16)
        remote(ebuf.at[:, at], ebuf.at[:, at], dsend.at[2], drecv.at[2], partner).start()

    both_wait(ebuf, 2, ffh, pl.multiple_of(core * ffh, 128), pl.multiple_of((1 - core) * ffh, 128))

    @pl.loop(0, blocks)
    def _(b):
        at = pl.ds(col(b), TILE)
        acc = hbuf[:, at].astype(F32)
        for k in range(3):
            s = base_down + 3 * b + k
            slot = wait_tile(s, ffc)
            part = jnp.dot(ebuf[:, k * ffc:(k + 1) * ffc], wring[slot, :ffc, :], preferred_element_type=F32)
            start_tile(s + SLOTS, base_down + k + SLOTS, base2 - 2 + k + SLOTS)
            down = part if k == 0 else down + part
        gbuf[:, at] = (acc + down).astype(BF16)
        remote(gbuf.at[:, at], gbuf.at[:, at], dsend.at[3], drecv.at[3], partner).start()

    both_wait(gbuf, 3, half, my_cols, other_cols)
    g_copy = pltpu.make_async_copy(gbuf.at[pl.ds(my_rows, rows), :], g_out, gsem.at[0])
    g_copy.start()
    norm(gbuf)

    attention(nbuf, base2, 2, cache2, k2_out, v2_out)

    @pl.loop(0, blocks)
    def _(b):
        s = base2 + 3 * blocks + b
        slot = wait_tile(s)
        ybuf[b] = jnp.dot(obuf[...], wring[slot], preferred_element_type=F32).astype(BF16)
        at = pl.ds(col(b), TILE)
        pltpu.make_async_copy(ybuf.at[b, pl.ds(my_rows, rows), :], y_out.at[:, at], gsem.at[1]).start()
        remote(ybuf.at[b, pl.ds(other_rows, rows), :], y_out.at[:, at], dsend.at[4], drecv.at[4], partner).start()

    y_mine = y_out.at[:, pl.ds(my_cols, half)]
    y_theirs = y_out.at[:, pl.ds(other_cols, half)]
    pltpu.make_async_copy(y_mine, y_mine, gsem.at[1]).wait()
    remote(y_mine, y_theirs, dsend.at[4], drecv.at[4], partner).wait_send()
    remote(y_mine, y_theirs, dsend.at[4], drecv.at[4], partner).wait_recv()
    g_copy.wait()


def solution(mesh):
    rows_spec = P(('dp', 'cp'), None)
    cache_spec = P(('dp', 'cp'), None, None)
    mat_spec = P(None, None)
    vec_spec = P(None)
    layer_specs = (cache_spec, cache_spec, mat_spec, vec_spec, mat_spec, vec_spec, mat_spec, mat_spec)
    in_specs = (rows_spec,) + layer_specs + (mat_spec, mat_spec, mat_spec) + layer_specs
    out_specs = (rows_spec, rows_spec, cache_spec, cache_spec, cache_spec, cache_spec)

    def forward(x_in, cache_k1, cache_v1, w_q1, b_q1, w_k1, b_k1, w_v1, w_o1, w_gate, w_up, w_down, cache_k2, cache_v2, w_q2, b_q2, w_k2, b_k2, w_v2, w_o2):
        rows, d_model = x_in.shape
        cache_rows, heads, head_dim = cache_k1.shape
        ff = w_gate.shape[1]
        half = d_model // 2
        blocks = half // TILE
        crows = 2 * rows
        first = 4 * cache_rows + (lax.axis_index('cp') // 2) * crows
        cos_t, sin_t = rope_tables(first + jnp.arange(crows), head_dim)
        bias = jnp.stack([b_q1, b_k1, b_q2, b_k2]).astype(F32)

        def flat(c):
            return c.reshape(cache_rows, d_model)

        any_spec = pl.BlockSpec(memory_space=pl.ANY)
        vmem_spec = pl.BlockSpec(memory_space=pltpu.VMEM)
        row_out = jax.ShapeDtypeStruct((rows, d_model), BF16)
        dma = pltpu.SemaphoreType.DMA
        out = pl.pallas_call(
            functools.partial(body, (d_model, ff, rows, cache_rows)),
            out_shape=[row_out] * 6,
            in_specs=[vmem_spec] * 3 + [any_spec] * 16,
            out_specs=[any_spec] * 6,
            scratch_shapes=[
                pltpu.VMEM((SLOTS, d_model, TILE), BF16),
                pltpu.VMEM((crows, d_model), BF16),
                pltpu.VMEM((crows, d_model), BF16),
                pltpu.VMEM((crows, d_model), BF16),
                pltpu.VMEM((crows, d_model), BF16),
                pltpu.VMEM((crows, ff), BF16),
                pltpu.VMEM((blocks, 2 * crows, TILE), BF16),
                pltpu.VMEM((blocks, crows, TILE), BF16),
                pltpu.VMEM((blocks, crows, TILE), BF16),
                pltpu.VMEM((2 * cache_rows, half), BF16),
                pltpu.VMEM((2 * cache_rows, half), BF16),
                pltpu.VMEM((blocks, crows, TILE), F32),
                pltpu.VMEM((blocks, crows, TILE), F32),
                pltpu.VMEM((blocks, crows, TILE), F32),
                pltpu.VMEM((crows, d_model), BF16),
                pltpu.VMEM((blocks, crows, TILE), BF16),
                pltpu.VMEM((blocks, crows, HEAD), F32),
                pltpu.VMEM((blocks, 8, HEAD), F32),
                pltpu.VMEM((blocks, 8, HEAD), F32),
                dma((SLOTS,)), dma((3,)), dma((6,)),
                dma((blocks,)), dma((blocks,)), dma((blocks,)), dma((blocks,)), dma((blocks,)), dma((blocks,)),
                dma((5,)), dma((5,)), dma((6,)), dma((2,)),
            ],
            compiler_params=pltpu.CompilerParams(
                collective_id=0, has_side_effects=True, vmem_limit_bytes=67043328),
        )(cos_t, sin_t, bias, x_in, flat(cache_k1), flat(cache_v1), flat(cache_k2), flat(cache_v2),
          w_q1, w_k1, w_v1, w_o1, w_gate, w_up, w_down, w_q2, w_k2, w_v2, w_o2)
        g, y2, k1, v1, k2, v2 = out

        def heads_of(a):
            return a.reshape(rows, heads, head_dim)

        return g, y2, heads_of(k1), heads_of(v1), heads_of(k2), heads_of(v2)

    return jax.shard_map(forward, mesh=mesh, in_specs=in_specs, out_specs=out_specs, check_vma=False)
```

```python
import functools

import jax
import jax.numpy as jnp
import numpy as np
from jax import lax
from jax.experimental import pallas as pl
from jax.experimental.pallas import tpu as pltpu
from jax.sharding import PartitionSpec as P

ROPE_THETA = 500000.0
NORM_EPS = 1e-5
MESH = pl.DeviceIdType.MESH
F32 = jnp.float32
BF16 = jnp.bfloat16

TILE = 512
HEAD = 128
PER_BLOCK = TILE // HEAD
SLOTS = 7


def rope_tables(positions, head_dim):
    half_dim = head_dim // 2
    inv_freq = (1.0 / (ROPE_THETA ** (np.arange(half_dim, dtype=np.float32) * np.float32(2.0 / head_dim)))).astype(np.float32)
    angles = positions.astype(np.float32)[:, None] * inv_freq[None, :]
    cos_t, sin_t = np.cos(angles), np.sin(angles)
    return np.concatenate([cos_t, cos_t], axis=1), np.concatenate([-sin_t, sin_t], axis=1)


def body(dims, cos_ref, sin_ref, bq1, bk1, bq2, bk2, x_hbm, ck1, cv1, ck2, cv2, wq1, wk1, wv1, wo1, w_gate, w_up, w_down,
         wq2, wk2, wv2, wo2, g_out, y_out, k1_out, v1_out, k2_out, v2_out,
         wring, nbuf, gbuf, ebuf, pre, kc, vc, o_loc, o_send, o_recv, obuf, opair,
         st_loc, st_send, st_recv, bias32,
         wsem, xsem, csem, c2send, c2recv, qsend, qrecv, osend, orecv, ssend, srecv, dsend, drecv, asem, gsem,
         gxs, gxr, a2send, a2recv):
    d_model, ff, rows, cache_rows = dims
    half = d_model // 2
    ffh = ff // 2
    ffc = ff // 3
    blocks = half // TILE
    ffn = ffh // (TILE // 2)
    crows = 2 * rows
    quart = half // 2
    ybuf = nbuf.at[pl.ds(0, rows), :]
    me = lax.axis_index("cp")
    core = lax.rem(me, 2)
    chip = me // 2
    partner = me + 1 - 2 * core
    peer = lax.rem(me + 2, 4)
    diag = 3 - me
    chip_rows = pl.multiple_of(chip * crows, 16)
    xin = hbuf = gbuf.at[pl.ds(pl.multiple_of(chip * crows, 16), crows), :]
    far_rows = pl.multiple_of((1 - chip) * crows, 16)
    my_cols = pl.multiple_of(core * half, 128)
    my_rows = pl.multiple_of(core * rows, 16)
    other_rows = pl.multiple_of((1 - core) * rows, 16)
    other_cols = pl.multiple_of((1 - core) * half, 128)

    def col(b):
        return pl.multiple_of(core * half + b * TILE, 128)

    attn_tiles = 4 * blocks
    base1 = 0
    base_up = attn_tiles
    base_down = base_up + ffn
    base2 = base_down + 3 * blocks
    qkv2 = 8

    def start_full(w, b, slot):
        pltpu.make_async_copy(w.at[:, pl.ds(col(b), TILE)], wring.at[slot], wsem.at[slot]).start()

    def start_mlp(n, slot):
        at = pl.ds(pl.multiple_of(core * ffh + n * (TILE // 2), 128), TILE // 2)
        pltpu.make_async_copy(w_gate.at[:, at], wring.at[slot, :, pl.ds(0, TILE // 2)], wsem.at[slot]).start()
        pltpu.make_async_copy(w_up.at[:, at], wring.at[slot, :, pl.ds(TILE // 2, TILE // 2)], wsem.at[slot]).start()

    def start_down(i, slot):
        pltpu.make_async_copy(
            w_down.at[pl.ds(pl.multiple_of(lax.rem(i, 3) * ffc, 16), ffc), pl.ds(col(i // 3), TILE)],
            wring.at[slot, pl.ds(0, ffc), :], wsem.at[slot]).start()

    loop_end = 3 * (blocks - 1) + 1

    def attn_segments(base, wq, wk, wv, wo):
        return [
            (base, base + 1, lambda r, slot: start_full(wq, 0, slot), None),
            (base + 1, base + loop_end, lambda r, slot: start_full(wq, r // 3 + 1, slot), 0),
            (base + 1, base + loop_end, lambda r, slot: start_full(wk, r // 3, slot), 1),
            (base + 1, base + loop_end, lambda r, slot: start_full(wv, r // 3, slot), 2),
            (base + loop_end, base + loop_end + 1, lambda r, slot: start_full(wk, blocks - 1, slot), None),
            (base + loop_end + 1, base + loop_end + 2, lambda r, slot: start_full(wv, blocks - 1, slot), None),
            (base + loop_end + 2, base + attn_tiles, lambda r, slot: start_full(wo, r, slot), None),
        ]

    PAIR = TILE // 2
    own2 = core * half + chip * quart

    def start_v2(t, slot):
        @pl.when(t < qkv2 - 2)
        def _():
            pltpu.make_async_copy(wv2.at[:, pl.ds(pl.multiple_of(own2 + (t // 3) * TILE, 128), TILE)], wring.at[slot],
                                  wsem.at[slot]).start()

        @pl.when(t >= qkv2 - 2)
        def _():
            pltpu.make_async_copy(wv2.at[:, pl.ds(pl.multiple_of(own2 + (t // 3) * TILE, 128), PAIR)],
                                  wring.at[slot, :, pl.ds(0, PAIR)], wsem.at[slot]).start()

    def start_qk2(t, slot):
        at = pl.ds(pl.multiple_of(own2 + (t - 1 - t // 3) * PAIR, 128), PAIR)
        pltpu.make_async_copy(wq2.at[:, at], wring.at[slot, :, pl.ds(0, PAIR)], wsem.at[slot]).start()
        pltpu.make_async_copy(wk2.at[:, at], wring.at[slot, :, pl.ds(PAIR, PAIR)], wsem.at[slot]).start()

    def start_wo2(b, slot):
        for i in range(2):
            pltpu.make_async_copy(
                wo2.at[pl.ds(my_cols, half), pl.ds(pl.multiple_of(b * 2 * TILE + i * TILE, 128), TILE)],
                wring.at[slot, pl.ds(i * half, half), :], wsem.at[slot]).start()

    segments = attn_segments(base1, wq1, wk1, wv1, wo1) + [
        (base_up, base_down, start_mlp, None),
        (base_down, base2, start_down, None),
        (base2, base2 + qkv2, start_v2, 0),
        (base2, base2 + qkv2, start_qk2, 1),
        (base2, base2 + qkv2, start_qk2, 2),
        (base2 + qkv2, base2 + qkv2 + blocks, start_wo2, None),
    ]

    def start_tile(s, lo, hi):
        slot = lax.rem(s, SLOTS) if not isinstance(s, int) else s % SLOTS
        for a, b, fn, phase in segments:
            if b <= lo or a >= hi:
                continue
            if isinstance(s, int):
                if a <= s < b and (phase is None or (s - a) % 3 == phase):
                    fn(s - a, slot)
                continue
            cond = (s >= a) & (s < b)
            if phase is not None:
                cond = cond & (lax.rem(s - a + 3, 3) == phase)

            @pl.when(cond)
            def _(a=a, fn=fn):
                fn(s - a, slot)

    def wait_tile(s, depth=None):
        slot = lax.rem(s, SLOTS) if not isinstance(s, int) else s % SLOTS
        ref = wring.at[slot] if depth is None else wring.at[slot, pl.ds(0, depth), :]
        pltpu.make_async_copy(ref, ref, wsem.at[slot]).wait()
        return slot

    def remote(src, dst, send, recv, who):
        return pltpu.make_async_remote_copy(src_ref=src, dst_ref=dst, send_sem=send, recv_sem=recv,
                                            device_id={"cp": who}, device_id_type=MESH)

    for s in range(SLOTS):
        start_tile(s, s, s + 1)

    barrier = pltpu.get_barrier_semaphore()
    for who in (partner, peer, diag):
        pl.semaphore_signal(barrier, inc=1, device_id={"cp": who}, device_id_type=MESH)
    pl.semaphore_wait(barrier, 3)

    x_loc = pltpu.make_async_copy(x_hbm, xin.at[pl.ds(my_rows, rows)], xsem.at[0])
    x_rem = remote(x_hbm, xin.at[pl.ds(my_rows, rows)], xsem.at[1], xsem.at[2], partner)
    x_rem.start()
    x_loc.start()

    def cache_copies(ck, cv):
        crow = pl.ds(pl.multiple_of(core * cache_rows, 16), cache_rows)
        out = []
        for i, (src, dst) in enumerate(((ck, kc), (cv, vc))):
            out.append(pltpu.make_async_copy(src.at[:, pl.ds(my_cols, half)], dst.at[crow], csem.at[3 * i]))
            out.append(remote(src.at[:, pl.ds(other_cols, half)], dst.at[crow], csem.at[3 * i + 1], csem.at[3 * i + 2],
                              partner))
        return out

    cache1 = cache_copies(ck1, cv1)
    for c in cache1:
        c.start()
    for i, ref in enumerate((bq1, bk1, bq2, bk2)):
        bias32[i] = ref[...].astype(F32)
    x_loc.wait()
    x_rem.wait()

    def biased_rope(vals, bias_row, first_head, table_at, n):
        parts = []
        cos_t, sin_t = cos_ref[table_at, :], sin_ref[table_at, :]
        for i in range(n):
            seg = vals[:, i * HEAD:(i + 1) * HEAD] + bias32[bias_row, pl.ds(first_head + i, 1), :]
            seg = seg.astype(BF16).astype(F32)
            parts.append((seg * cos_t + pltpu.roll(seg, HEAD // 2, 1) * sin_t).astype(BF16))
        return jnp.concatenate(parts, axis=1)

    def norm(src, dst, first, count):
        step = 16

        @pl.loop(0, count // step)
        def _(i):
            at = pl.ds(pl.multiple_of(first + i * step, step), step)
            wide = src[at, :].astype(F32)
            dst[at, :] = (wide * lax.rsqrt(jnp.mean(wide * wide, axis=-1, keepdims=True) + NORM_EPS)).astype(BF16)

    row_i = lax.broadcasted_iota(jnp.int32, (2 * crows, crows), 0)
    col_i = lax.broadcasted_iota(jnp.int32, (2 * crows, crows), 1)
    far_lim = jnp.where(chip == 0, crows, -1)
    scale = HEAD ** -0.5

    def attend(b):
        lane = lax.broadcasted_iota(jnp.int32, (2 * crows, HEAD), 1)
        visible = col_i <= jnp.where(row_i < crows, row_i, far_lim)
        stats = jnp.zeros((2 * crows, HEAD), F32)
        dims_t = (((1,), (1,)), ((), ()))
        for i in range(PER_BLOCK):
            at = pl.ds(i * HEAD, HEAD)
            cat = pl.ds(pl.multiple_of(b * TILE + i * HEAD, 128), HEAD)
            q = pre[b, :, at]
            s_old = lax.dot_general(q, kc[:, cat], dims_t, preferred_element_type=F32) * scale
            s_new = lax.dot_general(q, pre[blocks + b, pl.ds(0, crows), at], dims_t, preferred_element_type=F32) * scale
            s_new = jnp.where(visible, s_new, -jnp.inf)
            peak = jnp.maximum(jnp.max(s_old, axis=1, keepdims=True), jnp.max(s_new, axis=1, keepdims=True))
            p_old = jnp.exp(s_old - peak)
            p_new = jnp.exp(s_new - peak)
            total_p = jnp.sum(p_old, axis=1, keepdims=True) + jnp.sum(p_new, axis=1, keepdims=True)
            acc = jnp.dot(p_old.astype(BF16), vc[:, cat], preferred_element_type=F32)
            acc = acc + jnp.dot(p_new.astype(BF16), pre[blocks + b, pl.ds(crows, crows), at], preferred_element_type=F32)
            o_loc[b, :, at] = acc[:crows]
            o_send[b, :, at] = acc[crows:]
            stats = jnp.where(lane == 2 * i, peak, stats)
            stats = jnp.where(lane == 2 * i + 1, total_p, stats)
        st_loc[b] = stats[:crows]
        st_send[b] = stats[crows:].T[:8, :]

    def q_copy(b):
        return remote(pre.at[b, pl.ds(0, crows), :], pre.at[b, pl.ds(crows, crows), :], qsend.at[b], qrecv.at[b], peer)

    def o_copy(b):
        return remote(o_send.at[b], o_recv.at[b], osend.at[b], orecv.at[b], peer)

    def s_copy(b):
        return remote(st_send.at[b], st_recv.at[b], ssend.at[b], srecv.at[b], peer)

    def head_of(b):
        return core * (half // HEAD) + b * PER_BLOCK

    def attention(layer_in, base, bias_row, caches, k_out, v_out):
        def q_step(b, s, lo, hi):
            slot = wait_tile(s)
            raw = jnp.dot(layer_in[...], wring[slot], preferred_element_type=F32)
            start_tile(s + SLOTS, lo + SLOTS, hi + SLOTS)
            pre[b, pl.ds(0, crows), :] = biased_rope(raw, bias_row, head_of(b), pl.ds(chip_rows, crows), PER_BLOCK)
            q_copy(b).start()

        q_step(0, base, base, base + 1)

        @pl.loop(0, blocks)
        def _(b):
            has_q = (2 * blocks - 3 - b) // (blocks - 1)
            s = base + 1 + 3 * b

            @pl.when(b < blocks - 1)
            def _():
                q_step(b + 1, s, base + 1, base + loop_end)

            s = s + has_q
            slot = wait_tile(s)
            raw = jnp.dot(layer_in[...], wring[slot], preferred_element_type=F32)
            start_tile(s + SLOTS, base + 2 + SLOTS, base + loop_end + 2 + SLOTS)
            pre[blocks + b, pl.ds(0, crows), :] = biased_rope(raw, bias_row + 1, head_of(b), pl.ds(chip_rows, crows), PER_BLOCK)
            s = s + 1
            slot = wait_tile(s)
            vals = jnp.dot(layer_in[...], wring[slot], preferred_element_type=F32).astype(BF16)
            start_tile(s + SLOTS, base + 3 + SLOTS, base + loop_end + 2 + SLOTS)
            pre[blocks + b, pl.ds(crows, crows), :] = vals

            @pl.when(b == 0)
            def _():
                for c in caches:
                    c.wait()

            q_copy(b).wait_recv()
            attend(b)
            for part, dst, k in ((0, k_out, 0), (crows, v_out, 3)):
                pltpu.make_async_copy(pre.at[blocks + b, pl.ds(part + my_rows, rows), :], dst.at[:, pl.ds(col(b), TILE)], asem.at[k]).start()
                remote(pre.at[blocks + b, pl.ds(part + other_rows, rows), :], dst.at[:, pl.ds(col(b), TILE)], asem.at[k + 1],
                       asem.at[k + 2], partner).start()
            o_copy(b).start()
            s_copy(b).start()

        @pl.loop(0, blocks)
        def _(b):
            o_copy(b).wait_recv()
            s_copy(b).wait_recv()
            far = jnp.concatenate([st_recv[b], jnp.zeros((HEAD - 8, HEAD), F32)], axis=0).T
            near = st_loc[b]
            for i in range(PER_BLOCK):
                at = pl.ds(i * HEAD, HEAD)
                m_a, l_a = near[:, 2 * i:2 * i + 1], near[:, 2 * i + 1:2 * i + 2]
                m_b, l_b = far[:, 2 * i:2 * i + 1], far[:, 2 * i + 1:2 * i + 2]
                peak = jnp.maximum(m_a, m_b)
                w_a, w_b = jnp.exp(m_a - peak), jnp.exp(m_b - peak)
                norm_l = 1.0 / (l_a * w_a + l_b * w_b)
                o = o_loc[b, :, at] * (w_a * norm_l) + o_recv[b, :, at] * (w_b * norm_l)
                obuf[:, pl.ds(pl.multiple_of(core * half + b * TILE + i * HEAD, 128), HEAD)] = o.astype(BF16)
            piece = obuf.at[:, pl.ds(col(b), TILE)]
            remote(piece, piece, dsend.at[0], drecv.at[0], partner).start()

        mine = obuf.at[:, pl.ds(my_cols, half)]
        theirs = obuf.at[:, pl.ds(other_cols, half)]
        remote(mine, theirs, dsend.at[0], drecv.at[0], partner).wait_send()
        remote(mine, theirs, dsend.at[0], drecv.at[0], partner).wait_recv()

        @pl.loop(0, blocks)
        def _(b):
            q_copy(b).wait_send()
            o_copy(b).wait_send()
            s_copy(b).wait_send()

        for dst, k in ((k_out, 0), (v_out, 3)):
            to_me = dst.at[:, pl.ds(my_cols, half)]
            to_me2 = dst.at[:, pl.ds(other_cols, half)]
            pltpu.make_async_copy(to_me, to_me, asem.at[k]).wait()
            remote(to_me, to_me2, asem.at[k + 1], asem.at[k + 2], partner).wait_send()
            remote(to_me, to_me2, asem.at[k + 1], asem.at[k + 2], partner).wait_recv()

    def both_wait(buf, sem, width, my_at, other_at):
        mine = buf.at[:, pl.ds(my_at, width)]
        theirs = buf.at[:, pl.ds(other_at, width)]
        remote(mine, theirs, dsend.at[sem], drecv.at[sem], partner).wait_send()
        remote(mine, theirs, dsend.at[sem], drecv.at[sem], partner).wait_recv()

    attention(xin, base1, 0, cache1, k1_out, v1_out)

    def cache2_copy(kv, kind):
        src, dst = ((ck2, kc), (cv2, vc))[kv]
        who, to_core, to_chip = ((None, core, chip), (partner, 1 - core, chip), (peer, core, 1 - chip),
                                 (diag, 1 - core, 1 - chip))[kind]
        side = 0 if kind < 2 else quart
        from_at = pl.ds(pl.multiple_of(to_core * half + to_chip * quart, 128), quart)
        to = dst.at[pl.ds(pl.multiple_of(core * cache_rows, 16), cache_rows), pl.ds(side, quart)]
        if kind == 0:
            return pltpu.make_async_copy(src.at[:, from_at], to, c2send.at[4 * kv])
        return remote(src.at[:, from_at], to, c2send.at[4 * kv + kind], c2recv.at[4 * kv + kind], who)

    for kind in (2, 3, 1, 0):
        for kv in range(2):
            cache2_copy(kv, kind).start()

    @pl.loop(0, blocks)
    def _(b):
        s = base1 + 3 * blocks + b
        slot = wait_tile(s)
        y = jnp.dot(obuf[...], wring[slot], preferred_element_type=F32).astype(BF16)
        start_tile(s + SLOTS, base1 + 3 * blocks + SLOTS, base_up + SLOTS)
        at = pl.ds(col(b), TILE)
        hbuf[:, at] = (xin[:, at].astype(F32) + y.astype(F32)).astype(BF16)
        remote(hbuf.at[:, at], hbuf.at[:, at], dsend.at[1], drecv.at[1], partner).start()

    both_wait(hbuf, 1, half, my_cols, other_cols)
    norm(hbuf, nbuf, 0, crows)

    @pl.loop(0, ffn)
    def _(n):
        s = base_up + n
        slot = wait_tile(s)
        both = jnp.dot(nbuf[pl.ds(0, crows), :], wring[slot], preferred_element_type=F32)
        start_tile(s + SLOTS, base_up + SLOTS, base_down + SLOTS)
        gate = both[:, :TILE // 2].astype(BF16).astype(F32)
        up = both[:, TILE // 2:].astype(BF16).astype(F32)
        at = pl.ds(pl.multiple_of(core * ffh + n * (TILE // 2), 128), TILE // 2)
        ebuf[:, at] = (jax.nn.silu(gate) * up).astype(BF16)
        remote(ebuf.at[:, at], ebuf.at[:, at], dsend.at[2], drecv.at[2], partner).start()

    both_wait(ebuf, 2, ffh, pl.multiple_of(core * ffh, 128), pl.multiple_of((1 - core) * ffh, 128))

    def g_piece(b, first):
        return gbuf.at[pl.ds(first, crows), pl.ds(col(b), TILE)]

    @pl.loop(0, blocks)
    def _(b):
        at = pl.ds(col(b), TILE)
        acc = hbuf[:, at].astype(F32)
        for k in range(3):
            s = base_down + 3 * b + k
            slot = wait_tile(s, ffc)
            part = jnp.dot(ebuf[:, k * ffc:(k + 1) * ffc], wring[slot, :ffc, :], preferred_element_type=F32)
            start_tile(s + SLOTS, base_down + k + SLOTS, base2 - 2 + k + SLOTS)
            down = part if k == 0 else down + part
        gbuf[pl.ds(chip_rows, crows), at] = (acc + down).astype(BF16)
        piece = g_piece(b, chip_rows)
        remote(piece, piece, gxs.at[b], gxr.at[b], peer).start()
        remote(piece, piece, dsend.at[3], drecv.at[3], partner).start()

    def g_wait(first, sem):
        mine = gbuf.at[pl.ds(first, crows), pl.ds(my_cols, half)]
        theirs = gbuf.at[pl.ds(first, crows), pl.ds(other_cols, half)]
        remote(mine, theirs, dsend.at[sem], drecv.at[sem], partner).wait_send()
        remote(mine, theirs, dsend.at[sem], drecv.at[sem], partner).wait_recv()

    g_wait(chip_rows, 3)
    g_copy = pltpu.make_async_copy(gbuf.at[pl.ds(pl.multiple_of(chip_rows + my_rows, 16), rows), :], g_out, gsem.at[0])
    g_copy.start()
    norm(gbuf, nbuf, chip_rows, crows)

    @pl.loop(0, blocks)
    def _(b):
        far = g_piece(b, far_rows)
        remote(far, far, gxs.at[b], gxr.at[b], peer).wait_recv()
        remote(far, far, dsend.at[0], drecv.at[0], partner).start()

    g_wait(far_rows, 0)
    norm(gbuf, nbuf, far_rows, crows)

    heads2 = quart // HEAD
    row_2 = lax.broadcasted_iota(jnp.int32, (2 * crows, 2 * crows), 0)
    col_2 = lax.broadcasted_iota(jnp.int32, (2 * crows, 2 * crows), 1)

    def qk_tile(b):
        return b + 1 + b // 2

    def attend2(b):
        t = qk_tile(b)
        vt = 3 * (b // 2)
        dims_t = (((1,), (1,)), ((), ()))
        visible = col_2 <= row_2
        for i in range(2):
            near = pl.ds(pl.multiple_of(b * PAIR + i * HEAD, 128), HEAD)
            far = pl.ds(pl.multiple_of(quart + b * PAIR + i * HEAD, 128), HEAD)
            v_at = pl.ds(pl.multiple_of(lax.rem(b, 2) * PAIR + i * HEAD, 128), HEAD)
            q = pre[t, :, pl.ds(i * HEAD, HEAD)]
            s_a = lax.dot_general(q, kc[:, near], dims_t, preferred_element_type=F32) * scale
            s_b = lax.dot_general(q, kc[:, far], dims_t, preferred_element_type=F32) * scale
            s_n = lax.dot_general(q, pre[t, :, pl.ds(PAIR + i * HEAD, HEAD)], dims_t, preferred_element_type=F32) * scale
            s_n = jnp.where(visible, s_n, -jnp.inf)
            peak = jnp.maximum(jnp.maximum(jnp.max(s_a, axis=1, keepdims=True), jnp.max(s_b, axis=1, keepdims=True)),
                               jnp.max(s_n, axis=1, keepdims=True))
            p_a, p_b, p_n = jnp.exp(s_a - peak), jnp.exp(s_b - peak), jnp.exp(s_n - peak)
            total_p = (jnp.sum(p_a, axis=1, keepdims=True) + jnp.sum(p_b, axis=1, keepdims=True)
                       + jnp.sum(p_n, axis=1, keepdims=True))
            acc = jnp.dot(p_a.astype(BF16), vc[:, near], preferred_element_type=F32)
            acc = acc + jnp.dot(p_b.astype(BF16), vc[:, far], preferred_element_type=F32)
            acc = acc + jnp.dot(p_n.astype(BF16), pre[vt, :, v_at], preferred_element_type=F32)
            opair[:, pl.ds(i * HEAD, HEAD)] = (acc * (1.0 / total_p)).astype(BF16)

    def o2_piece(b, from_chip):
        return obuf.at[:, pl.ds(pl.multiple_of(from_chip * quart + b * PAIR, 128), PAIR)]

    def o2_far(b):
        return obuf.at[:, pl.ds(pl.multiple_of(half + b * PAIR, 128), PAIR)]

    def o2_copy(b):
        return remote(o2_far(b), o2_piece(b, chip), osend.at[b], orecv.at[b], peer)

    def append2(b, kind):
        who, to_core, to_chip = ((None, core, chip), (partner, 1 - core, chip), (peer, core, 1 - chip),
                                 (diag, 1 - core, 1 - chip))[kind]
        row_at = pl.ds(pl.multiple_of(to_chip * crows + to_core * rows, 16), rows)
        to_at = pl.ds(pl.multiple_of(own2 + b * PAIR, 128), PAIR)
        v_at = pl.ds(pl.multiple_of(lax.rem(b, 2) * PAIR, 128), PAIR)
        for kv, (part, dst) in enumerate(((pre.at[qk_tile(b), row_at, pl.ds(PAIR, PAIR)], k2_out),
                                          (pre.at[3 * (b // 2), row_at, v_at], v2_out))):
            if kind == 0:
                pltpu.make_async_copy(part, dst.at[:, to_at], a2send.at[4 * kv]).start()
            else:
                remote(part, dst.at[:, to_at], a2send.at[4 * kv + kind], a2recv.at[4 * kv + kind], who).start()

    early = 2

    @pl.loop(0, qkv2)
    def _(t):
        s = base2 + t

        @pl.when(t == qkv2 - 2)
        def _():
            at = wring.at[lax.rem(s, SLOTS), :, pl.ds(0, PAIR)]
            pltpu.make_async_copy(at, at, wsem.at[lax.rem(s, SLOTS)]).wait()

        @pl.when(t != qkv2 - 2)
        def _():
            wait_tile(s)

        raw = jnp.dot(nbuf[...], wring[lax.rem(s, SLOTS)], preferred_element_type=F32)
        start_tile(s + SLOTS, base2 + SLOTS, base2 + qkv2 + SLOTS)

        @pl.when(lax.rem(t, 3) == 0)
        def _():
            pre[t] = raw.astype(BF16)

        @pl.when(lax.rem(t, 3) != 0)
        def _():
            b = t - 1 - t // 3
            head = own2 // HEAD + 2 * b
            all_rows = pl.ds(0, 2 * crows)
            pre[t, :, pl.ds(0, PAIR)] = biased_rope(raw[:, :PAIR], 2, head, all_rows, 2)
            pre[t, :, pl.ds(PAIR, PAIR)] = biased_rope(raw[:, PAIR:], 3, head, all_rows, 2)

            @pl.when(b == 0)
            def _():
                for kv in range(2):
                    for kind in range(4):
                        cache2_copy(kv, kind).wait()

            attend2(b)
            obuf[:, pl.ds(pl.multiple_of(chip * quart + b * PAIR, 128), PAIR)] = opair[pl.ds(chip_rows, crows), :]
            obuf[:, pl.ds(pl.multiple_of(half + b * PAIR, 128), PAIR)] = opair[pl.ds(far_rows, crows), :]
            o2_copy(b).start()
            append2(b, 0)
            append2(b, 1)

            @pl.when(b < early)
            def _():
                append2(b, 2)
                append2(b, 3)

    @pl.loop(early, blocks)
    def _(b):
        append2(b, 2)
        append2(b, 3)

    @pl.loop(0, blocks)
    def _(b):
        remote(o2_far(b), o2_piece(b, 1 - chip), osend.at[b], orecv.at[b], peer).wait_recv()

    def y_copy(b):
        return remote(o_send.at[b], o_recv.at[b], qsend.at[b], qrecv.at[b], partner)

    @pl.loop(0, blocks)
    def _(b):
        slot = wait_tile(base2 + qkv2 + b)
        for i in range(2):
            y = jnp.dot(obuf[:, :half], wring[slot, i * half:(i + 1) * half, :], preferred_element_type=F32)
            at = pl.ds(i * rows, rows)
            for j in range(PER_BLOCK):
                lanes = pl.ds(j * HEAD, HEAD)
                st_loc[j] = y[:, j * HEAD:(j + 1) * HEAD]
                o_send[b, at, lanes] = st_loc[j, pl.ds(other_rows, rows), :]
                o_loc[b, at, lanes] = st_loc[j, pl.ds(my_rows, rows), :]
        y_copy(b).start()

    @pl.loop(0, blocks)
    def _(b):
        y_copy(b).wait_recv()
        for i in range(2):
            at = pl.ds(i * rows, rows)
            ybuf[:, pl.ds(pl.multiple_of(b * 2 * TILE + i * TILE, 128), TILE)] = (o_loc[b, at, :] + o_recv[b, at, :]).astype(BF16)

    y_copy_out = pltpu.make_async_copy(ybuf, y_out, gsem.at[1])
    y_copy_out.start()

    @pl.loop(0, blocks)
    def _(b):
        y_copy(b).wait_send()
        o2_copy(b).wait_send()
        remote(g_piece(b, chip_rows), g_piece(b, chip_rows), gxs.at[b], gxr.at[b], peer).wait_send()

    for kv, dst in enumerate((k2_out, v2_out)):
        ref = dst.at[:, pl.ds(0, quart)]
        pltpu.make_async_copy(ref, ref, a2send.at[4 * kv]).wait()
        for kind, who in ((1, partner), (2, peer), (3, diag)):
            remote(ref, ref, a2send.at[4 * kv + kind], a2recv.at[4 * kv + kind], who).wait_send()
            remote(ref, ref, a2send.at[4 * kv + kind], a2recv.at[4 * kv + kind], who).wait_recv()
    y_copy_out.wait()
    g_copy.wait()


def solution(mesh):
    rows_spec = P(('dp', 'cp'), None)
    cache_spec = P(('dp', 'cp'), None, None)
    mat_spec = P(None, None)
    vec_spec = P(None)
    layer_specs = (cache_spec, cache_spec, mat_spec, vec_spec, mat_spec, vec_spec, mat_spec, mat_spec)
    in_specs = (rows_spec,) + layer_specs + (mat_spec, mat_spec, mat_spec) + layer_specs
    out_specs = (rows_spec, rows_spec, cache_spec, cache_spec, cache_spec, cache_spec)

    def forward(x_in, cache_k1, cache_v1, w_q1, b_q1, w_k1, b_k1, w_v1, w_o1, w_gate, w_up, w_down, cache_k2, cache_v2, w_q2, b_q2, w_k2, b_k2, w_v2, w_o2):
        rows, d_model = x_in.shape
        cache_rows, heads, head_dim = cache_k1.shape
        ff = w_gate.shape[1]
        half = d_model // 2
        blocks = half // TILE
        crows = 2 * rows
        cos_t, sin_t = rope_tables(4 * cache_rows + np.arange(2 * crows), head_dim)
        bias = [v.reshape(heads, head_dim) for v in (b_q1, b_k1, b_q2, b_k2)]

        def flat(c):
            return c.reshape(cache_rows, d_model)

        any_spec = pl.BlockSpec(memory_space=pl.ANY)
        vmem_spec = pl.BlockSpec(memory_space=pltpu.VMEM)
        row_out = jax.ShapeDtypeStruct((rows, d_model), BF16)
        dma = pltpu.SemaphoreType.DMA
        out = pl.pallas_call(
            functools.partial(body, (d_model, ff, rows, cache_rows)),
            out_shape=[row_out] * 6,
            in_specs=[vmem_spec] * 6 + [any_spec] * 16,
            out_specs=[any_spec] * 6,
            scratch_shapes=[
                pltpu.VMEM((SLOTS, d_model, TILE), BF16),
                pltpu.VMEM((2 * crows, d_model), BF16),
                pltpu.VMEM((2 * crows, d_model), BF16),
                pltpu.VMEM((crows, ff), BF16),
                pltpu.VMEM((2 * blocks, 2 * crows, TILE), BF16),
                pltpu.VMEM((2 * cache_rows, half), BF16),
                pltpu.VMEM((2 * cache_rows, half), BF16),
                pltpu.VMEM((blocks, crows, TILE), F32),
                pltpu.VMEM((blocks, crows, TILE), F32),
                pltpu.VMEM((blocks, crows, TILE), F32),
                pltpu.VMEM((crows, d_model), BF16),
                pltpu.VMEM((2 * crows, TILE // 2), BF16),
                pltpu.VMEM((blocks, crows, HEAD), F32),
                pltpu.VMEM((blocks, 8, HEAD), F32),
                pltpu.VMEM((blocks, 8, HEAD), F32),
                pltpu.VMEM((4, heads, head_dim), F32),
                dma((SLOTS,)), dma((3,)), dma((6,)), dma((8,)), dma((8,)),
                dma((blocks,)), dma((blocks,)), dma((blocks,)), dma((blocks,)), dma((blocks,)), dma((blocks,)),
                dma((5,)), dma((5,)), dma((6,)), dma((2,)),
                dma((blocks,)), dma((blocks,)), dma((8,)), dma((8,)),
            ],
            compiler_params=pltpu.CompilerParams(
                collective_id=0, has_side_effects=True, vmem_limit_bytes=67043328),
        )(cos_t, sin_t, *bias, x_in, flat(cache_k1), flat(cache_v1), flat(cache_k2), flat(cache_v2),
          w_q1, w_k1, w_v1, w_o1, w_gate, w_up, w_down, w_q2, w_k2, w_v2, w_o2)
        g, y2, k1, v1, k2, v2 = out

        def heads_of(a):
            return a.reshape(rows, heads, head_dim)

        return g, y2, heads_of(k1), heads_of(v1), heads_of(k2), heads_of(v2)

    return jax.shard_map(forward, mesh=mesh, in_specs=in_specs, out_specs=out_specs, check_vma=False)
```

```python
import functools
import math

import jax
import jax.numpy as jnp
import numpy as np
from jax import lax
from jax.experimental import pallas as pl
from jax.experimental.pallas import tpu as pltpu
from jax.sharding import PartitionSpec as P

ROPE_THETA = 500000.0
NORM_EPS = 1e-5
MESH = pl.DeviceIdType.MESH
F32 = jnp.float32
BF16 = jnp.bfloat16

TILE = 512
HEAD = 128
PER_BLOCK = TILE // HEAD
SLOTS = 7


def rope_tables(positions, head_dim):
    half_dim = head_dim // 2
    inv_freq = (1.0 / (ROPE_THETA ** (np.arange(half_dim, dtype=np.float32) * np.float32(2.0 / head_dim)))).astype(np.float32)
    angles = positions.astype(np.float32)[:, None] * inv_freq[None, :]
    cos_t, sin_t = np.cos(angles), np.sin(angles)
    return np.concatenate([cos_t, cos_t], axis=1), np.concatenate([-sin_t, sin_t], axis=1)


def body(dims, cos_ref, sin_ref, bq1, bk1, bq2, bk2, x_hbm, ck1, cv1, ck2, cv2, wq1, wk1, wv1, wo1, w_gate, w_up, w_down,
         wq2, wk2, wv2, wo2, g_out, y_out, k1_out, v1_out, k2_out, v2_out,
         wring, nbuf, gbuf, ebuf, pre, kc, vc, o_loc, o_send, o_recv, obuf, opair,
         st_loc, st_send, st_recv, bias32,
         wsem, xsem, csem, c2send, c2recv, qsend, qrecv, osend, orecv, ssend, srecv, dsend, drecv, asem, gsem,
         gxs, gxr, a2send, a2recv):
    d_model, ff, rows, cache_rows = dims
    half = d_model // 2
    ffh = ff // 2
    ffc = ff // 3
    blocks = half // TILE
    ffn = ffh // (TILE // 2)
    crows = 2 * rows
    quart = half // 2
    ybuf = nbuf.at[pl.ds(0, rows), :]
    me = lax.axis_index("cp")
    core = lax.rem(me, 2)
    chip = me // 2
    partner = me + 1 - 2 * core
    peer = lax.rem(me + 2, 4)
    diag = 3 - me
    chip_rows = pl.multiple_of(chip * crows, 16)
    xin = hbuf = gbuf.at[pl.ds(pl.multiple_of(chip * crows, 16), crows), :]
    far_rows = pl.multiple_of((1 - chip) * crows, 16)
    my_cols = pl.multiple_of(core * half, 128)
    my_rows = pl.multiple_of(core * rows, 16)
    other_rows = pl.multiple_of((1 - core) * rows, 16)
    other_cols = pl.multiple_of((1 - core) * half, 128)

    def col(b):
        return pl.multiple_of(core * half + b * TILE, 128)

    attn_tiles = 4 * blocks
    base1 = 0
    base_up = attn_tiles
    base_down = base_up + ffn
    base2 = base_down + 3 * blocks
    qkv2 = 8

    def start_full(w, b, slot):
        pltpu.make_async_copy(w.at[:, pl.ds(col(b), TILE)], wring.at[slot], wsem.at[slot]).start()

    def start_mlp(n, slot):
        at = pl.ds(pl.multiple_of(core * ffh + n * (TILE // 2), 128), TILE // 2)
        pltpu.make_async_copy(w_gate.at[:, at], wring.at[slot, :, pl.ds(0, TILE // 2)], wsem.at[slot]).start()
        pltpu.make_async_copy(w_up.at[:, at], wring.at[slot, :, pl.ds(TILE // 2, TILE // 2)], wsem.at[slot]).start()

    def start_down(i, slot):
        pltpu.make_async_copy(
            w_down.at[pl.ds(pl.multiple_of(lax.rem(i, 3) * ffc, 16), ffc), pl.ds(col(i // 3), TILE)],
            wring.at[slot, pl.ds(0, ffc), :], wsem.at[slot]).start()

    loop_end = 3 * (blocks - 1) + 1

    def attn_segments(base, wq, wk, wv, wo):
        return [
            (base, base + 1, lambda r, slot: start_full(wq, 0, slot), None),
            (base + 1, base + loop_end, lambda r, slot: start_full(wq, r // 3 + 1, slot), 0),
            (base + 1, base + loop_end, lambda r, slot: start_full(wk, r // 3, slot), 1),
            (base + 1, base + loop_end, lambda r, slot: start_full(wv, r // 3, slot), 2),
            (base + loop_end, base + loop_end + 1, lambda r, slot: start_full(wk, blocks - 1, slot), None),
            (base + loop_end + 1, base + loop_end + 2, lambda r, slot: start_full(wv, blocks - 1, slot), None),
            (base + loop_end + 2, base + attn_tiles, lambda r, slot: start_full(wo, r, slot), None),
        ]

    PAIR = TILE // 2
    own2 = core * half + chip * quart

    def start_v2(t, slot):
        @pl.when(t < qkv2 - 2)
        def _():
            pltpu.make_async_copy(wv2.at[:, pl.ds(pl.multiple_of(own2 + (t // 3) * TILE, 128), TILE)], wring.at[slot],
                                  wsem.at[slot]).start()

        @pl.when(t >= qkv2 - 2)
        def _():
            pltpu.make_async_copy(wv2.at[:, pl.ds(pl.multiple_of(own2 + (t // 3) * TILE, 128), PAIR)],
                                  wring.at[slot, :, pl.ds(0, PAIR)], wsem.at[slot]).start()

    def start_qk2(t, slot):
        at = pl.ds(pl.multiple_of(own2 + (t - 1 - t // 3) * PAIR, 128), PAIR)
        pltpu.make_async_copy(wq2.at[:, at], wring.at[slot, :, pl.ds(0, PAIR)], wsem.at[slot]).start()
        pltpu.make_async_copy(wk2.at[:, at], wring.at[slot, :, pl.ds(PAIR, PAIR)], wsem.at[slot]).start()

    def start_wo2(b, slot):
        for i in range(2):
            pltpu.make_async_copy(
                wo2.at[pl.ds(my_cols, half), pl.ds(pl.multiple_of(b * 2 * TILE + i * TILE, 128), TILE)],
                wring.at[slot, pl.ds(i * half, half), :], wsem.at[slot]).start()

    segments = attn_segments(base1, wq1, wk1, wv1, wo1) + [
        (base_up, base_down, start_mlp, None),
        (base_down, base2, start_down, None),
        (base2, base2 + qkv2, start_v2, 0),
        (base2, base2 + qkv2, start_qk2, 1),
        (base2, base2 + qkv2, start_qk2, 2),
        (base2 + qkv2, base2 + qkv2 + blocks, start_wo2, None),
    ]

    def start_tile(s, lo, hi):
        slot = lax.rem(s, SLOTS) if not isinstance(s, int) else s % SLOTS
        for a, b, fn, phase in segments:
            if b <= lo or a >= hi:
                continue
            if isinstance(s, int):
                if a <= s < b and (phase is None or (s - a) % 3 == phase):
                    fn(s - a, slot)
                continue
            cond = (s >= a) & (s < b)
            if phase is not None:
                cond = cond & (lax.rem(s - a + 3, 3) == phase)

            @pl.when(cond)
            def _(a=a, fn=fn):
                fn(s - a, slot)

    def wait_tile(s, depth=None):
        slot = lax.rem(s, SLOTS) if not isinstance(s, int) else s % SLOTS
        ref = wring.at[slot] if depth is None else wring.at[slot, pl.ds(0, depth), :]
        pltpu.make_async_copy(ref, ref, wsem.at[slot]).wait()
        return slot

    def remote(src, dst, send, recv, who):
        return pltpu.make_async_remote_copy(src_ref=src, dst_ref=dst, send_sem=send, recv_sem=recv,
                                            device_id={"cp": who}, device_id_type=MESH)

    for s in range(2):
        start_tile(s, s, s + 1)

    barrier = pltpu.get_barrier_semaphore()
    for who in (partner, peer, diag):
        pl.semaphore_signal(barrier, inc=1, device_id={"cp": who}, device_id_type=MESH)
    pl.semaphore_wait(barrier, 3)

    x_loc = pltpu.make_async_copy(x_hbm, xin.at[pl.ds(my_rows, rows)], xsem.at[0])
    x_rem = remote(x_hbm, xin.at[pl.ds(my_rows, rows)], xsem.at[1], xsem.at[2], partner)
    x_rem.start()
    x_loc.start()

    def cache_copies(ck, cv):
        crow = pl.ds(pl.multiple_of(core * cache_rows, 16), cache_rows)
        out = []
        for i, (src, dst) in enumerate(((ck, kc), (cv, vc))):
            out.append(pltpu.make_async_copy(src.at[:, pl.ds(my_cols, half)], dst.at[crow], csem.at[3 * i]))
            out.append(remote(src.at[:, pl.ds(other_cols, half)], dst.at[crow], csem.at[3 * i + 1], csem.at[3 * i + 2],
                              partner))
        return out

    cache1 = cache_copies(ck1, cv1)
    for c in cache1:
        c.start()
    for s in range(2, SLOTS):
        start_tile(s, s, s + 1)
    for i, ref in enumerate((bq1, bk1, bq2, bk2)):
        bias32[i] = ref[...].astype(F32)
    x_loc.wait()
    x_rem.wait()

    def biased_rope(vals, bias_row, first_head, table_at, n):
        parts = []
        cos_t, sin_t = cos_ref[table_at, :], sin_ref[table_at, :]
        for i in range(n):
            seg = vals[:, i * HEAD:(i + 1) * HEAD] + bias32[bias_row, pl.ds(first_head + i, 1), :]
            seg = seg.astype(BF16).astype(F32)
            parts.append((seg * cos_t + pltpu.roll(seg, HEAD // 2, 1) * sin_t).astype(BF16))
        return jnp.concatenate(parts, axis=1)

    def norm(src, dst, first, count):
        step = 16

        @pl.loop(0, count // step)
        def _(i):
            at = pl.ds(pl.multiple_of(first + i * step, step), step)
            wide = src[at, :].astype(F32)
            dst[at, :] = (wide * lax.rsqrt(jnp.mean(wide * wide, axis=-1, keepdims=True) + NORM_EPS)).astype(BF16)

    row_i = lax.broadcasted_iota(jnp.int32, (2 * crows, crows), 0)
    col_i = lax.broadcasted_iota(jnp.int32, (2 * crows, crows), 1)
    far_lim = jnp.where(chip == 0, crows, -1)
    scale = HEAD ** -0.5 * math.log2(math.e)

    def attend(b):
        lane = lax.broadcasted_iota(jnp.int32, (2 * crows, HEAD), 1)
        visible = col_i <= jnp.where(row_i < crows, row_i, far_lim)
        stats = jnp.zeros((2 * crows, HEAD), F32)
        dims_t = (((1,), (1,)), ((), ()))
        for i in range(PER_BLOCK):
            at = pl.ds(i * HEAD, HEAD)
            cat = pl.ds(pl.multiple_of(b * TILE + i * HEAD, 128), HEAD)
            q = pre[b, :, at]
            s_old = lax.dot_general(q, kc[:, cat], dims_t, preferred_element_type=F32)
            s_new = lax.dot_general(q, pre[blocks + b, pl.ds(0, crows), at], dims_t, preferred_element_type=F32)
            s_new = jnp.where(visible, s_new, -jnp.inf)
            peak = jnp.maximum(jnp.max(s_old, axis=1, keepdims=True), jnp.max(s_new, axis=1, keepdims=True))
            p_old = jnp.exp2((s_old - peak) * scale)
            p_new = jnp.exp2((s_new - peak) * scale)
            total_p = jnp.sum(p_old, axis=1, keepdims=True) + jnp.sum(p_new, axis=1, keepdims=True)
            acc = jnp.dot(p_old.astype(BF16), vc[:, cat], preferred_element_type=F32)
            acc = acc + jnp.dot(p_new.astype(BF16), pre[blocks + b, pl.ds(crows, crows), at], preferred_element_type=F32)
            o_loc[b, :, at] = acc[:crows]
            o_send[b, :, at] = acc[crows:]
            stats = jnp.where(lane == 2 * i, peak, stats)
            stats = jnp.where(lane == 2 * i + 1, total_p, stats)
        st_loc[b] = stats[:crows]
        st_send[b] = stats[crows:].T[:8, :]

    def q_copy(b):
        return remote(pre.at[b, pl.ds(0, crows), :], pre.at[b, pl.ds(crows, crows), :], qsend.at[b], qrecv.at[b], peer)

    def o_copy(b):
        return remote(o_send.at[b], o_recv.at[b], osend.at[b], orecv.at[b], peer)

    def s_copy(b):
        return remote(st_send.at[b], st_recv.at[b], ssend.at[b], srecv.at[b], peer)

    def head_of(b):
        return core * (half // HEAD) + b * PER_BLOCK

    def attention(layer_in, base, bias_row, caches, k_out, v_out):
        def q_step(b, s, lo, hi):
            slot = wait_tile(s)
            raw = jnp.dot(layer_in[...], wring[slot], preferred_element_type=F32)
            start_tile(s + SLOTS, lo + SLOTS, hi + SLOTS)
            pre[b, pl.ds(0, crows), :] = biased_rope(raw, bias_row, head_of(b), pl.ds(chip_rows, crows), PER_BLOCK)
            q_copy(b).start()

        q_step(0, base, base, base + 1)

        @pl.loop(0, blocks)
        def _(b):
            has_q = (2 * blocks - 3 - b) // (blocks - 1)
            s = base + 1 + 3 * b

            @pl.when(b < blocks - 1)
            def _():
                q_step(b + 1, s, base + 1, base + loop_end)

            s = s + has_q
            slot = wait_tile(s)
            raw = jnp.dot(layer_in[...], wring[slot], preferred_element_type=F32)
            start_tile(s + SLOTS, base + 2 + SLOTS, base + loop_end + 2 + SLOTS)
            pre[blocks + b, pl.ds(0, crows), :] = biased_rope(raw, bias_row + 1, head_of(b), pl.ds(chip_rows, crows), PER_BLOCK)
            s = s + 1
            slot = wait_tile(s)
            vals = jnp.dot(layer_in[...], wring[slot], preferred_element_type=F32).astype(BF16)
            start_tile(s + SLOTS, base + 3 + SLOTS, base + loop_end + 2 + SLOTS)
            pre[blocks + b, pl.ds(crows, crows), :] = vals

            @pl.when(b == 0)
            def _():
                for c in caches:
                    c.wait()

            q_copy(b).wait_recv()
            attend(b)
            for part, dst, k in ((0, k_out, 0), (crows, v_out, 3)):
                pltpu.make_async_copy(pre.at[blocks + b, pl.ds(part + my_rows, rows), :], dst.at[:, pl.ds(col(b), TILE)], asem.at[k]).start()
                remote(pre.at[blocks + b, pl.ds(part + other_rows, rows), :], dst.at[:, pl.ds(col(b), TILE)], asem.at[k + 1],
                       asem.at[k + 2], partner).start()
            o_copy(b).start()
            s_copy(b).start()

        @pl.loop(0, blocks)
        def _(b):
            o_copy(b).wait_recv()
            s_copy(b).wait_recv()
            far = jnp.concatenate([st_recv[b], jnp.zeros((HEAD - 8, HEAD), F32)], axis=0).T
            near = st_loc[b]
            for i in range(PER_BLOCK):
                at = pl.ds(i * HEAD, HEAD)
                m_a, l_a = near[:, 2 * i:2 * i + 1], near[:, 2 * i + 1:2 * i + 2]
                m_b, l_b = far[:, 2 * i:2 * i + 1], far[:, 2 * i + 1:2 * i + 2]
                peak = jnp.maximum(m_a, m_b)
                w_a, w_b = jnp.exp2((m_a - peak) * scale), jnp.exp2((m_b - peak) * scale)
                norm_l = 1.0 / (l_a * w_a + l_b * w_b)
                o = o_loc[b, :, at] * (w_a * norm_l) + o_recv[b, :, at] * (w_b * norm_l)
                obuf[:, pl.ds(pl.multiple_of(core * half + b * TILE + i * HEAD, 128), HEAD)] = o.astype(BF16)
            piece = obuf.at[:, pl.ds(col(b), TILE)]
            remote(piece, piece, dsend.at[0], drecv.at[0], partner).start()

        mine = obuf.at[:, pl.ds(my_cols, half)]
        theirs = obuf.at[:, pl.ds(other_cols, half)]
        remote(mine, theirs, dsend.at[0], drecv.at[0], partner).wait_send()
        remote(mine, theirs, dsend.at[0], drecv.at[0], partner).wait_recv()

        @pl.loop(0, blocks)
        def _(b):
            q_copy(b).wait_send()
            o_copy(b).wait_send()
            s_copy(b).wait_send()

        for dst, k in ((k_out, 0), (v_out, 3)):
            to_me = dst.at[:, pl.ds(my_cols, half)]
            to_me2 = dst.at[:, pl.ds(other_cols, half)]
            pltpu.make_async_copy(to_me, to_me, asem.at[k]).wait()
            remote(to_me, to_me2, asem.at[k + 1], asem.at[k + 2], partner).wait_send()
            remote(to_me, to_me2, asem.at[k + 1], asem.at[k + 2], partner).wait_recv()

    def both_wait(buf, sem, width, my_at, other_at):
        mine = buf.at[:, pl.ds(my_at, width)]
        theirs = buf.at[:, pl.ds(other_at, width)]
        remote(mine, theirs, dsend.at[sem], drecv.at[sem], partner).wait_send()
        remote(mine, theirs, dsend.at[sem], drecv.at[sem], partner).wait_recv()

    attention(xin, base1, 0, cache1, k1_out, v1_out)

    PIECE = TILE // 2

    def cache2_copy(kv, kind, b=None):
        src, dst = ((ck2, kc), (cv2, vc))[kv]
        who, to_core, to_chip = ((None, core, chip), (partner, 1 - core, chip), (peer, core, 1 - chip),
                                 (diag, 1 - core, 1 - chip))[kind]
        off, width, sem = (0, quart, 0) if b is None else (b * PIECE, PIECE, 1 + b)
        side = 0 if kind < 2 else quart
        from_at = pl.ds(pl.multiple_of(to_core * half + to_chip * quart + off, 128), width)
        to = dst.at[pl.ds(pl.multiple_of(core * cache_rows, 16), cache_rows), pl.ds(pl.multiple_of(side + off, 128), width)]
        i = 4 * kv + kind
        if kind == 0:
            return pltpu.make_async_copy(src.at[:, from_at], to, c2send.at[i])
        return remote(src.at[:, from_at], to, c2send.at[i], c2recv.at[i, sem], who)

    def far_cache(b):
        for kv in range(2):
            for kind in (2, 3):
                cache2_copy(kv, kind, b).start()

    for b in range(3):
        far_cache(b)
    for kind in (1, 0):
        for kv in range(2):
            cache2_copy(kv, kind).start()

    @pl.loop(0, blocks)
    def _(b):
        s = base1 + 3 * blocks + b
        slot = wait_tile(s)
        y = jnp.dot(obuf[...], wring[slot], preferred_element_type=F32).astype(BF16)
        start_tile(s + SLOTS, base1 + 3 * blocks + SLOTS, base_up + SLOTS)
        at = pl.ds(col(b), TILE)
        hbuf[:, at] = (xin[:, at].astype(F32) + y.astype(F32)).astype(BF16)
        remote(hbuf.at[:, at], hbuf.at[:, at], dsend.at[1], drecv.at[1], partner).start()

    both_wait(hbuf, 1, half, my_cols, other_cols)
    norm(hbuf, nbuf, 0, crows)

    @pl.loop(0, ffn)
    def _(n):
        s = base_up + n
        slot = wait_tile(s)
        both = jnp.dot(nbuf[pl.ds(0, crows), :], wring[slot], preferred_element_type=F32)
        start_tile(s + SLOTS, base_up + SLOTS, base_down + SLOTS)
        gate = both[:, :TILE // 2].astype(BF16).astype(F32)
        up = both[:, TILE // 2:].astype(BF16).astype(F32)
        at = pl.ds(pl.multiple_of(core * ffh + n * (TILE // 2), 128), TILE // 2)
        ebuf[:, at] = (jax.nn.silu(gate) * up).astype(BF16)
        remote(ebuf.at[:, at], ebuf.at[:, at], dsend.at[2], drecv.at[2], partner).start()

        @pl.when(n == ffn // 2)
        def _():
            far_cache(3)

    both_wait(ebuf, 2, ffh, pl.multiple_of(core * ffh, 128), pl.multiple_of((1 - core) * ffh, 128))

    def g_piece(b, first):
        return gbuf.at[pl.ds(first, crows), pl.ds(col(b), TILE)]

    @pl.loop(0, blocks)
    def _(b):
        at = pl.ds(col(b), TILE)
        acc = hbuf[:, at].astype(F32)
        for k in range(3):
            s = base_down + 3 * b + k
            slot = wait_tile(s, ffc)
            part = jnp.dot(ebuf[:, k * ffc:(k + 1) * ffc], wring[slot, :ffc, :], preferred_element_type=F32)
            start_tile(s + SLOTS, base_down + k + SLOTS, base2 - 2 + k + SLOTS)
            down = part if k == 0 else down + part
        gbuf[pl.ds(chip_rows, crows), at] = (acc + down).astype(BF16)
        piece = g_piece(b, chip_rows)
        remote(piece, piece, gxs.at[b], gxr.at[b], peer).start()
        remote(piece, piece, dsend.at[3], drecv.at[3], partner).start()

    def g_wait(first, sem):
        mine = gbuf.at[pl.ds(first, crows), pl.ds(my_cols, half)]
        theirs = gbuf.at[pl.ds(first, crows), pl.ds(other_cols, half)]
        remote(mine, theirs, dsend.at[sem], drecv.at[sem], partner).wait_send()
        remote(mine, theirs, dsend.at[sem], drecv.at[sem], partner).wait_recv()

    far_cache(4)
    g_wait(chip_rows, 3)
    g_rows = pl.ds(pl.multiple_of(chip_rows + my_rows, 16), rows)
    g_copies = [pltpu.make_async_copy(gbuf.at[g_rows, pl.ds(j * TILE, TILE)], g_out.at[j], gsem.at[0]) for j in range(2 * blocks)]
    for c in g_copies:
        c.start()
    norm(gbuf, nbuf, chip_rows, crows)

    @pl.loop(0, blocks)
    def _(b):
        far = g_piece(b, far_rows)
        remote(far, far, gxs.at[b], gxr.at[b], peer).wait_recv()
        remote(far, far, dsend.at[0], drecv.at[0], partner).start()

    g_wait(far_rows, 0)
    norm(gbuf, nbuf, far_rows, crows)

    heads2 = quart // HEAD
    row_2 = lax.broadcasted_iota(jnp.int32, (2 * crows, 2 * crows), 0)
    col_2 = lax.broadcasted_iota(jnp.int32, (2 * crows, 2 * crows), 1)

    def qk_tile(b):
        return b + 1 + b // 2

    def attend2(b):
        t = qk_tile(b)
        vt = 3 * (b // 2)
        dims_t = (((1,), (1,)), ((), ()))
        visible = col_2 <= row_2
        for i in range(2):
            near = pl.ds(pl.multiple_of(b * PAIR + i * HEAD, 128), HEAD)
            far = pl.ds(pl.multiple_of(quart + b * PAIR + i * HEAD, 128), HEAD)
            v_at = pl.ds(pl.multiple_of(lax.rem(b, 2) * PAIR + i * HEAD, 128), HEAD)
            q = pre[t, :, pl.ds(i * HEAD, HEAD)]
            s_a = lax.dot_general(q, kc[:, near], dims_t, preferred_element_type=F32)
            s_b = lax.dot_general(q, kc[:, far], dims_t, preferred_element_type=F32)
            s_n = lax.dot_general(q, pre[t, :, pl.ds(PAIR + i * HEAD, HEAD)], dims_t, preferred_element_type=F32)
            s_n = jnp.where(visible, s_n, -jnp.inf)
            peak = jnp.maximum(jnp.maximum(jnp.max(s_a, axis=1, keepdims=True), jnp.max(s_b, axis=1, keepdims=True)),
                               jnp.max(s_n, axis=1, keepdims=True))
            p_a, p_b, p_n = (jnp.exp2((s - peak) * scale) for s in (s_a, s_b, s_n))
            total_p = (jnp.sum(p_a, axis=1, keepdims=True) + jnp.sum(p_b, axis=1, keepdims=True)
                       + jnp.sum(p_n, axis=1, keepdims=True))
            acc = jnp.dot(p_a.astype(BF16), vc[:, near], preferred_element_type=F32)
            acc = acc + jnp.dot(p_b.astype(BF16), vc[:, far], preferred_element_type=F32)
            acc = acc + jnp.dot(p_n.astype(BF16), pre[vt, :, v_at], preferred_element_type=F32)
            opair[:, pl.ds(i * HEAD, HEAD)] = (acc * (1.0 / total_p)).astype(BF16)

    def o2_piece(b, from_chip):
        return obuf.at[:, pl.ds(pl.multiple_of(from_chip * quart + b * PAIR, 128), PAIR)]

    def o2_far(b):
        return obuf.at[:, pl.ds(pl.multiple_of(half + b * PAIR, 128), PAIR)]

    def o2_copy(b):
        return remote(o2_far(b), o2_piece(b, chip), osend.at[b], orecv.at[b], peer)

    def append2(b, kind):
        who, to_core, to_chip = ((None, core, chip), (partner, 1 - core, chip), (peer, core, 1 - chip),
                                 (diag, 1 - core, 1 - chip))[kind]
        row_at = pl.ds(pl.multiple_of(to_chip * crows + to_core * rows, 16), rows)
        to_at = pl.ds(pl.multiple_of(own2 + b * PAIR, 128), PAIR)
        v_at = pl.ds(pl.multiple_of(lax.rem(b, 2) * PAIR, 128), PAIR)
        for kv, (part, dst) in enumerate(((pre.at[qk_tile(b), row_at, pl.ds(PAIR, PAIR)], k2_out),
                                          (pre.at[3 * (b // 2), row_at, v_at], v2_out))):
            if kind == 0:
                pltpu.make_async_copy(part, dst.at[:, to_at], a2send.at[4 * kv]).start()
            else:
                remote(part, dst.at[:, to_at], a2send.at[4 * kv + kind], a2recv.at[4 * kv + kind], who).start()

    early = 2

    @pl.loop(0, qkv2)
    def _(t):
        s = base2 + t

        @pl.when(t == qkv2 - 2)
        def _():
            at = wring.at[lax.rem(s, SLOTS), :, pl.ds(0, PAIR)]
            pltpu.make_async_copy(at, at, wsem.at[lax.rem(s, SLOTS)]).wait()

        @pl.when(t != qkv2 - 2)
        def _():
            wait_tile(s)

        raw = jnp.dot(nbuf[...], wring[lax.rem(s, SLOTS)], preferred_element_type=F32)
        start_tile(s + SLOTS, base2 + SLOTS, base2 + qkv2 + SLOTS)

        @pl.when(lax.rem(t, 3) == 0)
        def _():
            pre[t] = raw.astype(BF16)

        @pl.when(lax.rem(t, 3) != 0)
        def _():
            b = t - 1 - t // 3
            head = own2 // HEAD + 2 * b
            all_rows = pl.ds(0, 2 * crows)
            pre[t, :, pl.ds(0, PAIR)] = biased_rope(raw[:, :PAIR], 2, head, all_rows, 2)
            pre[t, :, pl.ds(PAIR, PAIR)] = biased_rope(raw[:, PAIR:], 3, head, all_rows, 2)

            @pl.when(b == 0)
            def _():
                for kv in range(2):
                    for kind in range(2):
                        cache2_copy(kv, kind).wait()

            for kv in range(2):
                for kind in (2, 3):
                    cache2_copy(kv, kind, b).wait_recv()
            attend2(b)
            obuf[:, pl.ds(pl.multiple_of(chip * quart + b * PAIR, 128), PAIR)] = opair[pl.ds(chip_rows, crows), :]
            obuf[:, pl.ds(pl.multiple_of(half + b * PAIR, 128), PAIR)] = opair[pl.ds(far_rows, crows), :]
            o2_copy(b).start()
            append2(b, 0)
            append2(b, 1)

            @pl.when(b < early)
            def _():
                append2(b, 2)
                append2(b, 3)

    @pl.loop(early, blocks)
    def _(b):
        append2(b, 2)
        append2(b, 3)

    @pl.loop(0, blocks)
    def _(b):
        remote(o2_far(b), o2_piece(b, 1 - chip), osend.at[b], orecv.at[b], peer).wait_recv()

    def y_copy(b):
        return remote(o_send.at[b], o_recv.at[b], qsend.at[b], qrecv.at[b], partner)

    @pl.loop(0, blocks)
    def _(b):
        slot = wait_tile(base2 + qkv2 + b)
        for i in range(2):
            y = jnp.dot(obuf[:, :half], wring[slot, i * half:(i + 1) * half, :], preferred_element_type=F32)
            at = pl.ds(i * rows, rows)
            for j in range(PER_BLOCK):
                lanes = pl.ds(j * HEAD, HEAD)
                st_loc[j] = y[:, j * HEAD:(j + 1) * HEAD]
                o_send[b, at, lanes] = st_loc[j, pl.ds(other_rows, rows), :]
                o_loc[b, at, lanes] = st_loc[j, pl.ds(my_rows, rows), :]
        y_copy(b).start()

    @pl.loop(0, blocks)
    def _(b):
        y_copy(b).wait_recv()
        for i in range(2):
            at = pl.ds(i * rows, rows)
            ybuf[:, pl.ds(pl.multiple_of(b * 2 * TILE + i * TILE, 128), TILE)] = (o_loc[b, at, :] + o_recv[b, at, :]).astype(BF16)

    y_copies = [pltpu.make_async_copy(ybuf.at[:, pl.ds(j * TILE, TILE)], y_out.at[j], gsem.at[1]) for j in range(2 * blocks)]
    for c in y_copies:
        c.start()

    @pl.loop(0, blocks)
    def _(b):
        y_copy(b).wait_send()
        o2_copy(b).wait_send()
        remote(g_piece(b, chip_rows), g_piece(b, chip_rows), gxs.at[b], gxr.at[b], peer).wait_send()

    for kv, dst in enumerate((k2_out, v2_out)):
        ref = dst.at[:, pl.ds(0, quart)]
        pltpu.make_async_copy(ref, ref, a2send.at[4 * kv]).wait()
        for kind, who in ((1, partner), (2, peer), (3, diag)):
            remote(ref, ref, a2send.at[4 * kv + kind], a2recv.at[4 * kv + kind], who).wait_send()
            remote(ref, ref, a2send.at[4 * kv + kind], a2recv.at[4 * kv + kind], who).wait_recv()
        for kind in (2, 3):
            cache2_copy(kv, kind).wait_send()
    for ref, sem in ((y_out, 1), (g_out, 0)):
        pltpu.make_async_copy(ref, ref, gsem.at[sem]).wait()


def solution(mesh):
    rows_spec = P(('dp', 'cp'), None)
    cache_spec = P(('dp', 'cp'), None, None)
    mat_spec = P(None, None)
    vec_spec = P(None)
    layer_specs = (cache_spec, cache_spec, mat_spec, vec_spec, mat_spec, vec_spec, mat_spec, mat_spec)
    in_specs = (rows_spec,) + layer_specs + (mat_spec, mat_spec, mat_spec) + layer_specs
    out_specs = (rows_spec, rows_spec, cache_spec, cache_spec, cache_spec, cache_spec)

    def forward(x_in, cache_k1, cache_v1, w_q1, b_q1, w_k1, b_k1, w_v1, w_o1, w_gate, w_up, w_down, cache_k2, cache_v2, w_q2, b_q2, w_k2, b_k2, w_v2, w_o2):
        rows, d_model = x_in.shape
        cache_rows, heads, head_dim = cache_k1.shape
        ff = w_gate.shape[1]
        half = d_model // 2
        blocks = half // TILE
        crows = 2 * rows
        cos_t, sin_t = rope_tables(4 * cache_rows + np.arange(2 * crows), head_dim)
        bias = [v.reshape(heads, head_dim) for v in (b_q1, b_k1, b_q2, b_k2)]

        def flat(c):
            return c.reshape(cache_rows, d_model)

        any_spec = pl.BlockSpec(memory_space=pl.ANY)
        vmem_spec = pl.BlockSpec(memory_space=pltpu.VMEM)
        blocked = jax.ShapeDtypeStruct((2 * blocks, rows, TILE), BF16)
        row_out = jax.ShapeDtypeStruct((rows, d_model), BF16)
        dma = pltpu.SemaphoreType.DMA
        out = pl.pallas_call(
            functools.partial(body, (d_model, ff, rows, cache_rows)),
            out_shape=[blocked] * 2 + [row_out] * 4,
            in_specs=[vmem_spec] * 6 + [any_spec] * 16,
            out_specs=[any_spec] * 6,
            scratch_shapes=[
                pltpu.VMEM((SLOTS, d_model, TILE), BF16),
                pltpu.VMEM((2 * crows, d_model), BF16),
                pltpu.VMEM((2 * crows, d_model), BF16),
                pltpu.VMEM((crows, ff), BF16),
                pltpu.VMEM((2 * blocks, 2 * crows, TILE), BF16),
                pltpu.VMEM((2 * cache_rows, half), BF16),
                pltpu.VMEM((2 * cache_rows, half), BF16),
                pltpu.VMEM((blocks, crows, TILE), F32),
                pltpu.VMEM((blocks, crows, TILE), F32),
                pltpu.VMEM((blocks, crows, TILE), F32),
                pltpu.VMEM((crows, d_model), BF16),
                pltpu.VMEM((2 * crows, TILE // 2), BF16),
                pltpu.VMEM((blocks, crows, HEAD), F32),
                pltpu.VMEM((blocks, 8, HEAD), F32),
                pltpu.VMEM((blocks, 8, HEAD), F32),
                pltpu.VMEM((4, heads, head_dim), F32),
                dma((SLOTS,)), dma((3,)), dma((6,)), dma((8,)), dma((8, 6)),
                dma((blocks,)), dma((blocks,)), dma((blocks,)), dma((blocks,)), dma((blocks,)), dma((blocks,)),
                dma((5,)), dma((5,)), dma((6,)), dma((2,)),
                dma((blocks,)), dma((blocks,)), dma((8,)), dma((8,)),
            ],
            compiler_params=pltpu.CompilerParams(
                collective_id=0, has_side_effects=True, vmem_limit_bytes=67043328),
        )(cos_t, sin_t, *bias, x_in, flat(cache_k1), flat(cache_v1), flat(cache_k2), flat(cache_v2),
          w_q1, w_k1, w_v1, w_o1, w_gate, w_up, w_down, w_q2, w_k2, w_v2, w_o2)
        g, y2, k1, v1, k2, v2 = out

        def heads_of(a):
            return a.reshape(rows, heads, head_dim)

        def unblock(a):
            return a.transpose(1, 0, 2).reshape(rows, d_model)

        return unblock(g), unblock(y2), heads_of(k1), heads_of(v1), heads_of(k2), heads_of(v2)

    return jax.shard_map(forward, mesh=mesh, in_specs=in_specs, out_specs=out_specs, check_vma=False)
```

```python
import functools
import math

import jax
import jax.numpy as jnp
import numpy as np
from jax import lax
from jax.experimental import pallas as pl
from jax.experimental.pallas import tpu as pltpu
from jax.sharding import PartitionSpec as P

ROPE_THETA = 500000.0
NORM_EPS = 1e-5
MESH = pl.DeviceIdType.MESH
F32 = jnp.float32
BF16 = jnp.bfloat16

TILE = 512
HEAD = 128
PER_BLOCK = TILE // HEAD
SLOTS = 7


def rope_tables(positions, head_dim):
    half_dim = head_dim // 2
    inv_freq = (1.0 / (ROPE_THETA ** (np.arange(half_dim, dtype=np.float32) * np.float32(2.0 / head_dim)))).astype(np.float32)
    angles = positions.astype(np.float32)[:, None] * inv_freq[None, :]
    cos_t, sin_t = np.cos(angles), np.sin(angles)
    return np.concatenate([cos_t, cos_t], axis=1), np.concatenate([-sin_t, sin_t], axis=1)


def body(dims, cos_ref, sin_ref, bq1, bk1, bq2, bk2, x_hbm, ck1, cv1, ck2, cv2, wq1, wk1, wv1, wo1, w_gate, w_up, w_down,
         wq2, wk2, wv2, wo2, g_out, y_out, k1_out, v1_out, k2_out, v2_out,
         wring, nbuf, gbuf, ebuf, pre, kc, vc, o_loc, o_send, o_recv, obuf, opair,
         st_loc, st_send, st_recv, bias32,
         wsem, xsem, csem, c2send, c2recv, qsend, qrecv, osend, orecv, ssend, srecv, dsend, drecv, asem, gsem,
         gxs, gxr, a2send, a2recv, hys, hyr, esem, yfree):
    d_model, ff, rows, cache_rows = dims
    half = d_model // 2
    ffh = ff // 2
    ffc = ff // 3
    third = ffc // 2
    part = third // (TILE // 2)
    blocks = half // TILE
    ffn = ffh // (TILE // 2)
    crows = 2 * rows
    quart = half // 2
    ybuf = nbuf.at[pl.ds(0, rows), :]
    me = lax.axis_index("cp")
    core = lax.rem(me, 2)
    chip = me // 2
    partner = me + 1 - 2 * core
    peer = lax.rem(me + 2, 4)
    diag = 3 - me
    dp = lax.axis_index("dp")
    side_y = 1 - dp
    chip_rows = pl.multiple_of(chip * crows, 16)
    xin = hbuf = gbuf.at[pl.ds(pl.multiple_of(chip * crows, 16), crows), :]
    far_rows = pl.multiple_of((1 - chip) * crows, 16)
    my_cols = pl.multiple_of(core * half, 128)
    my_rows = pl.multiple_of(core * rows, 16)
    other_rows = pl.multiple_of((1 - core) * rows, 16)
    other_cols = pl.multiple_of((1 - core) * half, 128)

    def col(b):
        return pl.multiple_of(core * half + b * TILE, 128)

    attn_tiles = 4 * blocks
    base1 = 0
    base_up = attn_tiles
    base_down = base_up + 2 * part
    base2 = base_down + 3 * blocks
    qkv2 = 8

    def start_full(w, b, slot):
        pltpu.make_async_copy(w.at[:, pl.ds(col(b), TILE)], wring.at[slot], wsem.at[slot]).start()

    def mlp_cols(tile):
        return pl.ds(pl.multiple_of(core * ffh + tile * (TILE // 2), 128), TILE // 2)

    def shared_tile(n):
        return part + dp * part + n

    def start_mlp(tile, slot):
        at = mlp_cols(tile)
        pltpu.make_async_copy(w_gate.at[:, at], wring.at[slot, :, pl.ds(0, TILE // 2)], wsem.at[slot]).start()
        pltpu.make_async_copy(w_up.at[:, at], wring.at[slot, :, pl.ds(TILE // 2, TILE // 2)], wsem.at[slot]).start()

    def start_down(b, chunk, slot):
        for i in range(2):
            pltpu.make_async_copy(
                w_down.at[pl.ds(pl.multiple_of(i * ffh + chunk * third, 16), third), pl.ds(col(b), TILE)],
                wring.at[slot, pl.ds(i * third, third), :], wsem.at[slot]).start()

    loop_end = 3 * (blocks - 1) + 1

    def attn_segments(base, wq, wk, wv, wo):
        return [
            (base, base + 1, lambda r, slot: start_full(wq, 0, slot), None),
            (base + 1, base + loop_end, lambda r, slot: start_full(wq, r // 3 + 1, slot), 0),
            (base + 1, base + loop_end, lambda r, slot: start_full(wk, r // 3, slot), 1),
            (base + 1, base + loop_end, lambda r, slot: start_full(wv, r // 3, slot), 2),
            (base + loop_end, base + loop_end + 1, lambda r, slot: start_full(wk, blocks - 1, slot), None),
            (base + loop_end + 1, base + loop_end + 2, lambda r, slot: start_full(wv, blocks - 1, slot), None),
            (base + loop_end + 2, base + attn_tiles, lambda r, slot: start_full(wo, r, slot), None),
        ]

    PAIR = TILE // 2
    own2 = core * half + chip * quart

    def start_v2(t, slot):
        @pl.when(t < qkv2 - 2)
        def _():
            pltpu.make_async_copy(wv2.at[:, pl.ds(pl.multiple_of(own2 + (t // 3) * TILE, 128), TILE)], wring.at[slot],
                                  wsem.at[slot]).start()

        @pl.when(t >= qkv2 - 2)
        def _():
            pltpu.make_async_copy(wv2.at[:, pl.ds(pl.multiple_of(own2 + (t // 3) * TILE, 128), PAIR)],
                                  wring.at[slot, :, pl.ds(0, PAIR)], wsem.at[slot]).start()

    def start_qk2(t, slot):
        at = pl.ds(pl.multiple_of(own2 + (t - 1 - t // 3) * PAIR, 128), PAIR)
        pltpu.make_async_copy(wq2.at[:, at], wring.at[slot, :, pl.ds(0, PAIR)], wsem.at[slot]).start()
        pltpu.make_async_copy(wk2.at[:, at], wring.at[slot, :, pl.ds(PAIR, PAIR)], wsem.at[slot]).start()

    def start_wo2(b, slot):
        for i in range(2):
            pltpu.make_async_copy(
                wo2.at[pl.ds(my_cols, half), pl.ds(pl.multiple_of(b * 2 * TILE + i * TILE, 128), TILE)],
                wring.at[slot, pl.ds(i * half, half), :], wsem.at[slot]).start()

    segments = attn_segments(base1, wq1, wk1, wv1, wo1) + [
        (base_up, base_up + part, start_mlp, None),
        (base_up + part, base_down, lambda r, slot: start_mlp(shared_tile(r), slot), None),
        (base_down, base_down + blocks, lambda r, slot: start_down(r, 0, slot), None),
        (base_down + blocks, base2, lambda r, slot: start_down(r // 2, 1 + r % 2 if isinstance(r, int) else 1 + lax.rem(r, 2), slot), None),
        (base2, base2 + qkv2, start_v2, 0),
        (base2, base2 + qkv2, start_qk2, 1),
        (base2, base2 + qkv2, start_qk2, 2),
        (base2 + qkv2, base2 + qkv2 + blocks, start_wo2, None),
    ]

    def start_tile(s, lo, hi):
        slot = lax.rem(s, SLOTS) if not isinstance(s, int) else s % SLOTS
        for a, b, fn, phase in segments:
            if b <= lo or a >= hi:
                continue
            if isinstance(s, int):
                if a <= s < b and (phase is None or (s - a) % 3 == phase):
                    fn(s - a, slot)
                continue
            cond = (s >= a) & (s < b)
            if phase is not None:
                cond = cond & (lax.rem(s - a + 3, 3) == phase)

            @pl.when(cond)
            def _(a=a, fn=fn):
                fn(s - a, slot)

    def wait_tile(s, depth=None):
        slot = lax.rem(s, SLOTS) if not isinstance(s, int) else s % SLOTS
        ref = wring.at[slot] if depth is None else wring.at[slot, pl.ds(0, depth), :]
        pltpu.make_async_copy(ref, ref, wsem.at[slot]).wait()
        return slot

    def remote(src, dst, send, recv, who):
        return pltpu.make_async_remote_copy(src_ref=src, dst_ref=dst, send_sem=send, recv_sem=recv,
                                            device_id={"cp": who}, device_id_type=MESH)

    def remote_y(src, dst, send, recv):
        return pltpu.make_async_remote_copy(src_ref=src, dst_ref=dst, send_sem=send, recv_sem=recv,
                                            device_id={"dp": side_y}, device_id_type=MESH)

    for s in range(2):
        start_tile(s, s, s + 1)

    barrier = pltpu.get_barrier_semaphore()
    for who in (partner, peer, diag):
        pl.semaphore_signal(barrier, inc=1, device_id={"cp": who}, device_id_type=MESH)
    pl.semaphore_signal(barrier, inc=1, device_id={"dp": side_y}, device_id_type=MESH)
    pl.semaphore_wait(barrier, 4)

    x_loc = pltpu.make_async_copy(x_hbm, xin.at[pl.ds(my_rows, rows)], xsem.at[0])
    x_rem = remote(x_hbm, xin.at[pl.ds(my_rows, rows)], xsem.at[1], xsem.at[2], partner)
    x_rem.start()
    x_loc.start()

    def cache_copies(ck, cv):
        crow = pl.ds(pl.multiple_of(core * cache_rows, 16), cache_rows)
        out = []
        for i, (src, dst) in enumerate(((ck, kc), (cv, vc))):
            out.append(pltpu.make_async_copy(src.at[:, pl.ds(my_cols, half)], dst.at[crow], csem.at[3 * i]))
            out.append(remote(src.at[:, pl.ds(other_cols, half)], dst.at[crow], csem.at[3 * i + 1], csem.at[3 * i + 2],
                              partner))
        return out

    cache1 = cache_copies(ck1, cv1)
    for c in cache1:
        c.start()
    for s in range(2, SLOTS):
        start_tile(s, s, s + 1)
    for i, ref in enumerate((bq1, bk1, bq2, bk2)):
        bias32[i] = ref[...].astype(F32)
    x_loc.wait()
    x_rem.wait()

    def biased_rope(vals, bias_row, first_head, table_at, n):
        parts = []
        cos_t, sin_t = cos_ref[table_at, :], sin_ref[table_at, :]
        for i in range(n):
            seg = vals[:, i * HEAD:(i + 1) * HEAD] + bias32[bias_row, pl.ds(first_head + i, 1), :]
            seg = seg.astype(BF16).astype(F32)
            parts.append((seg * cos_t + pltpu.roll(seg, HEAD // 2, 1) * sin_t).astype(BF16))
        return jnp.concatenate(parts, axis=1)

    def norm(src, dst, first, count):
        step = 16

        @pl.loop(0, count // step)
        def _(i):
            at = pl.ds(pl.multiple_of(first + i * step, step), step)
            wide = src[at, :].astype(F32)
            dst[at, :] = (wide * lax.rsqrt(jnp.mean(wide * wide, axis=-1, keepdims=True) + NORM_EPS)).astype(BF16)

    row_i = lax.broadcasted_iota(jnp.int32, (2 * crows, crows), 0)
    col_i = lax.broadcasted_iota(jnp.int32, (2 * crows, crows), 1)
    far_lim = jnp.where(chip == 0, crows, -1)
    scale = HEAD ** -0.5 * math.log2(math.e)

    def attend(b):
        lane = lax.broadcasted_iota(jnp.int32, (2 * crows, HEAD), 1)
        visible = col_i <= jnp.where(row_i < crows, row_i, far_lim)
        stats = jnp.zeros((2 * crows, HEAD), F32)
        dims_t = (((1,), (1,)), ((), ()))
        for i in range(PER_BLOCK):
            at = pl.ds(i * HEAD, HEAD)
            cat = pl.ds(pl.multiple_of(b * TILE + i * HEAD, 128), HEAD)
            q = pre[b, :, at]
            s_old = lax.dot_general(q, kc[:, cat], dims_t, preferred_element_type=F32)
            s_new = lax.dot_general(q, pre[blocks + b, pl.ds(0, crows), at], dims_t, preferred_element_type=F32)
            s_new = jnp.where(visible, s_new, -jnp.inf)
            peak = jnp.maximum(jnp.max(s_old, axis=1, keepdims=True), jnp.max(s_new, axis=1, keepdims=True))
            p_old = jnp.exp2((s_old - peak) * scale)
            p_new = jnp.exp2((s_new - peak) * scale)
            total_p = jnp.sum(p_old, axis=1, keepdims=True) + jnp.sum(p_new, axis=1, keepdims=True)
            acc = jnp.dot(p_old.astype(BF16), vc[:, cat], preferred_element_type=F32)
            acc = acc + jnp.dot(p_new.astype(BF16), pre[blocks + b, pl.ds(crows, crows), at], preferred_element_type=F32)
            o_loc[b, :, at] = acc[:crows]
            o_send[b, :, at] = acc[crows:]
            stats = jnp.where(lane == 2 * i, peak, stats)
            stats = jnp.where(lane == 2 * i + 1, total_p, stats)
        st_loc[b] = stats[:crows]
        st_send[b] = stats[crows:].T[:8, :]

    def q_copy(b):
        return remote(pre.at[b, pl.ds(0, crows), :], pre.at[b, pl.ds(crows, crows), :], qsend.at[b], qrecv.at[b], peer)

    def o_copy(b):
        return remote(o_send.at[b], o_recv.at[b], osend.at[b], orecv.at[b], peer)

    def s_copy(b):
        return remote(st_send.at[b], st_recv.at[b], ssend.at[b], srecv.at[b], peer)

    def head_of(b):
        return core * (half // HEAD) + b * PER_BLOCK

    def attention(layer_in, base, bias_row, caches, k_out, v_out):
        def q_step(b, s, lo, hi):
            slot = wait_tile(s)
            raw = jnp.dot(layer_in[...], wring[slot], preferred_element_type=F32)
            start_tile(s + SLOTS, lo + SLOTS, hi + SLOTS)
            pre[b, pl.ds(0, crows), :] = biased_rope(raw, bias_row, head_of(b), pl.ds(chip_rows, crows), PER_BLOCK)
            q_copy(b).start()

        q_step(0, base, base, base + 1)

        @pl.loop(0, blocks)
        def _(b):
            has_q = (2 * blocks - 3 - b) // (blocks - 1)
            s = base + 1 + 3 * b

            @pl.when(b < blocks - 1)
            def _():
                q_step(b + 1, s, base + 1, base + loop_end)

            s = s + has_q
            slot = wait_tile(s)
            raw = jnp.dot(layer_in[...], wring[slot], preferred_element_type=F32)
            start_tile(s + SLOTS, base + 2 + SLOTS, base + loop_end + 2 + SLOTS)
            pre[blocks + b, pl.ds(0, crows), :] = biased_rope(raw, bias_row + 1, head_of(b), pl.ds(chip_rows, crows), PER_BLOCK)
            s = s + 1
            slot = wait_tile(s)
            vals = jnp.dot(layer_in[...], wring[slot], preferred_element_type=F32).astype(BF16)
            start_tile(s + SLOTS, base + 3 + SLOTS, base + loop_end + 2 + SLOTS)
            pre[blocks + b, pl.ds(crows, crows), :] = vals

            @pl.when(b == 0)
            def _():
                for c in caches:
                    c.wait()

            q_copy(b).wait_recv()
            attend(b)
            for part, dst, k in ((0, k_out, 0), (crows, v_out, 3)):
                pltpu.make_async_copy(pre.at[blocks + b, pl.ds(part + my_rows, rows), :], dst.at[:, pl.ds(col(b), TILE)], asem.at[k]).start()
                remote(pre.at[blocks + b, pl.ds(part + other_rows, rows), :], dst.at[:, pl.ds(col(b), TILE)], asem.at[k + 1],
                       asem.at[k + 2], partner).start()
            o_copy(b).start()
            s_copy(b).start()

        @pl.loop(0, blocks)
        def _(b):
            o_copy(b).wait_recv()
            s_copy(b).wait_recv()
            far = jnp.concatenate([st_recv[b], jnp.zeros((HEAD - 8, HEAD), F32)], axis=0).T
            near = st_loc[b]
            for i in range(PER_BLOCK):
                at = pl.ds(i * HEAD, HEAD)
                m_a, l_a = near[:, 2 * i:2 * i + 1], near[:, 2 * i + 1:2 * i + 2]
                m_b, l_b = far[:, 2 * i:2 * i + 1], far[:, 2 * i + 1:2 * i + 2]
                peak = jnp.maximum(m_a, m_b)
                w_a, w_b = jnp.exp2((m_a - peak) * scale), jnp.exp2((m_b - peak) * scale)
                norm_l = 1.0 / (l_a * w_a + l_b * w_b)
                o = o_loc[b, :, at] * (w_a * norm_l) + o_recv[b, :, at] * (w_b * norm_l)
                obuf[:, pl.ds(pl.multiple_of(core * half + b * TILE + i * HEAD, 128), HEAD)] = o.astype(BF16)
            piece = obuf.at[:, pl.ds(col(b), TILE)]
            remote(piece, piece, dsend.at[0], drecv.at[0], partner).start()

        mine = obuf.at[:, pl.ds(my_cols, half)]
        theirs = obuf.at[:, pl.ds(other_cols, half)]
        remote(mine, theirs, dsend.at[0], drecv.at[0], partner).wait_send()
        remote(mine, theirs, dsend.at[0], drecv.at[0], partner).wait_recv()

        @pl.loop(0, blocks)
        def _(b):
            q_copy(b).wait_send()
            o_copy(b).wait_send()
            s_copy(b).wait_send()

        for dst, k in ((k_out, 0), (v_out, 3)):
            to_me = dst.at[:, pl.ds(my_cols, half)]
            to_me2 = dst.at[:, pl.ds(other_cols, half)]
            pltpu.make_async_copy(to_me, to_me, asem.at[k]).wait()
            remote(to_me, to_me2, asem.at[k + 1], asem.at[k + 2], partner).wait_send()
            remote(to_me, to_me2, asem.at[k + 1], asem.at[k + 2], partner).wait_recv()

    def both_wait(buf, sem, width, my_at, other_at):
        mine = buf.at[:, pl.ds(my_at, width)]
        theirs = buf.at[:, pl.ds(other_at, width)]
        remote(mine, theirs, dsend.at[sem], drecv.at[sem], partner).wait_send()
        remote(mine, theirs, dsend.at[sem], drecv.at[sem], partner).wait_recv()

    attention(xin, base1, 0, cache1, k1_out, v1_out)
    pl.semaphore_signal(yfree, inc=1, device_id={"dp": side_y}, device_id_type=MESH)

    PIECE = TILE // 2

    def cache2_copy(kv, kind, b=None):
        src, dst = ((ck2, kc), (cv2, vc))[kv]
        who, to_core, to_chip = ((None, core, chip), (partner, 1 - core, chip), (peer, core, 1 - chip),
                                 (diag, 1 - core, 1 - chip))[kind]
        off, width, sem = (0, quart, 0) if b is None else (b * PIECE, PIECE, 1 + b)
        side = 0 if kind < 2 else quart
        from_at = pl.ds(pl.multiple_of(to_core * half + to_chip * quart + off, 128), width)
        to = dst.at[pl.ds(pl.multiple_of(core * cache_rows, 16), cache_rows), pl.ds(pl.multiple_of(side + off, 128), width)]
        i = 4 * kv + kind
        if kind == 0:
            return pltpu.make_async_copy(src.at[:, from_at], to, c2send.at[i])
        return remote(src.at[:, from_at], to, c2send.at[i], c2recv.at[i, sem], who)

    def far_cache(b):
        for kv in range(2):
            for kind in (2, 3):
                cache2_copy(kv, kind, b).start()

    for b in range(3):
        far_cache(b)
    for kind in (1, 0):
        for kv in range(2):
            cache2_copy(kv, kind).start()

    pl.semaphore_wait(yfree, 1)

    def h_copy(b):
        return remote_y(hbuf.at[:, pl.ds(col(b), TILE)], pre.at[core * blocks + b, pl.ds(0, crows), :], hys.at[b], hyr.at[b])

    @pl.loop(0, blocks)
    def _(b):
        s = base1 + 3 * blocks + b
        slot = wait_tile(s)
        y = jnp.dot(obuf[...], wring[slot], preferred_element_type=F32).astype(BF16)
        start_tile(s + SLOTS, base1 + 3 * blocks + SLOTS, base_up + SLOTS)
        at = pl.ds(col(b), TILE)
        hbuf[:, at] = (xin[:, at].astype(F32) + y.astype(F32)).astype(BF16)
        h_copy(b).start()
        remote(hbuf.at[:, at], hbuf.at[:, at], dsend.at[1], drecv.at[1], partner).start()

    both_wait(hbuf, 1, half, my_cols, other_cols)
    norm(hbuf, nbuf, 0, crows)

    def glu(both):
        gate = both[:, :TILE // 2].astype(BF16).astype(F32)
        up = both[:, TILE // 2:].astype(BF16).astype(F32)
        return (jax.nn.silu(gate) * up).astype(BF16)

    @pl.loop(0, part)
    def _(n):
        s = base_up + n
        slot = wait_tile(s)
        both = jnp.dot(nbuf[pl.ds(0, crows), :], wring[slot], preferred_element_type=F32)
        start_tile(s + SLOTS, base_up + SLOTS, base_up + part + SLOTS)
        at = mlp_cols(n)
        ebuf[:, at] = glu(both)
        remote(ebuf.at[:, at], ebuf.at[:, at], dsend.at[2], drecv.at[2], partner).start()

    far_h = pre.at[pl.ds(core * blocks, blocks), pl.ds(0, crows), :]
    far_h_other = pre.at[pl.ds((1 - core) * blocks, blocks), pl.ds(0, crows), :]

    @pl.loop(0, blocks)
    def _(b):
        h_copy(b).wait_recv()
        h_copy(b).wait_send()

    remote(far_h, far_h, dsend.at[4], drecv.at[4], partner).start()
    remote(far_h, far_h, dsend.at[4], drecv.at[4], partner).wait_send()
    remote(far_h_other, far_h_other, dsend.at[4], drecv.at[4], partner).wait_recv()

    @pl.loop(0, crows // 16)
    def _(i):
        at = pl.ds(pl.multiple_of(i * 16, 16), 16)
        wide = [pre[j, at, :].astype(F32) for j in range(2 * blocks)]
        square = sum(jnp.sum(w * w, axis=-1, keepdims=True) for w in wide)
        inv = lax.rsqrt(square / d_model + NORM_EPS)
        for j in range(2 * blocks):
            nbuf[pl.ds(pl.multiple_of(crows + i * 16, 16), 16), pl.ds(j * TILE, TILE)] = (wide[j] * inv).astype(BF16)

    def e_return(n):
        return remote_y(pre.at[n, pl.ds(crows, crows), pl.ds(0, TILE // 2)], ebuf.at[:, mlp_cols(shared_tile(n))],
                        esem.at[0], esem.at[1])

    @pl.loop(0, part)
    def _(n):
        s = base_up + part + n
        slot = wait_tile(s)
        both = jnp.dot(nbuf[...], wring[slot], preferred_element_type=F32)
        start_tile(s + SLOTS, base_up + part + SLOTS, base_down + SLOTS)
        at = mlp_cols(shared_tile(n))
        mixed = glu(both)
        ebuf[:, at] = mixed[:crows]
        pre[n, pl.ds(crows, crows), pl.ds(0, TILE // 2)] = mixed[crows:]
        e_return(n).start()
        remote(ebuf.at[:, at], ebuf.at[:, at], dsend.at[2], drecv.at[2], partner).start()

    def returned(to_core):
        return ebuf.at[:, pl.ds(pl.multiple_of(to_core * ffh + (1 + side_y) * third, 128), third)]

    def partner_e_wait():
        some = ebuf.at[:, pl.ds(0, 2 * third)]
        remote(some, some, dsend.at[2], drecv.at[2], partner).wait_send()
        remote(some, some, dsend.at[2], drecv.at[2], partner).wait_recv()

    partner_e_wait()

    def down_dot(slot, chunk):
        out = None
        for i in range(2):
            at = pl.ds(pl.multiple_of(i * ffh + chunk * third, 128), third)
            term = jnp.dot(ebuf[:, at], wring[slot, i * third:(i + 1) * third, :], preferred_element_type=F32)
            out = term if out is None else out + term
        return out

    @pl.loop(0, blocks)
    def _(b):
        @pl.when(b == blocks - 2)
        def _():
            e_all = remote_y(returned(core), returned(core), esem.at[0], esem.at[1])
            e_all.wait_send()
            e_all.wait_recv()
            remote(returned(core), returned(core), dsend.at[1], drecv.at[1], partner).start()

        s = base_down + b
        slot = wait_tile(s, ffc)
        o_loc[b] = down_dot(slot, 0)
        start_tile(s + SLOTS, base_down + SLOTS, base_down + blocks + SLOTS)

    remote(returned(core), returned(core), dsend.at[1], drecv.at[1], partner).wait_send()
    remote(returned(1 - core), returned(1 - core), dsend.at[1], drecv.at[1], partner).wait_recv()

    def g_piece(b, first):
        return gbuf.at[pl.ds(first, crows), pl.ds(col(b), TILE)]

    @pl.loop(0, blocks)
    def _(b):
        at = pl.ds(col(b), TILE)
        down = o_loc[b]
        for k in range(2):
            s = base_down + blocks + 2 * b + k
            slot = wait_tile(s, ffc)
            down = down + down_dot(slot, 1 + k)
            start_tile(s + SLOTS, base_down + blocks + k + SLOTS, base2 - 1 + k + SLOTS)
        gbuf[pl.ds(chip_rows, crows), at] = (hbuf[:, at].astype(F32) + down).astype(BF16)
        piece = g_piece(b, chip_rows)
        remote(piece, piece, gxs.at[b], gxr.at[b], peer).start()
        remote(piece, piece, dsend.at[3], drecv.at[3], partner).start()

    def g_wait(first, sem):
        mine = gbuf.at[pl.ds(first, crows), pl.ds(my_cols, half)]
        theirs = gbuf.at[pl.ds(first, crows), pl.ds(other_cols, half)]
        remote(mine, theirs, dsend.at[sem], drecv.at[sem], partner).wait_send()
        remote(mine, theirs, dsend.at[sem], drecv.at[sem], partner).wait_recv()

    far_cache(3)
    far_cache(4)
    g_wait(chip_rows, 3)
    g_rows = pl.ds(pl.multiple_of(chip_rows + my_rows, 16), rows)
    g_copies = [pltpu.make_async_copy(gbuf.at[g_rows, pl.ds(j * TILE, TILE)], g_out.at[j], gsem.at[0]) for j in range(2 * blocks)]
    for c in g_copies:
        c.start()
    norm(gbuf, nbuf, chip_rows, crows)

    @pl.loop(0, blocks)
    def _(b):
        far = g_piece(b, far_rows)
        remote(far, far, gxs.at[b], gxr.at[b], peer).wait_recv()
        remote(far, far, dsend.at[0], drecv.at[0], partner).start()

    g_wait(far_rows, 0)
    norm(gbuf, nbuf, far_rows, crows)

    heads2 = quart // HEAD
    row_2 = lax.broadcasted_iota(jnp.int32, (2 * crows, 2 * crows), 0)
    col_2 = lax.broadcasted_iota(jnp.int32, (2 * crows, 2 * crows), 1)

    def qk_tile(b):
        return b + 1 + b // 2

    def attend2(b):
        t = qk_tile(b)
        vt = 3 * (b // 2)
        dims_t = (((1,), (1,)), ((), ()))
        visible = col_2 <= row_2
        for i in range(2):
            near = pl.ds(pl.multiple_of(b * PAIR + i * HEAD, 128), HEAD)
            far = pl.ds(pl.multiple_of(quart + b * PAIR + i * HEAD, 128), HEAD)
            v_at = pl.ds(pl.multiple_of(lax.rem(b, 2) * PAIR + i * HEAD, 128), HEAD)
            q = pre[t, :, pl.ds(i * HEAD, HEAD)]
            s_a = lax.dot_general(q, kc[:, near], dims_t, preferred_element_type=F32)
            s_b = lax.dot_general(q, kc[:, far], dims_t, preferred_element_type=F32)
            s_n = lax.dot_general(q, pre[t, :, pl.ds(PAIR + i * HEAD, HEAD)], dims_t, preferred_element_type=F32)
            s_n = jnp.where(visible, s_n, -jnp.inf)
            peak = jnp.maximum(jnp.maximum(jnp.max(s_a, axis=1, keepdims=True), jnp.max(s_b, axis=1, keepdims=True)),
                               jnp.max(s_n, axis=1, keepdims=True))
            p_a, p_b, p_n = (jnp.exp2((s - peak) * scale) for s in (s_a, s_b, s_n))
            total_p = (jnp.sum(p_a, axis=1, keepdims=True) + jnp.sum(p_b, axis=1, keepdims=True)
                       + jnp.sum(p_n, axis=1, keepdims=True))
            acc = jnp.dot(p_a.astype(BF16), vc[:, near], preferred_element_type=F32)
            acc = acc + jnp.dot(p_b.astype(BF16), vc[:, far], preferred_element_type=F32)
            acc = acc + jnp.dot(p_n.astype(BF16), pre[vt, :, v_at], preferred_element_type=F32)
            opair[:, pl.ds(i * HEAD, HEAD)] = (acc * (1.0 / total_p)).astype(BF16)

    def o2_piece(b, from_chip):
        return obuf.at[:, pl.ds(pl.multiple_of(from_chip * quart + b * PAIR, 128), PAIR)]

    def o2_far(b):
        return obuf.at[:, pl.ds(pl.multiple_of(half + b * PAIR, 128), PAIR)]

    def o2_copy(b):
        return remote(o2_far(b), o2_piece(b, chip), osend.at[b], orecv.at[b], peer)

    def append2(b, kind):
        who, to_core, to_chip = ((None, core, chip), (partner, 1 - core, chip), (peer, core, 1 - chip),
                                 (diag, 1 - core, 1 - chip))[kind]
        row_at = pl.ds(pl.multiple_of(to_chip * crows + to_core * rows, 16), rows)
        to_at = pl.ds(pl.multiple_of(own2 + b * PAIR, 128), PAIR)
        v_at = pl.ds(pl.multiple_of(lax.rem(b, 2) * PAIR, 128), PAIR)
        for kv, (part, dst) in enumerate(((pre.at[qk_tile(b), row_at, pl.ds(PAIR, PAIR)], k2_out),
                                          (pre.at[3 * (b // 2), row_at, v_at], v2_out))):
            if kind == 0:
                pltpu.make_async_copy(part, dst.at[:, to_at], a2send.at[4 * kv]).start()
            else:
                remote(part, dst.at[:, to_at], a2send.at[4 * kv + kind], a2recv.at[4 * kv + kind], who).start()

    early = 1

    @pl.loop(0, qkv2)
    def _(t):
        s = base2 + t

        @pl.when(t == qkv2 - 2)
        def _():
            at = wring.at[lax.rem(s, SLOTS), :, pl.ds(0, PAIR)]
            pltpu.make_async_copy(at, at, wsem.at[lax.rem(s, SLOTS)]).wait()

        @pl.when(t != qkv2 - 2)
        def _():
            wait_tile(s)

        raw = jnp.dot(nbuf[...], wring[lax.rem(s, SLOTS)], preferred_element_type=F32)
        start_tile(s + SLOTS, base2 + SLOTS, base2 + qkv2 + SLOTS)

        @pl.when(lax.rem(t, 3) == 0)
        def _():
            pre[t] = raw.astype(BF16)

        @pl.when(lax.rem(t, 3) != 0)
        def _():
            b = t - 1 - t // 3
            head = own2 // HEAD + 2 * b
            all_rows = pl.ds(0, 2 * crows)
            pre[t, :, pl.ds(0, PAIR)] = biased_rope(raw[:, :PAIR], 2, head, all_rows, 2)
            pre[t, :, pl.ds(PAIR, PAIR)] = biased_rope(raw[:, PAIR:], 3, head, all_rows, 2)

            @pl.when(b == 0)
            def _():
                for kv in range(2):
                    for kind in range(2):
                        cache2_copy(kv, kind).wait()

            for kv in range(2):
                for kind in (2, 3):
                    cache2_copy(kv, kind, b).wait_recv()
            attend2(b)
            obuf[:, pl.ds(pl.multiple_of(chip * quart + b * PAIR, 128), PAIR)] = opair[pl.ds(chip_rows, crows), :]
            obuf[:, pl.ds(pl.multiple_of(half + b * PAIR, 128), PAIR)] = opair[pl.ds(far_rows, crows), :]
            o2_copy(b).start()
            append2(b, 0)
            append2(b, 1)

            @pl.when(b < early)
            def _():
                append2(b, 2)
                append2(b, 3)

    @pl.loop(early, blocks)
    def _(b):
        append2(b, 2)
        append2(b, 3)

    @pl.loop(0, blocks)
    def _(b):
        remote(o2_far(b), o2_piece(b, 1 - chip), osend.at[b], orecv.at[b], peer).wait_recv()

    def y_copy(b):
        return remote(o_send.at[b], o_recv.at[b], qsend.at[b], qrecv.at[b], partner)

    @pl.loop(0, blocks)
    def _(b):
        slot = wait_tile(base2 + qkv2 + b)
        for i in range(2):
            y = jnp.dot(obuf[:, :half], wring[slot, i * half:(i + 1) * half, :], preferred_element_type=F32)
            at = pl.ds(i * rows, rows)
            for j in range(PER_BLOCK):
                lanes = pl.ds(j * HEAD, HEAD)
                st_loc[j] = y[:, j * HEAD:(j + 1) * HEAD]
                o_send[b, at, lanes] = st_loc[j, pl.ds(other_rows, rows), :]
                o_loc[b, at, lanes] = st_loc[j, pl.ds(my_rows, rows), :]
        y_copy(b).start()

    @pl.loop(0, blocks)
    def _(b):
        y_copy(b).wait_recv()
        for i in range(2):
            at = pl.ds(i * rows, rows)
            ybuf[:, pl.ds(pl.multiple_of(b * 2 * TILE + i * TILE, 128), TILE)] = (o_loc[b, at, :] + o_recv[b, at, :]).astype(BF16)

    y_copies = [pltpu.make_async_copy(ybuf.at[:, pl.ds(j * TILE, TILE)], y_out.at[j], gsem.at[1]) for j in range(2 * blocks)]
    for c in y_copies:
        c.start()

    @pl.loop(0, blocks)
    def _(b):
        y_copy(b).wait_send()
        o2_copy(b).wait_send()
        remote(g_piece(b, chip_rows), g_piece(b, chip_rows), gxs.at[b], gxr.at[b], peer).wait_send()

    for kv, dst in enumerate((k2_out, v2_out)):
        ref = dst.at[:, pl.ds(0, quart)]
        pltpu.make_async_copy(ref, ref, a2send.at[4 * kv]).wait()
        for kind, who in ((1, partner), (2, peer), (3, diag)):
            remote(ref, ref, a2send.at[4 * kv + kind], a2recv.at[4 * kv + kind], who).wait_send()
            remote(ref, ref, a2send.at[4 * kv + kind], a2recv.at[4 * kv + kind], who).wait_recv()
        for kind in (2, 3):
            cache2_copy(kv, kind).wait_send()
    for ref, sem in ((y_out, 1), (g_out, 0)):
        pltpu.make_async_copy(ref, ref, gsem.at[sem]).wait()


def solution(mesh):
    rows_spec = P(('dp', 'cp'), None)
    cache_spec = P(('dp', 'cp'), None, None)
    mat_spec = P(None, None)
    vec_spec = P(None)
    layer_specs = (cache_spec, cache_spec, mat_spec, vec_spec, mat_spec, vec_spec, mat_spec, mat_spec)
    in_specs = (rows_spec,) + layer_specs + (mat_spec, mat_spec, mat_spec) + layer_specs
    out_specs = (rows_spec, rows_spec, cache_spec, cache_spec, cache_spec, cache_spec)

    def forward(x_in, cache_k1, cache_v1, w_q1, b_q1, w_k1, b_k1, w_v1, w_o1, w_gate, w_up, w_down, cache_k2, cache_v2, w_q2, b_q2, w_k2, b_k2, w_v2, w_o2):
        rows, d_model = x_in.shape
        cache_rows, heads, head_dim = cache_k1.shape
        ff = w_gate.shape[1]
        half = d_model // 2
        blocks = half // TILE
        crows = 2 * rows
        cos_t, sin_t = rope_tables(4 * cache_rows + np.arange(2 * crows), head_dim)
        bias = [v.reshape(heads, head_dim) for v in (b_q1, b_k1, b_q2, b_k2)]

        def flat(c):
            return c.reshape(cache_rows, d_model)

        any_spec = pl.BlockSpec(memory_space=pl.ANY)
        vmem_spec = pl.BlockSpec(memory_space=pltpu.VMEM)
        blocked = jax.ShapeDtypeStruct((2 * blocks, rows, TILE), BF16)
        row_out = jax.ShapeDtypeStruct((rows, d_model), BF16)
        dma = pltpu.SemaphoreType.DMA
        out = pl.pallas_call(
            functools.partial(body, (d_model, ff, rows, cache_rows)),
            out_shape=[blocked] * 2 + [row_out] * 4,
            in_specs=[vmem_spec] * 6 + [any_spec] * 16,
            out_specs=[any_spec] * 6,
            scratch_shapes=[
                pltpu.VMEM((SLOTS, d_model, TILE), BF16),
                pltpu.VMEM((2 * crows, d_model), BF16),
                pltpu.VMEM((2 * crows, d_model), BF16),
                pltpu.VMEM((crows, ff), BF16),
                pltpu.VMEM((2 * blocks, 2 * crows, TILE), BF16),
                pltpu.VMEM((2 * cache_rows, half), BF16),
                pltpu.VMEM((2 * cache_rows, half), BF16),
                pltpu.VMEM((blocks, crows, TILE), F32),
                pltpu.VMEM((blocks, crows, TILE), F32),
                pltpu.VMEM((blocks, crows, TILE), F32),
                pltpu.VMEM((crows, d_model), BF16),
                pltpu.VMEM((2 * crows, TILE // 2), BF16),
                pltpu.VMEM((blocks, crows, HEAD), F32),
                pltpu.VMEM((blocks, 8, HEAD), F32),
                pltpu.VMEM((blocks, 8, HEAD), F32),
                pltpu.VMEM((4, heads, head_dim), F32),
                dma((SLOTS,)), dma((3,)), dma((6,)), dma((8,)), dma((8, 6)),
                dma((blocks,)), dma((blocks,)), dma((blocks,)), dma((blocks,)), dma((blocks,)), dma((blocks,)),
                dma((5,)), dma((5,)), dma((6,)), dma((2,)),
                dma((blocks,)), dma((blocks,)), dma((8,)), dma((8,)),
                dma((blocks,)), dma((blocks,)), dma((2,)), pltpu.SemaphoreType.REGULAR,
            ],
            compiler_params=pltpu.CompilerParams(
                collective_id=0, has_side_effects=True, vmem_limit_bytes=67043328),
        )(cos_t, sin_t, *bias, x_in, flat(cache_k1), flat(cache_v1), flat(cache_k2), flat(cache_v2),
          w_q1, w_k1, w_v1, w_o1, w_gate, w_up, w_down, w_q2, w_k2, w_v2, w_o2)
        g, y2, k1, v1, k2, v2 = out

        def heads_of(a):
            return a.reshape(rows, heads, head_dim)

        def unblock(a):
            return a.transpose(1, 0, 2).reshape(rows, d_model)

        return unblock(g), unblock(y2), heads_of(k1), heads_of(v1), heads_of(k2), heads_of(v2)

    return jax.shard_map(forward, mesh=mesh, in_specs=in_specs, out_specs=out_specs, check_vma=False)
```

```python
import functools
import math

import jax
import jax.numpy as jnp
import numpy as np
from jax import lax
from jax.experimental import pallas as pl
from jax.experimental.pallas import tpu as pltpu
from jax.sharding import PartitionSpec as P

ROPE_THETA = 500000.0
NORM_EPS = 1e-5
MESH = pl.DeviceIdType.MESH
F32 = jnp.float32
BF16 = jnp.bfloat16

TILE = 512
HEAD = 128
PER_BLOCK = TILE // HEAD
SLOTS = 7


def rope_tables(positions, head_dim):
    half_dim = head_dim // 2
    inv_freq = (1.0 / (ROPE_THETA ** (np.arange(half_dim, dtype=np.float32) * np.float32(2.0 / head_dim)))).astype(np.float32)
    angles = positions.astype(np.float32)[:, None] * inv_freq[None, :]
    cos_t, sin_t = np.cos(angles), np.sin(angles)
    return np.concatenate([cos_t, cos_t], axis=1), np.concatenate([-sin_t, sin_t], axis=1)


def body(dims, cos_ref, sin_ref, bq1, bk1, bq2, bk2, x_hbm, ck1, cv1, ck2, cv2, wq1, wk1, wv1, wo1, w_gate, w_up, w_down,
         wq2, wk2, wv2, wo2, g_out, y_out, k1_out, v1_out, k2_out, v2_out,
         wring, nbuf, gbuf, ebuf, pre, kc, vc, o_loc, o_send, o_recv, obuf, opair,
         st_loc, st_send, st_recv, bias32,
         wsem, xsem, csem, c2send, c2recv, qsend, qrecv, osend, orecv, ssend, srecv, dsend, drecv, asem, gsem,
         gxs, gxr, a2send, a2recv, hys, hyr, esem, yfree):
    d_model, ff, rows, cache_rows = dims
    half = d_model // 2
    ffh = ff // 2
    ffc = ff // 3
    third = ffc // 2
    part = third // (TILE // 2)
    blocks = half // TILE
    ffn = ffh // (TILE // 2)
    crows = 2 * rows
    quart = half // 2
    ybuf = nbuf.at[pl.ds(0, rows), :]
    me = lax.axis_index("cp")
    core = lax.rem(me, 2)
    chip = me // 2
    partner = me + 1 - 2 * core
    peer = lax.rem(me + 2, 4)
    diag = 3 - me
    dp = lax.axis_index("dp")
    side_y = 1 - dp
    chip_rows = pl.multiple_of(chip * crows, 16)
    xin = hbuf = gbuf.at[pl.ds(pl.multiple_of(chip * crows, 16), crows), :]
    far_rows = pl.multiple_of((1 - chip) * crows, 16)
    my_cols = pl.multiple_of(core * half, 128)
    my_rows = pl.multiple_of(core * rows, 16)
    other_rows = pl.multiple_of((1 - core) * rows, 16)
    other_cols = pl.multiple_of((1 - core) * half, 128)

    def col(b):
        return pl.multiple_of(core * half + b * TILE, 128)

    attn_tiles = 4 * blocks
    base1 = 0
    base_up = attn_tiles
    base_down = base_up + 2 * part
    base_x = base_down + 3 * blocks
    base2 = base_x + blocks
    qkv2 = 8

    def start_full(w, b, slot):
        pltpu.make_async_copy(w.at[:, pl.ds(col(b), TILE)], wring.at[slot], wsem.at[slot]).start()

    def mlp_cols(tile):
        return pl.ds(pl.multiple_of(core * ffh + tile * (TILE // 2), 128), TILE // 2)

    def shared_tile(n):
        return part + dp * part + n

    def start_mlp(tile, slot):
        at = mlp_cols(tile)
        pltpu.make_async_copy(w_gate.at[:, at], wring.at[slot, :, pl.ds(0, TILE // 2)], wsem.at[slot]).start()
        pltpu.make_async_copy(w_up.at[:, at], wring.at[slot, :, pl.ds(TILE // 2, TILE // 2)], wsem.at[slot]).start()

    def start_down(b, chunk, slot):
        for i in range(2):
            pltpu.make_async_copy(
                w_down.at[pl.ds(pl.multiple_of(i * ffh + chunk * third, 16), third), pl.ds(col(b), TILE)],
                wring.at[slot, pl.ds(i * third, third), :], wsem.at[slot]).start()

    loop_end = 3 * (blocks - 1) + 1

    def attn_segments(base, wq, wk, wv, wo):
        return [
            (base, base + 1, lambda r, slot: start_full(wq, 0, slot), None),
            (base + 1, base + loop_end, lambda r, slot: start_full(wq, r // 3 + 1, slot), 0),
            (base + 1, base + loop_end, lambda r, slot: start_full(wk, r // 3, slot), 1),
            (base + 1, base + loop_end, lambda r, slot: start_full(wv, r // 3, slot), 2),
            (base + loop_end, base + loop_end + 1, lambda r, slot: start_full(wk, blocks - 1, slot), None),
            (base + loop_end + 1, base + loop_end + 2, lambda r, slot: start_full(wv, blocks - 1, slot), None),
            (base + loop_end + 2, base + attn_tiles, lambda r, slot: start_full(wo, r, slot), None),
        ]

    PAIR = TILE // 2
    own2 = core * half + chip * quart

    def start_v2(t, slot):
        @pl.when(t < qkv2 - 2)
        def _():
            pltpu.make_async_copy(wv2.at[:, pl.ds(pl.multiple_of(own2 + (t // 3) * TILE, 128), TILE)], wring.at[slot],
                                  wsem.at[slot]).start()

        @pl.when(t >= qkv2 - 2)
        def _():
            pltpu.make_async_copy(wv2.at[:, pl.ds(pl.multiple_of(own2 + (t // 3) * TILE, 128), PAIR)],
                                  wring.at[slot, :, pl.ds(0, PAIR)], wsem.at[slot]).start()

    def start_qk2(t, slot):
        at = pl.ds(pl.multiple_of(own2 + (t - 1 - t // 3) * PAIR, 128), PAIR)
        pltpu.make_async_copy(wq2.at[:, at], wring.at[slot, :, pl.ds(0, PAIR)], wsem.at[slot]).start()
        pltpu.make_async_copy(wk2.at[:, at], wring.at[slot, :, pl.ds(PAIR, PAIR)], wsem.at[slot]).start()

    other2 = core * half + (1 - chip) * quart

    def start_kv_other(b, slot):
        at = pl.ds(pl.multiple_of(other2 + b * PAIR, 128), PAIR)
        pltpu.make_async_copy(wk2.at[:, at], wring.at[slot, :, pl.ds(0, PAIR)], wsem.at[slot]).start()
        pltpu.make_async_copy(wv2.at[:, at], wring.at[slot, :, pl.ds(PAIR, PAIR)], wsem.at[slot]).start()

    def start_wo2(b, slot):
        for i in range(2):
            pltpu.make_async_copy(
                wo2.at[pl.ds(my_cols, half), pl.ds(pl.multiple_of(b * 2 * TILE + i * TILE, 128), TILE)],
                wring.at[slot, pl.ds(i * half, half), :], wsem.at[slot]).start()

    segments = attn_segments(base1, wq1, wk1, wv1, wo1) + [
        (base_up, base_up + part, start_mlp, None),
        (base_up + part, base_down, lambda r, slot: start_mlp(shared_tile(r), slot), None),
        (base_down, base_down + blocks, lambda r, slot: start_down(r, 0, slot), None),
        (base_down + blocks, base_x, lambda r, slot: start_down(r // 2, 1 + r % 2 if isinstance(r, int) else 1 + lax.rem(r, 2), slot), None),
        (base_x, base2, start_kv_other, None),
        (base2, base2 + qkv2, start_v2, 0),
        (base2, base2 + qkv2, start_qk2, 1),
        (base2, base2 + qkv2, start_qk2, 2),
        (base2 + qkv2, base2 + qkv2 + blocks, start_wo2, None),
    ]

    def start_tile(s, lo, hi):
        slot = lax.rem(s, SLOTS) if not isinstance(s, int) else s % SLOTS
        for a, b, fn, phase in segments:
            if b <= lo or a >= hi:
                continue
            if isinstance(s, int):
                if a <= s < b and (phase is None or (s - a) % 3 == phase):
                    fn(s - a, slot)
                continue
            cond = (s >= a) & (s < b)
            if phase is not None:
                cond = cond & (lax.rem(s - a + 3, 3) == phase)

            @pl.when(cond)
            def _(a=a, fn=fn):
                fn(s - a, slot)

    def wait_tile(s, depth=None):
        slot = lax.rem(s, SLOTS) if not isinstance(s, int) else s % SLOTS
        ref = wring.at[slot] if depth is None else wring.at[slot, pl.ds(0, depth), :]
        pltpu.make_async_copy(ref, ref, wsem.at[slot]).wait()
        return slot

    def remote(src, dst, send, recv, who):
        return pltpu.make_async_remote_copy(src_ref=src, dst_ref=dst, send_sem=send, recv_sem=recv,
                                            device_id={"cp": who}, device_id_type=MESH)

    def remote_y(src, dst, send, recv):
        return pltpu.make_async_remote_copy(src_ref=src, dst_ref=dst, send_sem=send, recv_sem=recv,
                                            device_id={"dp": side_y}, device_id_type=MESH)

    for s in range(2):
        start_tile(s, s, s + 1)

    barrier = pltpu.get_barrier_semaphore()
    for who in (partner, peer, diag):
        pl.semaphore_signal(barrier, inc=1, device_id={"cp": who}, device_id_type=MESH)
    pl.semaphore_signal(barrier, inc=1, device_id={"dp": side_y}, device_id_type=MESH)
    pl.semaphore_wait(barrier, 4)

    x_loc = pltpu.make_async_copy(x_hbm, xin.at[pl.ds(my_rows, rows)], xsem.at[0])
    x_rem = remote(x_hbm, xin.at[pl.ds(my_rows, rows)], xsem.at[1], xsem.at[2], partner)
    x_rem.start()
    x_loc.start()

    def cache_copies(ck, cv):
        crow = pl.ds(pl.multiple_of(core * cache_rows, 16), cache_rows)
        out = []
        for i, (src, dst) in enumerate(((ck, kc), (cv, vc))):
            out.append(pltpu.make_async_copy(src.at[:, pl.ds(my_cols, half)], dst.at[crow], csem.at[3 * i]))
            out.append(remote(src.at[:, pl.ds(other_cols, half)], dst.at[crow], csem.at[3 * i + 1], csem.at[3 * i + 2],
                              partner))
        return out

    cache1 = cache_copies(ck1, cv1)
    for c in cache1:
        c.start()
    for s in range(2, SLOTS):
        start_tile(s, s, s + 1)
    for i, ref in enumerate((bq1, bk1, bq2, bk2)):
        bias32[i] = ref[...].astype(F32)
    x_loc.wait()
    x_rem.wait()

    def biased_rope(vals, bias_row, first_head, table_at, n):
        parts = []
        cos_t, sin_t = cos_ref[table_at, :], sin_ref[table_at, :]
        for i in range(n):
            seg = vals[:, i * HEAD:(i + 1) * HEAD] + bias32[bias_row, pl.ds(first_head + i, 1), :]
            seg = seg.astype(BF16).astype(F32)
            parts.append((seg * cos_t + pltpu.roll(seg, HEAD // 2, 1) * sin_t).astype(BF16))
        return jnp.concatenate(parts, axis=1)

    def norm(src, dst, first, count):
        step = 16

        @pl.loop(0, count // step)
        def _(i):
            at = pl.ds(pl.multiple_of(first + i * step, step), step)
            wide = src[at, :].astype(F32)
            dst[at, :] = (wide * lax.rsqrt(jnp.mean(wide * wide, axis=-1, keepdims=True) + NORM_EPS)).astype(BF16)

    row_i = lax.broadcasted_iota(jnp.int32, (2 * crows, crows), 0)
    col_i = lax.broadcasted_iota(jnp.int32, (2 * crows, crows), 1)
    far_lim = jnp.where(chip == 0, crows, -1)
    scale = HEAD ** -0.5 * math.log2(math.e)

    def attend(b):
        lane = lax.broadcasted_iota(jnp.int32, (2 * crows, HEAD), 1)
        visible = col_i <= jnp.where(row_i < crows, row_i, far_lim)
        stats = jnp.zeros((2 * crows, HEAD), F32)
        dims_t = (((1,), (1,)), ((), ()))
        for i in range(PER_BLOCK):
            at = pl.ds(i * HEAD, HEAD)
            cat = pl.ds(pl.multiple_of(b * TILE + i * HEAD, 128), HEAD)
            q = pre[b, :, at]
            s_old = lax.dot_general(q, kc[:, cat], dims_t, preferred_element_type=F32)
            s_new = lax.dot_general(q, pre[blocks + b, pl.ds(0, crows), at], dims_t, preferred_element_type=F32)
            s_new = jnp.where(visible, s_new, -jnp.inf)
            peak = jnp.maximum(jnp.max(s_old, axis=1, keepdims=True), jnp.max(s_new, axis=1, keepdims=True))
            p_old = jnp.exp2((s_old - peak) * scale)
            p_new = jnp.exp2((s_new - peak) * scale)
            total_p = jnp.sum(p_old, axis=1, keepdims=True) + jnp.sum(p_new, axis=1, keepdims=True)
            acc = jnp.dot(p_old.astype(BF16), vc[:, cat], preferred_element_type=F32)
            acc = acc + jnp.dot(p_new.astype(BF16), pre[blocks + b, pl.ds(crows, crows), at], preferred_element_type=F32)
            o_loc[b, :, at] = acc[:crows]
            o_send[b, :, at] = acc[crows:]
            stats = jnp.where(lane == 2 * i, peak, stats)
            stats = jnp.where(lane == 2 * i + 1, total_p, stats)
        st_loc[b] = stats[:crows]
        st_send[b] = stats[crows:].T[:8, :]

    def q_copy(b):
        return remote(pre.at[b, pl.ds(0, crows), :], pre.at[b, pl.ds(crows, crows), :], qsend.at[b], qrecv.at[b], peer)

    def o_copy(b):
        return remote(o_send.at[b], o_recv.at[b], osend.at[b], orecv.at[b], peer)

    def s_copy(b):
        return remote(st_send.at[b], st_recv.at[b], ssend.at[b], srecv.at[b], peer)

    def head_of(b):
        return core * (half // HEAD) + b * PER_BLOCK

    def attention(layer_in, base, bias_row, caches, k_out, v_out):
        def q_step(b, s, lo, hi):
            slot = wait_tile(s)
            raw = jnp.dot(layer_in[...], wring[slot], preferred_element_type=F32)
            start_tile(s + SLOTS, lo + SLOTS, hi + SLOTS)
            pre[b, pl.ds(0, crows), :] = biased_rope(raw, bias_row, head_of(b), pl.ds(chip_rows, crows), PER_BLOCK)
            q_copy(b).start()

        q_step(0, base, base, base + 1)

        @pl.loop(0, blocks)
        def _(b):
            has_q = (2 * blocks - 3 - b) // (blocks - 1)
            s = base + 1 + 3 * b

            @pl.when(b < blocks - 1)
            def _():
                q_step(b + 1, s, base + 1, base + loop_end)

            s = s + has_q
            slot = wait_tile(s)
            raw = jnp.dot(layer_in[...], wring[slot], preferred_element_type=F32)
            start_tile(s + SLOTS, base + 2 + SLOTS, base + loop_end + 2 + SLOTS)
            pre[blocks + b, pl.ds(0, crows), :] = biased_rope(raw, bias_row + 1, head_of(b), pl.ds(chip_rows, crows), PER_BLOCK)
            s = s + 1
            slot = wait_tile(s)
            vals = jnp.dot(layer_in[...], wring[slot], preferred_element_type=F32).astype(BF16)
            start_tile(s + SLOTS, base + 3 + SLOTS, base + loop_end + 2 + SLOTS)
            pre[blocks + b, pl.ds(crows, crows), :] = vals

            @pl.when(b == 0)
            def _():
                for c in caches:
                    c.wait()

            q_copy(b).wait_recv()
            attend(b)
            for part, dst, k in ((0, k_out, 0), (crows, v_out, 3)):
                pltpu.make_async_copy(pre.at[blocks + b, pl.ds(part + my_rows, rows), :], dst.at[:, pl.ds(col(b), TILE)], asem.at[k]).start()
                remote(pre.at[blocks + b, pl.ds(part + other_rows, rows), :], dst.at[:, pl.ds(col(b), TILE)], asem.at[k + 1],
                       asem.at[k + 2], partner).start()
            o_copy(b).start()
            s_copy(b).start()

        @pl.loop(0, blocks)
        def _(b):
            o_copy(b).wait_recv()
            s_copy(b).wait_recv()
            far = jnp.concatenate([st_recv[b], jnp.zeros((HEAD - 8, HEAD), F32)], axis=0).T
            near = st_loc[b]
            for i in range(PER_BLOCK):
                at = pl.ds(i * HEAD, HEAD)
                m_a, l_a = near[:, 2 * i:2 * i + 1], near[:, 2 * i + 1:2 * i + 2]
                m_b, l_b = far[:, 2 * i:2 * i + 1], far[:, 2 * i + 1:2 * i + 2]
                peak = jnp.maximum(m_a, m_b)
                w_a, w_b = jnp.exp2((m_a - peak) * scale), jnp.exp2((m_b - peak) * scale)
                norm_l = 1.0 / (l_a * w_a + l_b * w_b)
                o = o_loc[b, :, at] * (w_a * norm_l) + o_recv[b, :, at] * (w_b * norm_l)
                obuf[:, pl.ds(pl.multiple_of(core * half + b * TILE + i * HEAD, 128), HEAD)] = o.astype(BF16)
            piece = obuf.at[:, pl.ds(col(b), TILE)]
            remote(piece, piece, dsend.at[0], drecv.at[0], partner).start()

        mine = obuf.at[:, pl.ds(my_cols, half)]
        theirs = obuf.at[:, pl.ds(other_cols, half)]
        remote(mine, theirs, dsend.at[0], drecv.at[0], partner).wait_send()
        remote(mine, theirs, dsend.at[0], drecv.at[0], partner).wait_recv()

        @pl.loop(0, blocks)
        def _(b):
            q_copy(b).wait_send()
            o_copy(b).wait_send()
            s_copy(b).wait_send()

        for dst, k in ((k_out, 0), (v_out, 3)):
            to_me = dst.at[:, pl.ds(my_cols, half)]
            to_me2 = dst.at[:, pl.ds(other_cols, half)]
            pltpu.make_async_copy(to_me, to_me, asem.at[k]).wait()
            remote(to_me, to_me2, asem.at[k + 1], asem.at[k + 2], partner).wait_send()
            remote(to_me, to_me2, asem.at[k + 1], asem.at[k + 2], partner).wait_recv()

    def both_wait(buf, sem, width, my_at, other_at):
        mine = buf.at[:, pl.ds(my_at, width)]
        theirs = buf.at[:, pl.ds(other_at, width)]
        remote(mine, theirs, dsend.at[sem], drecv.at[sem], partner).wait_send()
        remote(mine, theirs, dsend.at[sem], drecv.at[sem], partner).wait_recv()

    attention(xin, base1, 0, cache1, k1_out, v1_out)
    pl.semaphore_signal(yfree, inc=1, device_id={"dp": side_y}, device_id_type=MESH)

    PIECE = TILE // 2

    def cache2_copy(kv, kind, b=None):
        src, dst = ((ck2, kc), (cv2, vc))[kv]
        who, to_core, to_chip = ((None, core, chip), (partner, 1 - core, chip), (peer, core, 1 - chip),
                                 (diag, 1 - core, 1 - chip))[kind]
        off, width, sem = (0, quart, 0) if b is None else (b * PIECE, PIECE, 1 + b)
        side = 0 if kind < 2 else quart
        from_at = pl.ds(pl.multiple_of(to_core * half + to_chip * quart + off, 128), width)
        to = dst.at[pl.ds(pl.multiple_of(core * cache_rows, 16), cache_rows), pl.ds(pl.multiple_of(side + off, 128), width)]
        i = 4 * kv + kind
        if kind == 0:
            return pltpu.make_async_copy(src.at[:, from_at], to, c2send.at[i])
        return remote(src.at[:, from_at], to, c2send.at[i], c2recv.at[i, sem], who)

    def far_cache(b):
        for kv in range(2):
            for kind in (2, 3):
                cache2_copy(kv, kind, b).start()

    for b in range(3):
        far_cache(b)
    for kind in (1, 0):
        for kv in range(2):
            cache2_copy(kv, kind).start()

    pl.semaphore_wait(yfree, 1)

    def h_copy(b):
        return remote_y(hbuf.at[:, pl.ds(col(b), TILE)], pre.at[core * blocks + b, pl.ds(0, crows), :], hys.at[b], hyr.at[b])

    @pl.loop(0, blocks)
    def _(b):
        s = base1 + 3 * blocks + b
        slot = wait_tile(s)
        y = jnp.dot(obuf[...], wring[slot], preferred_element_type=F32).astype(BF16)
        start_tile(s + SLOTS, base1 + 3 * blocks + SLOTS, base_up + SLOTS)
        at = pl.ds(col(b), TILE)
        hbuf[:, at] = (xin[:, at].astype(F32) + y.astype(F32)).astype(BF16)
        h_copy(b).start()
        remote(hbuf.at[:, at], hbuf.at[:, at], dsend.at[1], drecv.at[1], partner).start()

    both_wait(hbuf, 1, half, my_cols, other_cols)
    norm(hbuf, nbuf, 0, crows)

    def glu(both):
        gate = both[:, :TILE // 2].astype(BF16).astype(F32)
        up = both[:, TILE // 2:].astype(BF16).astype(F32)
        return (jax.nn.silu(gate) * up).astype(BF16)

    @pl.loop(0, part)
    def _(n):
        s = base_up + n
        slot = wait_tile(s)
        both = jnp.dot(nbuf[pl.ds(0, crows), :], wring[slot], preferred_element_type=F32)
        start_tile(s + SLOTS, base_up + SLOTS, base_up + part + SLOTS)
        at = mlp_cols(n)
        ebuf[:, at] = glu(both)
        remote(ebuf.at[:, at], ebuf.at[:, at], dsend.at[2], drecv.at[2], partner).start()

    far_h = pre.at[pl.ds(core * blocks, blocks), pl.ds(0, crows), :]
    far_h_other = pre.at[pl.ds((1 - core) * blocks, blocks), pl.ds(0, crows), :]

    @pl.loop(0, blocks)
    def _(b):
        h_copy(b).wait_recv()
        h_copy(b).wait_send()

    remote(far_h, far_h, dsend.at[4], drecv.at[4], partner).start()
    remote(far_h, far_h, dsend.at[4], drecv.at[4], partner).wait_send()
    remote(far_h_other, far_h_other, dsend.at[4], drecv.at[4], partner).wait_recv()

    @pl.loop(0, crows // 16)
    def _(i):
        at = pl.ds(pl.multiple_of(i * 16, 16), 16)
        wide = [pre[j, at, :].astype(F32) for j in range(2 * blocks)]
        square = sum(jnp.sum(w * w, axis=-1, keepdims=True) for w in wide)
        inv = lax.rsqrt(square / d_model + NORM_EPS)
        for j in range(2 * blocks):
            nbuf[pl.ds(pl.multiple_of(crows + i * 16, 16), 16), pl.ds(j * TILE, TILE)] = (wide[j] * inv).astype(BF16)

    def e_return(n):
        return remote_y(pre.at[n, pl.ds(crows, crows), pl.ds(0, TILE // 2)], ebuf.at[:, mlp_cols(shared_tile(n))],
                        esem.at[0], esem.at[1])

    @pl.loop(0, part)
    def _(n):
        s = base_up + part + n
        slot = wait_tile(s)
        both = jnp.dot(nbuf[...], wring[slot], preferred_element_type=F32)
        start_tile(s + SLOTS, base_up + part + SLOTS, base_down + SLOTS)
        at = mlp_cols(shared_tile(n))
        mixed = glu(both)
        ebuf[:, at] = mixed[:crows]
        pre[n, pl.ds(crows, crows), pl.ds(0, TILE // 2)] = mixed[crows:]
        e_return(n).start()
        remote(ebuf.at[:, at], ebuf.at[:, at], dsend.at[2], drecv.at[2], partner).start()

    def returned(to_core):
        return ebuf.at[:, pl.ds(pl.multiple_of(to_core * ffh + (1 + side_y) * third, 128), third)]

    def partner_e_wait():
        some = ebuf.at[:, pl.ds(0, 2 * third)]
        remote(some, some, dsend.at[2], drecv.at[2], partner).wait_send()
        remote(some, some, dsend.at[2], drecv.at[2], partner).wait_recv()

    partner_e_wait()

    def down_dot(slot, chunk):
        out = None
        for i in range(2):
            at = pl.ds(pl.multiple_of(i * ffh + chunk * third, 128), third)
            term = jnp.dot(ebuf[:, at], wring[slot, i * third:(i + 1) * third, :], preferred_element_type=F32)
            out = term if out is None else out + term
        return out

    @pl.loop(0, blocks)
    def _(b):
        @pl.when(b == blocks - 2)
        def _():
            e_all = remote_y(returned(core), returned(core), esem.at[0], esem.at[1])
            e_all.wait_send()
            e_all.wait_recv()
            remote(returned(core), returned(core), dsend.at[1], drecv.at[1], partner).start()

        s = base_down + b
        slot = wait_tile(s, ffc)
        o_loc[b] = down_dot(slot, 0)
        start_tile(s + SLOTS, base_down + SLOTS, base_down + blocks + SLOTS)

    remote(returned(core), returned(core), dsend.at[1], drecv.at[1], partner).wait_send()
    remote(returned(1 - core), returned(1 - core), dsend.at[1], drecv.at[1], partner).wait_recv()

    def g_piece(b, first):
        return gbuf.at[pl.ds(first, crows), pl.ds(col(b), TILE)]

    @pl.loop(0, blocks)
    def _(b):
        at = pl.ds(col(b), TILE)
        down = o_loc[b]
        for k in range(2):
            s = base_down + blocks + 2 * b + k
            slot = wait_tile(s, ffc)
            down = down + down_dot(slot, 1 + k)
            start_tile(s + SLOTS, base_down + blocks + k + SLOTS, base_x - 1 + k + SLOTS)
        gbuf[pl.ds(chip_rows, crows), at] = (hbuf[:, at].astype(F32) + down).astype(BF16)
        piece = g_piece(b, chip_rows)
        remote(piece, piece, gxs.at[b], gxr.at[b], peer).start()
        remote(piece, piece, dsend.at[3], drecv.at[3], partner).start()

    def g_wait(first, sem):
        mine = gbuf.at[pl.ds(first, crows), pl.ds(my_cols, half)]
        theirs = gbuf.at[pl.ds(first, crows), pl.ds(other_cols, half)]
        remote(mine, theirs, dsend.at[sem], drecv.at[sem], partner).wait_send()
        remote(mine, theirs, dsend.at[sem], drecv.at[sem], partner).wait_recv()

    far_cache(3)
    far_cache(4)
    g_wait(chip_rows, 3)
    g_rows = pl.ds(pl.multiple_of(chip_rows + my_rows, 16), rows)
    g_copies = [pltpu.make_async_copy(gbuf.at[g_rows, pl.ds(j * TILE, TILE)], g_out.at[j], gsem.at[0]) for j in range(2 * blocks)]
    for c in g_copies:
        c.start()
    norm(gbuf, nbuf, chip_rows, crows)

    def g_forward(b):
        far = g_piece(b, far_rows)
        remote(far, far, gxs.at[b], gxr.at[b], peer).wait_recv()
        remote(far, far, dsend.at[0], drecv.at[0], partner).start()

    @pl.loop(0, blocks - 1)
    def _(b):
        g_forward(b)

    @pl.loop(0, blocks)
    def _(b):
        s = base_x + b
        slot = wait_tile(s)
        raw = jnp.dot(nbuf[pl.ds(chip_rows, crows), :], wring[slot], preferred_element_type=F32)
        start_tile(s + SLOTS, base_x + SLOTS, base2 + SLOTS)
        k_at = pl.ds(pl.multiple_of(b * TILE, 128), PAIR)
        v_at = pl.ds(pl.multiple_of(b * TILE + PAIR, 128), PAIR)
        ebuf[:, k_at] = biased_rope(raw[:, :PAIR], 3, other2 // HEAD + 2 * b, pl.ds(chip_rows, crows), 2)
        ebuf[:, v_at] = raw[:, PAIR:].astype(BF16)
        to_at = pl.ds(pl.multiple_of(other2 + b * PAIR, 128), PAIR)
        for kv, (at, dst) in enumerate(((k_at, k2_out), (v_at, v2_out))):
            pltpu.make_async_copy(ebuf.at[pl.ds(my_rows, rows), at], dst.at[:, to_at], a2send.at[2 * kv]).start()
            remote(ebuf.at[pl.ds(other_rows, rows), at], dst.at[:, to_at], a2send.at[2 * kv + 1], a2recv.at[kv], partner).start()

    g_forward(blocks - 1)
    g_wait(far_rows, 0)
    norm(gbuf, nbuf, far_rows, crows)

    heads2 = quart // HEAD
    row_2 = lax.broadcasted_iota(jnp.int32, (2 * crows, 2 * crows), 0)
    col_2 = lax.broadcasted_iota(jnp.int32, (2 * crows, 2 * crows), 1)

    def qk_tile(b):
        return b + 1 + b // 2

    def attend2(b):
        t = qk_tile(b)
        vt = 3 * (b // 2)
        dims_t = (((1,), (1,)), ((), ()))
        visible = col_2 <= row_2
        for i in range(2):
            near = pl.ds(pl.multiple_of(b * PAIR + i * HEAD, 128), HEAD)
            far = pl.ds(pl.multiple_of(quart + b * PAIR + i * HEAD, 128), HEAD)
            v_at = pl.ds(pl.multiple_of(lax.rem(b, 2) * PAIR + i * HEAD, 128), HEAD)
            q = pre[t, :, pl.ds(i * HEAD, HEAD)]
            s_a = lax.dot_general(q, kc[:, near], dims_t, preferred_element_type=F32)
            s_b = lax.dot_general(q, kc[:, far], dims_t, preferred_element_type=F32)
            s_n = lax.dot_general(q, pre[t, :, pl.ds(PAIR + i * HEAD, HEAD)], dims_t, preferred_element_type=F32)
            s_n = jnp.where(visible, s_n, -jnp.inf)
            peak = jnp.maximum(jnp.maximum(jnp.max(s_a, axis=1, keepdims=True), jnp.max(s_b, axis=1, keepdims=True)),
                               jnp.max(s_n, axis=1, keepdims=True))
            p_a, p_b, p_n = (jnp.exp2((s - peak) * scale) for s in (s_a, s_b, s_n))
            total_p = (jnp.sum(p_a, axis=1, keepdims=True) + jnp.sum(p_b, axis=1, keepdims=True)
                       + jnp.sum(p_n, axis=1, keepdims=True))
            acc = jnp.dot(p_a.astype(BF16), vc[:, near], preferred_element_type=F32)
            acc = acc + jnp.dot(p_b.astype(BF16), vc[:, far], preferred_element_type=F32)
            acc = acc + jnp.dot(p_n.astype(BF16), pre[vt, :, v_at], preferred_element_type=F32)
            opair[:, pl.ds(i * HEAD, HEAD)] = (acc * (1.0 / total_p)).astype(BF16)

    def o2_piece(b, from_chip):
        return obuf.at[:, pl.ds(pl.multiple_of(from_chip * quart + b * PAIR, 128), PAIR)]

    def o2_far(b):
        return obuf.at[:, pl.ds(pl.multiple_of(half + b * PAIR, 128), PAIR)]

    def o2_copy(b):
        return remote(o2_far(b), o2_piece(b, chip), osend.at[b], orecv.at[b], peer)

    def append2(b):
        to_at = pl.ds(pl.multiple_of(own2 + b * PAIR, 128), PAIR)
        v_at = pl.ds(pl.multiple_of(lax.rem(b, 2) * PAIR, 128), PAIR)
        mine = pl.ds(pl.multiple_of(chip_rows + my_rows, 16), rows)
        others = pl.ds(pl.multiple_of(chip_rows + other_rows, 16), rows)
        for kv, (t, at, dst) in enumerate(((qk_tile(b), pl.ds(PAIR, PAIR), k2_out), (3 * (b // 2), v_at, v2_out))):
            pltpu.make_async_copy(pre.at[t, mine, at], dst.at[:, to_at], a2send.at[2 * kv]).start()
            remote(pre.at[t, others, at], dst.at[:, to_at], a2send.at[2 * kv + 1], a2recv.at[kv], partner).start()

    @pl.loop(0, qkv2)
    def _(t):
        s = base2 + t

        @pl.when(t == qkv2 - 2)
        def _():
            at = wring.at[lax.rem(s, SLOTS), :, pl.ds(0, PAIR)]
            pltpu.make_async_copy(at, at, wsem.at[lax.rem(s, SLOTS)]).wait()

        @pl.when(t != qkv2 - 2)
        def _():
            wait_tile(s)

        raw = jnp.dot(nbuf[...], wring[lax.rem(s, SLOTS)], preferred_element_type=F32)
        start_tile(s + SLOTS, base2 + SLOTS, base2 + qkv2 + SLOTS)

        @pl.when(lax.rem(t, 3) == 0)
        def _():
            pre[t] = raw.astype(BF16)

        @pl.when(lax.rem(t, 3) != 0)
        def _():
            b = t - 1 - t // 3
            head = own2 // HEAD + 2 * b
            all_rows = pl.ds(0, 2 * crows)
            pre[t, :, pl.ds(0, PAIR)] = biased_rope(raw[:, :PAIR], 2, head, all_rows, 2)
            pre[t, :, pl.ds(PAIR, PAIR)] = biased_rope(raw[:, PAIR:], 3, head, all_rows, 2)

            @pl.when(b == 0)
            def _():
                for kv in range(2):
                    for kind in range(2):
                        cache2_copy(kv, kind).wait()

            for kv in range(2):
                for kind in (2, 3):
                    cache2_copy(kv, kind, b).wait_recv()
            attend2(b)
            obuf[:, pl.ds(pl.multiple_of(chip * quart + b * PAIR, 128), PAIR)] = opair[pl.ds(chip_rows, crows), :]
            obuf[:, pl.ds(pl.multiple_of(half + b * PAIR, 128), PAIR)] = opair[pl.ds(far_rows, crows), :]
            o2_copy(b).start()
            append2(b)

    @pl.loop(0, blocks)
    def _(b):
        remote(o2_far(b), o2_piece(b, 1 - chip), osend.at[b], orecv.at[b], peer).wait_recv()

    def y_copy(b):
        return remote(o_send.at[b], o_recv.at[b], qsend.at[b], qrecv.at[b], partner)

    @pl.loop(0, blocks)
    def _(b):
        slot = wait_tile(base2 + qkv2 + b)
        for i in range(2):
            y = jnp.dot(obuf[:, :half], wring[slot, i * half:(i + 1) * half, :], preferred_element_type=F32)
            at = pl.ds(i * rows, rows)
            for j in range(PER_BLOCK):
                lanes = pl.ds(j * HEAD, HEAD)
                st_loc[j] = y[:, j * HEAD:(j + 1) * HEAD]
                o_send[b, at, lanes] = st_loc[j, pl.ds(other_rows, rows), :]
                o_loc[b, at, lanes] = st_loc[j, pl.ds(my_rows, rows), :]
        y_copy(b).start()

    @pl.loop(0, blocks)
    def _(b):
        y_copy(b).wait_recv()
        for i in range(2):
            at = pl.ds(i * rows, rows)
            ybuf[:, pl.ds(pl.multiple_of(b * 2 * TILE + i * TILE, 128), TILE)] = (o_loc[b, at, :] + o_recv[b, at, :]).astype(BF16)

    y_copies = [pltpu.make_async_copy(ybuf.at[:, pl.ds(j * TILE, TILE)], y_out.at[j], gsem.at[1]) for j in range(2 * blocks)]
    for c in y_copies:
        c.start()

    @pl.loop(0, blocks)
    def _(b):
        y_copy(b).wait_send()
        o2_copy(b).wait_send()
        remote(g_piece(b, chip_rows), g_piece(b, chip_rows), gxs.at[b], gxr.at[b], peer).wait_send()

    for kv, dst in enumerate((k2_out, v2_out)):
        ref = dst.at[:, pl.ds(0, half)]
        pltpu.make_async_copy(ref, ref, a2send.at[2 * kv]).wait()
        remote(ref, ref, a2send.at[2 * kv + 1], a2recv.at[kv], partner).wait_send()
        remote(ref, ref, a2send.at[2 * kv + 1], a2recv.at[kv], partner).wait_recv()
        for kind in (2, 3):
            cache2_copy(kv, kind).wait_send()
    for ref, sem in ((y_out, 1), (g_out, 0)):
        pltpu.make_async_copy(ref, ref, gsem.at[sem]).wait()


def solution(mesh):
    rows_spec = P(('dp', 'cp'), None)
    cache_spec = P(('dp', 'cp'), None, None)
    mat_spec = P(None, None)
    vec_spec = P(None)
    layer_specs = (cache_spec, cache_spec, mat_spec, vec_spec, mat_spec, vec_spec, mat_spec, mat_spec)
    in_specs = (rows_spec,) + layer_specs + (mat_spec, mat_spec, mat_spec) + layer_specs
    out_specs = (rows_spec, rows_spec, cache_spec, cache_spec, cache_spec, cache_spec)

    def forward(x_in, cache_k1, cache_v1, w_q1, b_q1, w_k1, b_k1, w_v1, w_o1, w_gate, w_up, w_down, cache_k2, cache_v2, w_q2, b_q2, w_k2, b_k2, w_v2, w_o2):
        rows, d_model = x_in.shape
        cache_rows, heads, head_dim = cache_k1.shape
        ff = w_gate.shape[1]
        half = d_model // 2
        blocks = half // TILE
        crows = 2 * rows
        cos_t, sin_t = rope_tables(4 * cache_rows + np.arange(2 * crows), head_dim)
        bias = [v.reshape(heads, head_dim) for v in (b_q1, b_k1, b_q2, b_k2)]

        def flat(c):
            return c.reshape(cache_rows, d_model)

        any_spec = pl.BlockSpec(memory_space=pl.ANY)
        vmem_spec = pl.BlockSpec(memory_space=pltpu.VMEM)
        blocked = jax.ShapeDtypeStruct((2 * blocks, rows, TILE), BF16)
        row_out = jax.ShapeDtypeStruct((rows, d_model), BF16)
        dma = pltpu.SemaphoreType.DMA
        out = pl.pallas_call(
            functools.partial(body, (d_model, ff, rows, cache_rows)),
            out_shape=[blocked] * 2 + [row_out] * 4,
            in_specs=[vmem_spec] * 6 + [any_spec] * 16,
            out_specs=[any_spec] * 6,
            scratch_shapes=[
                pltpu.VMEM((SLOTS, d_model, TILE), BF16),
                pltpu.VMEM((2 * crows, d_model), BF16),
                pltpu.VMEM((2 * crows, d_model), BF16),
                pltpu.VMEM((crows, ff), BF16),
                pltpu.VMEM((2 * blocks, 2 * crows, TILE), BF16),
                pltpu.VMEM((2 * cache_rows, half), BF16),
                pltpu.VMEM((2 * cache_rows, half), BF16),
                pltpu.VMEM((blocks, crows, TILE), F32),
                pltpu.VMEM((blocks, crows, TILE), F32),
                pltpu.VMEM((blocks, crows, TILE), F32),
                pltpu.VMEM((crows, d_model), BF16),
                pltpu.VMEM((2 * crows, TILE // 2), BF16),
                pltpu.VMEM((blocks, crows, HEAD), F32),
                pltpu.VMEM((blocks, 8, HEAD), F32),
                pltpu.VMEM((blocks, 8, HEAD), F32),
                pltpu.VMEM((4, heads, head_dim), F32),
                dma((SLOTS,)), dma((3,)), dma((6,)), dma((8,)), dma((8, 6)),
                dma((blocks,)), dma((blocks,)), dma((blocks,)), dma((blocks,)), dma((blocks,)), dma((blocks,)),
                dma((5,)), dma((5,)), dma((6,)), dma((2,)),
                dma((blocks,)), dma((blocks,)), dma((4,)), dma((2,)),
                dma((blocks,)), dma((blocks,)), dma((2,)), pltpu.SemaphoreType.REGULAR,
            ],
            compiler_params=pltpu.CompilerParams(
                collective_id=0, has_side_effects=True, vmem_limit_bytes=67043328),
        )(cos_t, sin_t, *bias, x_in, flat(cache_k1), flat(cache_v1), flat(cache_k2), flat(cache_v2),
          w_q1, w_k1, w_v1, w_o1, w_gate, w_up, w_down, w_q2, w_k2, w_v2, w_o2)
        g, y2, k1, v1, k2, v2 = out

        def heads_of(a):
            return a.reshape(rows, heads, head_dim)

        def unblock(a):
            return a.transpose(1, 0, 2).reshape(rows, d_model)

        return unblock(g), unblock(y2), heads_of(k1), heads_of(v1), heads_of(k2), heads_of(v2)

    return jax.shard_map(forward, mesh=mesh, in_specs=in_specs, out_specs=out_specs, check_vma=False)
```

```python
import functools
import math

import jax
import jax.numpy as jnp
import numpy as np
from jax import lax
from jax.experimental import pallas as pl
from jax.experimental.pallas import tpu as pltpu
from jax.sharding import PartitionSpec as P

ROPE_THETA = 500000.0
NORM_EPS = 1e-5
MESH = pl.DeviceIdType.MESH
F32 = jnp.float32
BF16 = jnp.bfloat16

TILE = 512
HEAD = 128
PER_BLOCK = TILE // HEAD
SLOTS = 7


def rope_tables(positions, head_dim):
    half_dim = head_dim // 2
    inv_freq = (1.0 / (ROPE_THETA ** (np.arange(half_dim, dtype=np.float32) * np.float32(2.0 / head_dim)))).astype(np.float32)
    angles = positions.astype(np.float32)[:, None] * inv_freq[None, :]
    cos_t, sin_t = np.cos(angles), np.sin(angles)
    return np.concatenate([cos_t, cos_t], axis=1), np.concatenate([-sin_t, sin_t], axis=1)


def body(dims, cos_ref, sin_ref, bq1, bk1, bq2, bk2, x_hbm, raw_k1, raw_v1, raw_k2, raw_v2, wq1, wk1, wv1, wo1, w_gate, w_up, w_down,
         wq2, wk2, wv2, wo2, g_out, y_out, k1_out, v1_out, k2_out, v2_out, ck1, cv1, ck2, cv2,
         wring, nbuf, gbuf, ebuf, pre, kc, vc, o_loc, o_send, o_recv, obuf, opair,
         st_loc, st_send, st_recv, bias32,
         wsem, xsem, csem, c2send, c2recv, qsend, qrecv, osend, orecv, ssend, srecv, dsend, drecv, asem, gsem,
         gxs, gxr, a2send, a2recv, hys, hyr, esem, yfree, rawbuf, psem, fsem):
    d_model, ff, rows, cache_rows = dims
    half = d_model // 2
    ffh = ff // 2
    ffc = ff // 3
    third = ffc // 2
    part = third // (TILE // 2)
    blocks = half // TILE
    ffn = ffh // (TILE // 2)
    crows = 2 * rows
    quart = half // 2
    ybuf = nbuf.at[pl.ds(0, rows), :]
    me = lax.axis_index("cp")
    core = lax.rem(me, 2)
    chip = me // 2
    partner = me + 1 - 2 * core
    peer = lax.rem(me + 2, 4)
    diag = 3 - me
    dp = lax.axis_index("dp")
    side_y = 1 - dp
    chip_rows = pl.multiple_of(chip * crows, 16)
    xin = hbuf = gbuf.at[pl.ds(pl.multiple_of(chip * crows, 16), crows), :]
    far_rows = pl.multiple_of((1 - chip) * crows, 16)
    my_cols = pl.multiple_of(core * half, 128)
    my_rows = pl.multiple_of(core * rows, 16)
    other_rows = pl.multiple_of((1 - core) * rows, 16)
    other_cols = pl.multiple_of((1 - core) * half, 128)

    def col(b):
        return pl.multiple_of(core * half + b * TILE, 128)

    attn_tiles = 4 * blocks
    base1 = 0
    base_up = attn_tiles
    base_down = base_up + 2 * part
    base_x = base_down + 3 * blocks
    base2 = base_x + blocks
    qkv2 = 8

    def start_full(w, b, slot):
        pltpu.make_async_copy(w.at[:, pl.ds(col(b), TILE)], wring.at[slot], wsem.at[slot]).start()

    def mlp_cols(tile):
        return pl.ds(pl.multiple_of(core * ffh + tile * (TILE // 2), 128), TILE // 2)

    def shared_tile(n):
        return part + dp * part + n

    def start_mlp(tile, slot):
        at = mlp_cols(tile)
        pltpu.make_async_copy(w_gate.at[:, at], wring.at[slot, :, pl.ds(0, TILE // 2)], wsem.at[slot]).start()
        pltpu.make_async_copy(w_up.at[:, at], wring.at[slot, :, pl.ds(TILE // 2, TILE // 2)], wsem.at[slot]).start()

    def start_down(b, chunk, slot):
        for i in range(2):
            pltpu.make_async_copy(
                w_down.at[pl.ds(pl.multiple_of(i * ffh + chunk * third, 16), third), pl.ds(col(b), TILE)],
                wring.at[slot, pl.ds(i * third, third), :], wsem.at[slot]).start()

    loop_end = 3 * (blocks - 1) + 1

    def attn_segments(base, wq, wk, wv, wo):
        return [
            (base, base + 1, lambda r, slot: start_full(wq, 0, slot), None),
            (base + 1, base + loop_end, lambda r, slot: start_full(wq, r // 3 + 1, slot), 0),
            (base + 1, base + loop_end, lambda r, slot: start_full(wk, r // 3, slot), 1),
            (base + 1, base + loop_end, lambda r, slot: start_full(wv, r // 3, slot), 2),
            (base + loop_end, base + loop_end + 1, lambda r, slot: start_full(wk, blocks - 1, slot), None),
            (base + loop_end + 1, base + loop_end + 2, lambda r, slot: start_full(wv, blocks - 1, slot), None),
            (base + loop_end + 2, base + attn_tiles, lambda r, slot: start_full(wo, r, slot), None),
        ]

    PAIR = TILE // 2
    own2 = core * half + chip * quart

    def start_v2(t, slot):
        @pl.when(t < qkv2 - 2)
        def _():
            pltpu.make_async_copy(wv2.at[:, pl.ds(pl.multiple_of(own2 + (t // 3) * TILE, 128), TILE)], wring.at[slot],
                                  wsem.at[slot]).start()

        @pl.when(t >= qkv2 - 2)
        def _():
            pltpu.make_async_copy(wv2.at[:, pl.ds(pl.multiple_of(own2 + (t // 3) * TILE, 128), PAIR)],
                                  wring.at[slot, :, pl.ds(0, PAIR)], wsem.at[slot]).start()

    def start_qk2(t, slot):
        at = pl.ds(pl.multiple_of(own2 + (t - 1 - t // 3) * PAIR, 128), PAIR)
        pltpu.make_async_copy(wq2.at[:, at], wring.at[slot, :, pl.ds(0, PAIR)], wsem.at[slot]).start()
        pltpu.make_async_copy(wk2.at[:, at], wring.at[slot, :, pl.ds(PAIR, PAIR)], wsem.at[slot]).start()

    other2 = core * half + (1 - chip) * quart

    def start_kv_other(b, slot):
        at = pl.ds(pl.multiple_of(other2 + b * PAIR, 128), PAIR)
        pltpu.make_async_copy(wk2.at[:, at], wring.at[slot, :, pl.ds(0, PAIR)], wsem.at[slot]).start()
        pltpu.make_async_copy(wv2.at[:, at], wring.at[slot, :, pl.ds(PAIR, PAIR)], wsem.at[slot]).start()

    def start_wo2(b, slot):
        for i in range(2):
            pltpu.make_async_copy(
                wo2.at[pl.ds(my_cols, half), pl.ds(pl.multiple_of(b * 2 * TILE + i * TILE, 128), TILE)],
                wring.at[slot, pl.ds(i * half, half), :], wsem.at[slot]).start()

    segments = attn_segments(base1, wq1, wk1, wv1, wo1) + [
        (base_up, base_up + part, start_mlp, None),
        (base_up + part, base_down, lambda r, slot: start_mlp(shared_tile(r), slot), None),
        (base_down, base_down + blocks, lambda r, slot: start_down(r, 0, slot), None),
        (base_down + blocks, base_x, lambda r, slot: start_down(r // 2, 1 + r % 2 if isinstance(r, int) else 1 + lax.rem(r, 2), slot), None),
        (base_x, base2, start_kv_other, None),
        (base2, base2 + qkv2, start_v2, 0),
        (base2, base2 + qkv2, start_qk2, 1),
        (base2, base2 + qkv2, start_qk2, 2),
        (base2 + qkv2, base2 + qkv2 + blocks, start_wo2, None),
    ]

    def start_tile(s, lo, hi):
        slot = lax.rem(s, SLOTS) if not isinstance(s, int) else s % SLOTS
        for a, b, fn, phase in segments:
            if b <= lo or a >= hi:
                continue
            if isinstance(s, int):
                if a <= s < b and (phase is None or (s - a) % 3 == phase):
                    fn(s - a, slot)
                continue
            cond = (s >= a) & (s < b)
            if phase is not None:
                cond = cond & (lax.rem(s - a + 3, 3) == phase)

            @pl.when(cond)
            def _(a=a, fn=fn):
                fn(s - a, slot)

    def wait_tile(s, depth=None):
        slot = lax.rem(s, SLOTS) if not isinstance(s, int) else s % SLOTS
        ref = wring.at[slot] if depth is None else wring.at[slot, pl.ds(0, depth), :]
        pltpu.make_async_copy(ref, ref, wsem.at[slot]).wait()
        return slot

    def remote(src, dst, send, recv, who):
        return pltpu.make_async_remote_copy(src_ref=src, dst_ref=dst, send_sem=send, recv_sem=recv,
                                            device_id={"cp": who}, device_id_type=MESH)

    def remote_y(src, dst, send, recv):
        return pltpu.make_async_remote_copy(src_ref=src, dst_ref=dst, send_sem=send, recv_sem=recv,
                                            device_id={"dp": side_y}, device_id_type=MESH)

    HEADS8 = 8
    WIDE = HEADS8 * HEAD
    groups = d_model // WIDE

    def raw_copy(raw, j, slot):
        return pltpu.make_async_copy(raw.at[:, pl.ds(pl.multiple_of(j * HEADS8, HEADS8), HEADS8), :], rawbuf.at[slot],
                                     psem.at[slot])

    def flat_wait(flat, slot):
        ref = flat.at[:, pl.ds(0, WIDE)]
        pltpu.make_async_copy(ref, ref, fsem.at[slot]).wait()

    def flatten_heads(flat, j, slot):
        for i in range(cache_rows // crows):
            at = pl.ds((slot * 2 + i) * WIDE, WIDE)
            ebuf[:, at] = pltpu.einshape("thd->t(hd)", rawbuf[slot, i * crows:(i + 1) * crows])
            pltpu.make_async_copy(ebuf.at[:, at], flat.at[pl.ds(i * crows, crows), pl.ds(pl.multiple_of(j * WIDE, 128), WIDE)],
                                  fsem.at[slot]).start()

    layer1 = ((raw_k1, ck1), (raw_v1, cv1))
    layer2 = ((raw_k2, ck2), (raw_v2, cv2))
    for slot in range(2):
        raw_copy(layer1[slot][0], 0, slot).start()
    for s in range(2):
        start_tile(s, s, s + 1)

    barrier = pltpu.get_barrier_semaphore()
    for who in (partner, peer, diag):
        pl.semaphore_signal(barrier, inc=1, device_id={"cp": who}, device_id_type=MESH)
    pl.semaphore_signal(barrier, inc=1, device_id={"dp": side_y}, device_id_type=MESH)
    pl.semaphore_wait(barrier, 4)

    x_loc = pltpu.make_async_copy(x_hbm, xin.at[pl.ds(my_rows, rows)], xsem.at[0])
    x_rem = remote(x_hbm, xin.at[pl.ds(my_rows, rows)], xsem.at[1], xsem.at[2], partner)
    x_rem.start()
    x_loc.start()

    def cache_copies(ck, cv):
        crow = pl.ds(pl.multiple_of(core * cache_rows, 16), cache_rows)
        out = []
        for i, (src, dst) in enumerate(((ck, kc), (cv, vc))):
            out.append(pltpu.make_async_copy(src.at[:, pl.ds(my_cols, half)], dst.at[crow], csem.at[3 * i]))
            out.append(remote(src.at[:, pl.ds(other_cols, half)], dst.at[crow], csem.at[3 * i + 1], csem.at[3 * i + 2],
                              partner))
        return out

    @pl.loop(0, groups)
    def _(j):
        for slot, (raw, flat) in enumerate(layer1):
            raw_copy(raw, j, slot).wait()

            @pl.when(j > 0)
            def _():
                flat_wait(flat, slot)

            flatten_heads(flat, j, slot)

            @pl.when(j < groups - 1)
            def _():
                raw_copy(raw, j + 1, slot).start()

    for slot, (raw, flat) in enumerate(layer1):
        flat_wait(flat, slot)
        raw_copy(layer2[slot][0], 0, slot).start()
    cache1 = cache_copies(ck1, cv1)
    for c in cache1:
        c.start()
    for s in range(2, SLOTS):
        start_tile(s, s, s + 1)
    for i, ref in enumerate((bq1, bk1, bq2, bk2)):
        bias32[i] = ref[...].astype(F32)
    x_loc.wait()
    x_rem.wait()

    def biased_rope(vals, bias_row, first_head, table_at, n):
        parts = []
        cos_t, sin_t = cos_ref[table_at, :], sin_ref[table_at, :]
        for i in range(n):
            seg = vals[:, i * HEAD:(i + 1) * HEAD] + bias32[bias_row, pl.ds(first_head + i, 1), :]
            seg = seg.astype(BF16).astype(F32)
            parts.append((seg * cos_t + pltpu.roll(seg, HEAD // 2, 1) * sin_t).astype(BF16))
        return jnp.concatenate(parts, axis=1)

    def norm(src, dst, first, count):
        step = 16

        @pl.loop(0, count // step)
        def _(i):
            at = pl.ds(pl.multiple_of(first + i * step, step), step)
            wide = src[at, :].astype(F32)
            dst[at, :] = (wide * lax.rsqrt(jnp.mean(wide * wide, axis=-1, keepdims=True) + NORM_EPS)).astype(BF16)

    row_i = lax.broadcasted_iota(jnp.int32, (2 * crows, crows), 0)
    col_i = lax.broadcasted_iota(jnp.int32, (2 * crows, crows), 1)
    far_lim = jnp.where(chip == 0, crows, -1)
    scale = HEAD ** -0.5 * math.log2(math.e)

    def attend(b):
        lane = lax.broadcasted_iota(jnp.int32, (2 * crows, HEAD), 1)
        visible = col_i <= jnp.where(row_i < crows, row_i, far_lim)
        stats = jnp.zeros((2 * crows, HEAD), F32)
        dims_t = (((1,), (1,)), ((), ()))
        for i in range(PER_BLOCK):
            at = pl.ds(i * HEAD, HEAD)
            cat = pl.ds(pl.multiple_of(b * TILE + i * HEAD, 128), HEAD)
            q = pre[b, :, at]
            s_old = lax.dot_general(q, kc[:, cat], dims_t, preferred_element_type=F32)
            s_new = lax.dot_general(q, pre[blocks + b, pl.ds(0, crows), at], dims_t, preferred_element_type=F32)
            s_new = jnp.where(visible, s_new, -jnp.inf)
            peak = jnp.maximum(jnp.max(s_old, axis=1, keepdims=True), jnp.max(s_new, axis=1, keepdims=True))
            p_old = jnp.exp2((s_old - peak) * scale)
            p_new = jnp.exp2((s_new - peak) * scale)
            total_p = jnp.sum(p_old, axis=1, keepdims=True) + jnp.sum(p_new, axis=1, keepdims=True)
            acc = jnp.dot(p_old.astype(BF16), vc[:, cat], preferred_element_type=F32)
            acc = acc + jnp.dot(p_new.astype(BF16), pre[blocks + b, pl.ds(crows, crows), at], preferred_element_type=F32)
            o_loc[b, :, at] = acc[:crows]
            o_send[b, :, at] = acc[crows:]
            stats = jnp.where(lane == 2 * i, peak, stats)
            stats = jnp.where(lane == 2 * i + 1, total_p, stats)
        st_loc[b] = stats[:crows]
        st_send[b] = stats[crows:].T[:8, :]

    def q_copy(b):
        return remote(pre.at[b, pl.ds(0, crows), :], pre.at[b, pl.ds(crows, crows), :], qsend.at[b], qrecv.at[b], peer)

    def o_copy(b):
        return remote(o_send.at[b], o_recv.at[b], osend.at[b], orecv.at[b], peer)

    def s_copy(b):
        return remote(st_send.at[b], st_recv.at[b], ssend.at[b], srecv.at[b], peer)

    def head_of(b):
        return core * (half // HEAD) + b * PER_BLOCK

    def attention(layer_in, base, bias_row, caches, k_out, v_out):
        def q_step(b, s, lo, hi):
            slot = wait_tile(s)
            raw = jnp.dot(layer_in[...], wring[slot], preferred_element_type=F32)
            start_tile(s + SLOTS, lo + SLOTS, hi + SLOTS)
            pre[b, pl.ds(0, crows), :] = biased_rope(raw, bias_row, head_of(b), pl.ds(chip_rows, crows), PER_BLOCK)
            q_copy(b).start()

        q_step(0, base, base, base + 1)

        @pl.loop(0, blocks)
        def _(b):
            has_q = (2 * blocks - 3 - b) // (blocks - 1)
            s = base + 1 + 3 * b

            @pl.when(b < blocks - 1)
            def _():
                q_step(b + 1, s, base + 1, base + loop_end)

            s = s + has_q
            slot = wait_tile(s)
            raw = jnp.dot(layer_in[...], wring[slot], preferred_element_type=F32)
            start_tile(s + SLOTS, base + 2 + SLOTS, base + loop_end + 2 + SLOTS)
            pre[blocks + b, pl.ds(0, crows), :] = biased_rope(raw, bias_row + 1, head_of(b), pl.ds(chip_rows, crows), PER_BLOCK)
            s = s + 1
            slot = wait_tile(s)
            vals = jnp.dot(layer_in[...], wring[slot], preferred_element_type=F32).astype(BF16)
            start_tile(s + SLOTS, base + 3 + SLOTS, base + loop_end + 2 + SLOTS)
            pre[blocks + b, pl.ds(crows, crows), :] = vals

            @pl.when(b == 0)
            def _():
                for c in caches:
                    c.wait()

            q_copy(b).wait_recv()
            attend(b)
            for part, dst, k in ((0, k_out, 0), (crows, v_out, 3)):
                pltpu.make_async_copy(pre.at[blocks + b, pl.ds(part + my_rows, rows), :], dst.at[:, pl.ds(col(b), TILE)], asem.at[k]).start()
                remote(pre.at[blocks + b, pl.ds(part + other_rows, rows), :], dst.at[:, pl.ds(col(b), TILE)], asem.at[k + 1],
                       asem.at[k + 2], partner).start()
            o_copy(b).start()
            s_copy(b).start()
            for slot, (raw, flat) in enumerate(layer2):
                raw_copy(raw, b, slot).wait()

                @pl.when(b > 0)
                def _():
                    flat_wait(flat, slot)

                flatten_heads(flat, b, slot)

                @pl.when(b < blocks - 1)
                def _():
                    raw_copy(raw, b + 1, slot).start()

        for slot, (raw, flat) in enumerate(layer2):
            flat_wait(flat, slot)

        @pl.loop(0, blocks)
        def _(b):
            o_copy(b).wait_recv()
            s_copy(b).wait_recv()
            far = jnp.concatenate([st_recv[b], jnp.zeros((HEAD - 8, HEAD), F32)], axis=0).T
            near = st_loc[b]
            for i in range(PER_BLOCK):
                at = pl.ds(i * HEAD, HEAD)
                m_a, l_a = near[:, 2 * i:2 * i + 1], near[:, 2 * i + 1:2 * i + 2]
                m_b, l_b = far[:, 2 * i:2 * i + 1], far[:, 2 * i + 1:2 * i + 2]
                peak = jnp.maximum(m_a, m_b)
                w_a, w_b = jnp.exp2((m_a - peak) * scale), jnp.exp2((m_b - peak) * scale)
                norm_l = 1.0 / (l_a * w_a + l_b * w_b)
                o = o_loc[b, :, at] * (w_a * norm_l) + o_recv[b, :, at] * (w_b * norm_l)
                obuf[:, pl.ds(pl.multiple_of(core * half + b * TILE + i * HEAD, 128), HEAD)] = o.astype(BF16)
            piece = obuf.at[:, pl.ds(col(b), TILE)]
            remote(piece, piece, dsend.at[0], drecv.at[0], partner).start()

        mine = obuf.at[:, pl.ds(my_cols, half)]
        theirs = obuf.at[:, pl.ds(other_cols, half)]
        remote(mine, theirs, dsend.at[0], drecv.at[0], partner).wait_send()
        remote(mine, theirs, dsend.at[0], drecv.at[0], partner).wait_recv()

        @pl.loop(0, blocks)
        def _(b):
            q_copy(b).wait_send()
            o_copy(b).wait_send()
            s_copy(b).wait_send()

        for dst, k in ((k_out, 0), (v_out, 3)):
            to_me = dst.at[:, pl.ds(my_cols, half)]
            to_me2 = dst.at[:, pl.ds(other_cols, half)]
            pltpu.make_async_copy(to_me, to_me, asem.at[k]).wait()
            remote(to_me, to_me2, asem.at[k + 1], asem.at[k + 2], partner).wait_send()
            remote(to_me, to_me2, asem.at[k + 1], asem.at[k + 2], partner).wait_recv()

    def both_wait(buf, sem, width, my_at, other_at):
        mine = buf.at[:, pl.ds(my_at, width)]
        theirs = buf.at[:, pl.ds(other_at, width)]
        remote(mine, theirs, dsend.at[sem], drecv.at[sem], partner).wait_send()
        remote(mine, theirs, dsend.at[sem], drecv.at[sem], partner).wait_recv()

    attention(xin, base1, 0, cache1, k1_out, v1_out)
    pl.semaphore_signal(yfree, inc=1, device_id={"dp": side_y}, device_id_type=MESH)

    PIECE = TILE // 2

    def cache2_copy(kv, kind, b=None):
        src, dst = ((ck2, kc), (cv2, vc))[kv]
        who, to_core, to_chip = ((None, core, chip), (partner, 1 - core, chip), (peer, core, 1 - chip),
                                 (diag, 1 - core, 1 - chip))[kind]
        off, width, sem = (0, quart, 0) if b is None else (b * PIECE, PIECE, 1 + b)
        side = 0 if kind < 2 else quart
        from_at = pl.ds(pl.multiple_of(to_core * half + to_chip * quart + off, 128), width)
        to = dst.at[pl.ds(pl.multiple_of(core * cache_rows, 16), cache_rows), pl.ds(pl.multiple_of(side + off, 128), width)]
        i = 4 * kv + kind
        if kind == 0:
            return pltpu.make_async_copy(src.at[:, from_at], to, c2send.at[i])
        return remote(src.at[:, from_at], to, c2send.at[i], c2recv.at[i, sem], who)

    def far_cache(b):
        for kv in range(2):
            for kind in (2, 3):
                cache2_copy(kv, kind, b).start()

    for b in range(3):
        far_cache(b)
    for kind in (1, 0):
        for kv in range(2):
            cache2_copy(kv, kind).start()

    pl.semaphore_wait(yfree, 1)

    def h_copy(b):
        return remote_y(hbuf.at[:, pl.ds(col(b), TILE)], pre.at[core * blocks + b, pl.ds(0, crows), :], hys.at[b], hyr.at[b])

    @pl.loop(0, blocks)
    def _(b):
        s = base1 + 3 * blocks + b
        slot = wait_tile(s)
        y = jnp.dot(obuf[...], wring[slot], preferred_element_type=F32).astype(BF16)
        start_tile(s + SLOTS, base1 + 3 * blocks + SLOTS, base_up + SLOTS)
        at = pl.ds(col(b), TILE)
        hbuf[:, at] = (xin[:, at].astype(F32) + y.astype(F32)).astype(BF16)
        h_copy(b).start()
        remote(hbuf.at[:, at], hbuf.at[:, at], dsend.at[1], drecv.at[1], partner).start()

    both_wait(hbuf, 1, half, my_cols, other_cols)
    norm(hbuf, nbuf, 0, crows)

    def glu(both):
        gate = both[:, :TILE // 2].astype(BF16).astype(F32)
        up = both[:, TILE // 2:].astype(BF16).astype(F32)
        return (jax.nn.silu(gate) * up).astype(BF16)

    @pl.loop(0, part)
    def _(n):
        s = base_up + n
        slot = wait_tile(s)
        both = jnp.dot(nbuf[pl.ds(0, crows), :], wring[slot], preferred_element_type=F32)
        start_tile(s + SLOTS, base_up + SLOTS, base_up + part + SLOTS)
        at = mlp_cols(n)
        ebuf[:, at] = glu(both)
        remote(ebuf.at[:, at], ebuf.at[:, at], dsend.at[2], drecv.at[2], partner).start()

    far_h = pre.at[pl.ds(core * blocks, blocks), pl.ds(0, crows), :]
    far_h_other = pre.at[pl.ds((1 - core) * blocks, blocks), pl.ds(0, crows), :]

    @pl.loop(0, blocks)
    def _(b):
        h_copy(b).wait_recv()
        h_copy(b).wait_send()

    remote(far_h, far_h, dsend.at[4], drecv.at[4], partner).start()
    remote(far_h, far_h, dsend.at[4], drecv.at[4], partner).wait_send()
    remote(far_h_other, far_h_other, dsend.at[4], drecv.at[4], partner).wait_recv()

    @pl.loop(0, crows // 16)
    def _(i):
        at = pl.ds(pl.multiple_of(i * 16, 16), 16)
        wide = [pre[j, at, :].astype(F32) for j in range(2 * blocks)]
        square = sum(jnp.sum(w * w, axis=-1, keepdims=True) for w in wide)
        inv = lax.rsqrt(square / d_model + NORM_EPS)
        for j in range(2 * blocks):
            nbuf[pl.ds(pl.multiple_of(crows + i * 16, 16), 16), pl.ds(j * TILE, TILE)] = (wide[j] * inv).astype(BF16)

    def e_return(n):
        return remote_y(pre.at[n, pl.ds(crows, crows), pl.ds(0, TILE // 2)], ebuf.at[:, mlp_cols(shared_tile(n))],
                        esem.at[0], esem.at[1])

    @pl.loop(0, part)
    def _(n):
        s = base_up + part + n
        slot = wait_tile(s)
        both = jnp.dot(nbuf[...], wring[slot], preferred_element_type=F32)
        start_tile(s + SLOTS, base_up + part + SLOTS, base_down + SLOTS)
        at = mlp_cols(shared_tile(n))
        mixed = glu(both)
        ebuf[:, at] = mixed[:crows]
        pre[n, pl.ds(crows, crows), pl.ds(0, TILE // 2)] = mixed[crows:]
        e_return(n).start()
        remote(ebuf.at[:, at], ebuf.at[:, at], dsend.at[2], drecv.at[2], partner).start()

    def returned(to_core):
        return ebuf.at[:, pl.ds(pl.multiple_of(to_core * ffh + (1 + side_y) * third, 128), third)]

    def partner_e_wait():
        some = ebuf.at[:, pl.ds(0, 2 * third)]
        remote(some, some, dsend.at[2], drecv.at[2], partner).wait_send()
        remote(some, some, dsend.at[2], drecv.at[2], partner).wait_recv()

    partner_e_wait()

    def down_dot(slot, chunk):
        out = None
        for i in range(2):
            at = pl.ds(pl.multiple_of(i * ffh + chunk * third, 128), third)
            term = jnp.dot(ebuf[:, at], wring[slot, i * third:(i + 1) * third, :], preferred_element_type=F32)
            out = term if out is None else out + term
        return out

    @pl.loop(0, blocks)
    def _(b):
        @pl.when(b == blocks - 2)
        def _():
            e_all = remote_y(returned(core), returned(core), esem.at[0], esem.at[1])
            e_all.wait_send()
            e_all.wait_recv()
            remote(returned(core), returned(core), dsend.at[1], drecv.at[1], partner).start()

        s = base_down + b
        slot = wait_tile(s, ffc)
        o_loc[b] = down_dot(slot, 0)
        start_tile(s + SLOTS, base_down + SLOTS, base_down + blocks + SLOTS)

    remote(returned(core), returned(core), dsend.at[1], drecv.at[1], partner).wait_send()
    remote(returned(1 - core), returned(1 - core), dsend.at[1], drecv.at[1], partner).wait_recv()

    def g_piece(b, first):
        return gbuf.at[pl.ds(first, crows), pl.ds(col(b), TILE)]

    @pl.loop(0, blocks)
    def _(b):
        at = pl.ds(col(b), TILE)
        down = o_loc[b]
        for k in range(2):
            s = base_down + blocks + 2 * b + k
            slot = wait_tile(s, ffc)
            down = down + down_dot(slot, 1 + k)
            start_tile(s + SLOTS, base_down + blocks + k + SLOTS, base_x - 1 + k + SLOTS)
        gbuf[pl.ds(chip_rows, crows), at] = (hbuf[:, at].astype(F32) + down).astype(BF16)
        piece = g_piece(b, chip_rows)
        remote(piece, piece, gxs.at[b], gxr.at[b], peer).start()
        remote(piece, piece, dsend.at[3], drecv.at[3], partner).start()

    def g_wait(first, sem):
        mine = gbuf.at[pl.ds(first, crows), pl.ds(my_cols, half)]
        theirs = gbuf.at[pl.ds(first, crows), pl.ds(other_cols, half)]
        remote(mine, theirs, dsend.at[sem], drecv.at[sem], partner).wait_send()
        remote(mine, theirs, dsend.at[sem], drecv.at[sem], partner).wait_recv()

    far_cache(3)
    far_cache(4)
    g_wait(chip_rows, 3)
    g_rows = pl.ds(pl.multiple_of(chip_rows + my_rows, 16), rows)
    g_copies = [pltpu.make_async_copy(gbuf.at[g_rows, :], g_out, gsem.at[0])]
    for c in g_copies:
        c.start()
    norm(gbuf, nbuf, chip_rows, crows)

    def g_forward(b):
        far = g_piece(b, far_rows)
        remote(far, far, gxs.at[b], gxr.at[b], peer).wait_recv()
        remote(far, far, dsend.at[0], drecv.at[0], partner).start()

    @pl.loop(0, blocks - 1)
    def _(b):
        g_forward(b)

    @pl.loop(0, blocks)
    def _(b):
        s = base_x + b
        slot = wait_tile(s)
        raw = jnp.dot(nbuf[pl.ds(chip_rows, crows), :], wring[slot], preferred_element_type=F32)
        start_tile(s + SLOTS, base_x + SLOTS, base2 + SLOTS)
        k_at = pl.ds(pl.multiple_of(b * TILE, 128), PAIR)
        v_at = pl.ds(pl.multiple_of(b * TILE + PAIR, 128), PAIR)
        ebuf[:, k_at] = biased_rope(raw[:, :PAIR], 3, other2 // HEAD + 2 * b, pl.ds(chip_rows, crows), 2)
        ebuf[:, v_at] = raw[:, PAIR:].astype(BF16)
        to_at = pl.ds(pl.multiple_of(other2 + b * PAIR, 128), PAIR)
        for kv, (at, dst) in enumerate(((k_at, k2_out), (v_at, v2_out))):
            pltpu.make_async_copy(ebuf.at[pl.ds(my_rows, rows), at], dst.at[:, to_at], a2send.at[2 * kv]).start()
            remote(ebuf.at[pl.ds(other_rows, rows), at], dst.at[:, to_at], a2send.at[2 * kv + 1], a2recv.at[kv], partner).start()

    g_forward(blocks - 1)
    g_wait(far_rows, 0)
    norm(gbuf, nbuf, far_rows, crows)

    heads2 = quart // HEAD
    row_2 = lax.broadcasted_iota(jnp.int32, (2 * crows, 2 * crows), 0)
    col_2 = lax.broadcasted_iota(jnp.int32, (2 * crows, 2 * crows), 1)

    def qk_tile(b):
        return b + 1 + b // 2

    def attend2(b):
        t = qk_tile(b)
        vt = 3 * (b // 2)
        dims_t = (((1,), (1,)), ((), ()))
        visible = col_2 <= row_2
        for i in range(2):
            near = pl.ds(pl.multiple_of(b * PAIR + i * HEAD, 128), HEAD)
            far = pl.ds(pl.multiple_of(quart + b * PAIR + i * HEAD, 128), HEAD)
            v_at = pl.ds(pl.multiple_of(lax.rem(b, 2) * PAIR + i * HEAD, 128), HEAD)
            q = pre[t, :, pl.ds(i * HEAD, HEAD)]
            s_a = lax.dot_general(q, kc[:, near], dims_t, preferred_element_type=F32)
            s_b = lax.dot_general(q, kc[:, far], dims_t, preferred_element_type=F32)
            s_n = lax.dot_general(q, pre[t, :, pl.ds(PAIR + i * HEAD, HEAD)], dims_t, preferred_element_type=F32)
            s_n = jnp.where(visible, s_n, -jnp.inf)
            peak = jnp.maximum(jnp.maximum(jnp.max(s_a, axis=1, keepdims=True), jnp.max(s_b, axis=1, keepdims=True)),
                               jnp.max(s_n, axis=1, keepdims=True))
            p_a, p_b, p_n = (jnp.exp2((s - peak) * scale) for s in (s_a, s_b, s_n))
            total_p = (jnp.sum(p_a, axis=1, keepdims=True) + jnp.sum(p_b, axis=1, keepdims=True)
                       + jnp.sum(p_n, axis=1, keepdims=True))
            acc = jnp.dot(p_a.astype(BF16), vc[:, near], preferred_element_type=F32)
            acc = acc + jnp.dot(p_b.astype(BF16), vc[:, far], preferred_element_type=F32)
            acc = acc + jnp.dot(p_n.astype(BF16), pre[vt, :, v_at], preferred_element_type=F32)
            opair[:, pl.ds(i * HEAD, HEAD)] = (acc * (1.0 / total_p)).astype(BF16)

    def o2_piece(b, from_chip):
        return obuf.at[:, pl.ds(pl.multiple_of(from_chip * quart + b * PAIR, 128), PAIR)]

    def o2_far(b):
        return obuf.at[:, pl.ds(pl.multiple_of(half + b * PAIR, 128), PAIR)]

    def o2_copy(b):
        return remote(o2_far(b), o2_piece(b, chip), osend.at[b], orecv.at[b], peer)

    def append2(b):
        to_at = pl.ds(pl.multiple_of(own2 + b * PAIR, 128), PAIR)
        v_at = pl.ds(pl.multiple_of(lax.rem(b, 2) * PAIR, 128), PAIR)
        mine = pl.ds(pl.multiple_of(chip_rows + my_rows, 16), rows)
        others = pl.ds(pl.multiple_of(chip_rows + other_rows, 16), rows)
        for kv, (t, at, dst) in enumerate(((qk_tile(b), pl.ds(PAIR, PAIR), k2_out), (3 * (b // 2), v_at, v2_out))):
            pltpu.make_async_copy(pre.at[t, mine, at], dst.at[:, to_at], a2send.at[2 * kv]).start()
            remote(pre.at[t, others, at], dst.at[:, to_at], a2send.at[2 * kv + 1], a2recv.at[kv], partner).start()

    @pl.loop(0, qkv2)
    def _(t):
        s = base2 + t

        @pl.when(t == qkv2 - 2)
        def _():
            at = wring.at[lax.rem(s, SLOTS), :, pl.ds(0, PAIR)]
            pltpu.make_async_copy(at, at, wsem.at[lax.rem(s, SLOTS)]).wait()

        @pl.when(t != qkv2 - 2)
        def _():
            wait_tile(s)

        raw = jnp.dot(nbuf[...], wring[lax.rem(s, SLOTS)], preferred_element_type=F32)
        start_tile(s + SLOTS, base2 + SLOTS, base2 + qkv2 + SLOTS)

        @pl.when(lax.rem(t, 3) == 0)
        def _():
            pre[t] = raw.astype(BF16)

        @pl.when(lax.rem(t, 3) != 0)
        def _():
            b = t - 1 - t // 3
            head = own2 // HEAD + 2 * b
            all_rows = pl.ds(0, 2 * crows)
            pre[t, :, pl.ds(0, PAIR)] = biased_rope(raw[:, :PAIR], 2, head, all_rows, 2)
            pre[t, :, pl.ds(PAIR, PAIR)] = biased_rope(raw[:, PAIR:], 3, head, all_rows, 2)

            @pl.when(b == 0)
            def _():
                for kv in range(2):
                    for kind in range(2):
                        cache2_copy(kv, kind).wait()

            for kv in range(2):
                for kind in (2, 3):
                    cache2_copy(kv, kind, b).wait_recv()
            attend2(b)
            obuf[:, pl.ds(pl.multiple_of(chip * quart + b * PAIR, 128), PAIR)] = opair[pl.ds(chip_rows, crows), :]
            obuf[:, pl.ds(pl.multiple_of(half + b * PAIR, 128), PAIR)] = opair[pl.ds(far_rows, crows), :]
            o2_copy(b).start()
            append2(b)

    @pl.loop(0, blocks)
    def _(b):
        remote(o2_far(b), o2_piece(b, 1 - chip), osend.at[b], orecv.at[b], peer).wait_recv()

    def y_copy(b):
        return remote(o_send.at[b], o_recv.at[b], qsend.at[b], qrecv.at[b], partner)

    @pl.loop(0, blocks)
    def _(b):
        slot = wait_tile(base2 + qkv2 + b)
        for i in range(2):
            y = jnp.dot(obuf[:, :half], wring[slot, i * half:(i + 1) * half, :], preferred_element_type=F32)
            at = pl.ds(i * rows, rows)
            for j in range(PER_BLOCK):
                lanes = pl.ds(j * HEAD, HEAD)
                st_loc[j] = y[:, j * HEAD:(j + 1) * HEAD]
                o_send[b, at, lanes] = st_loc[j, pl.ds(other_rows, rows), :]
                o_loc[b, at, lanes] = st_loc[j, pl.ds(my_rows, rows), :]
        y_copy(b).start()

    @pl.loop(0, blocks)
    def _(b):
        y_copy(b).wait_recv()
        for i in range(2):
            at = pl.ds(i * rows, rows)
            ybuf[:, pl.ds(pl.multiple_of(b * 2 * TILE + i * TILE, 128), TILE)] = (o_loc[b, at, :] + o_recv[b, at, :]).astype(BF16)

    y_copies = [pltpu.make_async_copy(ybuf, y_out, gsem.at[1])]
    for c in y_copies:
        c.start()

    @pl.loop(0, blocks)
    def _(b):
        y_copy(b).wait_send()
        o2_copy(b).wait_send()
        remote(g_piece(b, chip_rows), g_piece(b, chip_rows), gxs.at[b], gxr.at[b], peer).wait_send()

    for kv, dst in enumerate((k2_out, v2_out)):
        ref = dst.at[:, pl.ds(0, half)]
        pltpu.make_async_copy(ref, ref, a2send.at[2 * kv]).wait()
        remote(ref, ref, a2send.at[2 * kv + 1], a2recv.at[kv], partner).wait_send()
        remote(ref, ref, a2send.at[2 * kv + 1], a2recv.at[kv], partner).wait_recv()
        for kind in (2, 3):
            cache2_copy(kv, kind).wait_send()
    for ref, sem in ((y_out, 1), (g_out, 0)):
        pltpu.make_async_copy(ref, ref, gsem.at[sem]).wait()


def deliver(*refs):
    for i in range(6):
        src, dst = refs[i], refs[6 + i]
        dst[...] = src[...] if i < 2 else pltpu.einshape("t(hd)->thd", src[...], d=HEAD)


def solution(mesh):
    rows_spec = P(('dp', 'cp'), None)
    cache_spec = P(('dp', 'cp'), None, None)
    mat_spec = P(None, None)
    vec_spec = P(None)
    layer_specs = (cache_spec, cache_spec, mat_spec, vec_spec, mat_spec, vec_spec, mat_spec, mat_spec)
    in_specs = (rows_spec,) + layer_specs + (mat_spec, mat_spec, mat_spec) + layer_specs
    out_specs = (rows_spec, rows_spec, cache_spec, cache_spec, cache_spec, cache_spec)

    def forward(x_in, cache_k1, cache_v1, w_q1, b_q1, w_k1, b_k1, w_v1, w_o1, w_gate, w_up, w_down, cache_k2, cache_v2, w_q2, b_q2, w_k2, b_k2, w_v2, w_o2):
        rows, d_model = x_in.shape
        cache_rows, heads, head_dim = cache_k1.shape
        ff = w_gate.shape[1]
        half = d_model // 2
        blocks = half // TILE
        crows = 2 * rows
        cos_t, sin_t = rope_tables(4 * cache_rows + np.arange(2 * crows), head_dim)
        bias = [v.reshape(heads, head_dim) for v in (b_q1, b_k1, b_q2, b_k2)]

        any_spec = pl.BlockSpec(memory_space=pl.ANY)
        vmem_spec = pl.BlockSpec(memory_space=pltpu.VMEM)
        row_out = jax.ShapeDtypeStruct((rows, d_model), BF16)
        dma = pltpu.SemaphoreType.DMA
        out = pl.pallas_call(
            functools.partial(body, (d_model, ff, rows, cache_rows)),
            out_shape=[row_out] * 6 + [jax.ShapeDtypeStruct((cache_rows, d_model), BF16)] * 4,
            in_specs=[vmem_spec] * 6 + [any_spec] * 16,
            out_specs=[any_spec] * 10,
            scratch_shapes=[
                pltpu.VMEM((SLOTS, d_model, TILE), BF16),
                pltpu.VMEM((2 * crows, d_model), BF16),
                pltpu.VMEM((2 * crows, d_model), BF16),
                pltpu.VMEM((crows, ff), BF16),
                pltpu.VMEM((2 * blocks, 2 * crows, TILE), BF16),
                pltpu.VMEM((2 * cache_rows, half), BF16),
                pltpu.VMEM((2 * cache_rows, half), BF16),
                pltpu.VMEM((blocks, crows, TILE), F32),
                pltpu.VMEM((blocks, crows, TILE), F32),
                pltpu.VMEM((blocks, crows, TILE), F32),
                pltpu.VMEM((crows, d_model), BF16),
                pltpu.VMEM((2 * crows, TILE // 2), BF16),
                pltpu.VMEM((blocks, crows, HEAD), F32),
                pltpu.VMEM((blocks, 8, HEAD), F32),
                pltpu.VMEM((blocks, 8, HEAD), F32),
                pltpu.VMEM((4, heads, head_dim), F32),
                dma((SLOTS,)), dma((3,)), dma((6,)), dma((8,)), dma((8, 6)),
                dma((blocks,)), dma((blocks,)), dma((blocks,)), dma((blocks,)), dma((blocks,)), dma((blocks,)),
                dma((5,)), dma((5,)), dma((6,)), dma((2,)),
                dma((blocks,)), dma((blocks,)), dma((4,)), dma((2,)),
                dma((blocks,)), dma((blocks,)), dma((2,)), pltpu.SemaphoreType.REGULAR,
                pltpu.VMEM((2, cache_rows, 8, head_dim), BF16), dma((2,)), dma((2,)),
            ],
            compiler_params=pltpu.CompilerParams(
                collective_id=0, has_side_effects=True, vmem_limit_bytes=67043328),
        )(cos_t, sin_t, *bias, x_in, cache_k1, cache_v1, cache_k2, cache_v2,
          w_q1, w_k1, w_v1, w_o1, w_gate, w_up, w_down, w_q2, w_k2, w_v2, w_o2)
        steps = 4
        step_rows = pl.BlockSpec((rows // steps, d_model), lambda i: (i, 0))
        step_heads = pl.BlockSpec((rows // steps, heads, head_dim), lambda i: (i, 0, 0))
        head_out = jax.ShapeDtypeStruct((rows, heads, head_dim), BF16)
        return pl.pallas_call(
            deliver,
            grid=(steps,),
            out_shape=[row_out] * 2 + [head_out] * 4,
            in_specs=[step_rows] * 6,
            out_specs=[step_rows] * 2 + [step_heads] * 4,
        )(*out[:6])

    return jax.shard_map(forward, mesh=mesh, in_specs=in_specs, out_specs=out_specs, check_vma=False)
```

```python
import functools
import math

import jax
import jax.numpy as jnp
import numpy as np
from jax import lax
from jax.experimental import pallas as pl
from jax.experimental.pallas import tpu as pltpu
from jax.sharding import PartitionSpec as P

ROPE_THETA = 500000.0
NORM_EPS = 1e-5
MESH = pl.DeviceIdType.MESH
F32 = jnp.float32
BF16 = jnp.bfloat16

TILE = 512
HEAD = 128
PER_BLOCK = TILE // HEAD
SLOTS = 7


def rope_tables(positions, head_dim):
    half_dim = head_dim // 2
    inv_freq = (1.0 / (ROPE_THETA ** (np.arange(half_dim, dtype=np.float32) * np.float32(2.0 / head_dim)))).astype(np.float32)
    angles = positions.astype(np.float32)[:, None] * inv_freq[None, :]
    cos_t, sin_t = np.cos(angles), np.sin(angles)
    return np.concatenate([cos_t, cos_t], axis=1), np.concatenate([-sin_t, sin_t], axis=1)


def body(dims, cos_ref, sin_ref, bq1, bk1, bq2, bk2, x_hbm, raw_k1, raw_v1, raw_k2, raw_v2, wq1, wk1, wv1, wo1, w_gate, w_up, w_down,
         wq2, wk2, wv2, wo2, g_out, y_out, k1_out, v1_out, k2_out, v2_out, ck2, cv2,
         wring, nbuf, gbuf, ebuf, pre, kc, vc, o_loc, o_send, o_recv, obuf, opair,
         st_loc, st_send, st_recv, bias32,
         wsem, xsem, csem, c2send, c2recv, qsend, qrecv, osend, orecv, ssend, srecv, dsend, drecv, asem, gsem,
         gxs, gxr, a2send, a2recv, hys, hyr, esem, yfree, rawbuf, psem, fsem):
    d_model, ff, rows, cache_rows = dims
    half = d_model // 2
    ffh = ff // 2
    ffc = ff // 3
    third = ffc // 2
    part = third // (TILE // 2)
    blocks = half // TILE
    ffn = ffh // (TILE // 2)
    crows = 2 * rows
    quart = half // 2
    ybuf = nbuf.at[pl.ds(0, rows), :]
    me = lax.axis_index("cp")
    core = lax.rem(me, 2)
    chip = me // 2
    partner = me + 1 - 2 * core
    peer = lax.rem(me + 2, 4)
    diag = 3 - me
    dp = lax.axis_index("dp")
    side_y = 1 - dp
    chip_rows = pl.multiple_of(chip * crows, 16)
    xin = hbuf = gbuf.at[pl.ds(pl.multiple_of(chip * crows, 16), crows), :]
    far_rows = pl.multiple_of((1 - chip) * crows, 16)
    my_cols = pl.multiple_of(core * half, 128)
    my_rows = pl.multiple_of(core * rows, 16)
    other_rows = pl.multiple_of((1 - core) * rows, 16)
    other_cols = pl.multiple_of((1 - core) * half, 128)

    def col(b):
        return pl.multiple_of(core * half + b * TILE, 128)

    attn_tiles = 4 * blocks
    base1 = 0
    base_up = attn_tiles
    base_down = base_up + 2 * part
    base_x = base_down + 3 * blocks
    base2 = base_x + blocks
    qkv2 = 8

    def start_full(w, b, slot):
        pltpu.make_async_copy(w.at[:, pl.ds(col(b), TILE)], wring.at[slot], wsem.at[slot]).start()

    def mlp_cols(tile):
        return pl.ds(pl.multiple_of(core * ffh + tile * (TILE // 2), 128), TILE // 2)

    def shared_tile(n):
        return part + dp * part + n

    def start_mlp(tile, slot):
        at = mlp_cols(tile)
        pltpu.make_async_copy(w_gate.at[:, at], wring.at[slot, :, pl.ds(0, TILE // 2)], wsem.at[slot]).start()
        pltpu.make_async_copy(w_up.at[:, at], wring.at[slot, :, pl.ds(TILE // 2, TILE // 2)], wsem.at[slot]).start()

    def start_down(b, chunk, slot):
        for i in range(2):
            pltpu.make_async_copy(
                w_down.at[pl.ds(pl.multiple_of(i * ffh + chunk * third, 16), third), pl.ds(col(b), TILE)],
                wring.at[slot, pl.ds(i * third, third), :], wsem.at[slot]).start()

    loop_end = 3 * (blocks - 1) + 1

    def attn_segments(base, wq, wk, wv, wo):
        return [
            (base, base + 1, lambda r, slot: start_full(wq, 0, slot), None),
            (base + 1, base + loop_end, lambda r, slot: start_full(wq, r // 3 + 1, slot), 0),
            (base + 1, base + loop_end, lambda r, slot: start_full(wk, r // 3, slot), 1),
            (base + 1, base + loop_end, lambda r, slot: start_full(wv, r // 3, slot), 2),
            (base + loop_end, base + loop_end + 1, lambda r, slot: start_full(wk, blocks - 1, slot), None),
            (base + loop_end + 1, base + loop_end + 2, lambda r, slot: start_full(wv, blocks - 1, slot), None),
            (base + loop_end + 2, base + attn_tiles, lambda r, slot: start_full(wo, r, slot), None),
        ]

    PAIR = TILE // 2
    own2 = core * half + chip * quart

    def start_v2(t, slot):
        @pl.when(t < qkv2 - 2)
        def _():
            pltpu.make_async_copy(wv2.at[:, pl.ds(pl.multiple_of(own2 + (t // 3) * TILE, 128), TILE)], wring.at[slot],
                                  wsem.at[slot]).start()

        @pl.when(t >= qkv2 - 2)
        def _():
            pltpu.make_async_copy(wv2.at[:, pl.ds(pl.multiple_of(own2 + (t // 3) * TILE, 128), PAIR)],
                                  wring.at[slot, :, pl.ds(0, PAIR)], wsem.at[slot]).start()

    def start_qk2(t, slot):
        at = pl.ds(pl.multiple_of(own2 + (t - 1 - t // 3) * PAIR, 128), PAIR)
        pltpu.make_async_copy(wq2.at[:, at], wring.at[slot, :, pl.ds(0, PAIR)], wsem.at[slot]).start()
        pltpu.make_async_copy(wk2.at[:, at], wring.at[slot, :, pl.ds(PAIR, PAIR)], wsem.at[slot]).start()

    other2 = core * half + (1 - chip) * quart

    def start_kv_other(b, slot):
        at = pl.ds(pl.multiple_of(other2 + b * PAIR, 128), PAIR)
        pltpu.make_async_copy(wk2.at[:, at], wring.at[slot, :, pl.ds(0, PAIR)], wsem.at[slot]).start()
        pltpu.make_async_copy(wv2.at[:, at], wring.at[slot, :, pl.ds(PAIR, PAIR)], wsem.at[slot]).start()

    def start_wo2(b, slot):
        for i in range(2):
            pltpu.make_async_copy(
                wo2.at[pl.ds(my_cols, half), pl.ds(pl.multiple_of(b * 2 * TILE + i * TILE, 128), TILE)],
                wring.at[slot, pl.ds(i * half, half), :], wsem.at[slot]).start()

    segments = attn_segments(base1, wq1, wk1, wv1, wo1) + [
        (base_up, base_up + part, start_mlp, None),
        (base_up + part, base_down, lambda r, slot: start_mlp(shared_tile(r), slot), None),
        (base_down, base_down + blocks, lambda r, slot: start_down(r, 0, slot), None),
        (base_down + blocks, base_x, lambda r, slot: start_down(r // 2, 1 + r % 2 if isinstance(r, int) else 1 + lax.rem(r, 2), slot), None),
        (base_x, base2, start_kv_other, None),
        (base2, base2 + qkv2, start_v2, 0),
        (base2, base2 + qkv2, start_qk2, 1),
        (base2, base2 + qkv2, start_qk2, 2),
        (base2 + qkv2, base2 + qkv2 + blocks, start_wo2, None),
    ]

    def start_tile(s, lo, hi):
        slot = lax.rem(s, SLOTS) if not isinstance(s, int) else s % SLOTS
        for a, b, fn, phase in segments:
            if b <= lo or a >= hi:
                continue
            if isinstance(s, int):
                if a <= s < b and (phase is None or (s - a) % 3 == phase):
                    fn(s - a, slot)
                continue
            cond = (s >= a) & (s < b)
            if phase is not None:
                cond = cond & (lax.rem(s - a + 3, 3) == phase)

            @pl.when(cond)
            def _(a=a, fn=fn):
                fn(s - a, slot)

    def wait_tile(s, depth=None):
        slot = lax.rem(s, SLOTS) if not isinstance(s, int) else s % SLOTS
        ref = wring.at[slot] if depth is None else wring.at[slot, pl.ds(0, depth), :]
        pltpu.make_async_copy(ref, ref, wsem.at[slot]).wait()
        return slot

    def remote(src, dst, send, recv, who):
        return pltpu.make_async_remote_copy(src_ref=src, dst_ref=dst, send_sem=send, recv_sem=recv,
                                            device_id={"cp": who}, device_id_type=MESH)

    def remote_y(src, dst, send, recv):
        return pltpu.make_async_remote_copy(src_ref=src, dst_ref=dst, send_sem=send, recv_sem=recv,
                                            device_id={"dp": side_y}, device_id_type=MESH)

    HEADS8 = 8
    WIDE = HEADS8 * HEAD
    groups = d_model // WIDE

    def raw_copy(raw, j, slot):
        return pltpu.make_async_copy(raw.at[:, pl.ds(pl.multiple_of(j * HEADS8, HEADS8), HEADS8), :], rawbuf.at[slot],
                                     psem.at[slot])

    def flat_wait(flat, slot):
        ref = flat.at[:, pl.ds(0, WIDE)]
        pltpu.make_async_copy(ref, ref, fsem.at[slot]).wait()

    def flatten_heads(flat, j, slot):
        for i in range(cache_rows // crows):
            at = pl.ds((slot * 2 + i) * WIDE, WIDE)
            ebuf[:, at] = pltpu.einshape("thd->t(hd)", rawbuf[slot, i * crows:(i + 1) * crows])
            pltpu.make_async_copy(ebuf.at[:, at], flat.at[pl.ds(i * crows, crows), pl.ds(pl.multiple_of(j * WIDE, 128), WIDE)],
                                  fsem.at[slot]).start()

    layer1 = ((raw_k1, kc), (raw_v1, vc))
    layer2 = ((raw_k2, ck2), (raw_v2, cv2))
    for j in range(2):
        for kv in range(2):
            raw_copy(layer1[kv][0], j, 2 * j + kv).start()
    for s in range(3):
        start_tile(s, s, s + 1)

    barrier = pltpu.get_barrier_semaphore()
    for who in (partner, peer, diag):
        pl.semaphore_signal(barrier, inc=1, device_id={"cp": who}, device_id_type=MESH)
    pl.semaphore_signal(barrier, inc=1, device_id={"dp": side_y}, device_id_type=MESH)
    pl.semaphore_wait(barrier, 4)

    x_loc = pltpu.make_async_copy(x_hbm, xin.at[pl.ds(my_rows, rows)], xsem.at[0])
    x_rem = remote(x_hbm, xin.at[pl.ds(my_rows, rows)], xsem.at[1], xsem.at[2], partner)
    x_rem.start()
    x_loc.start()

    crow = pl.ds(pl.multiple_of(core * cache_rows, 16), cache_rows)
    cache1 = [remote(c.at[crow], c.at[crow], csem.at[2 * kv], csem.at[2 * kv + 1], partner) for kv, c in enumerate((kc, vc))]

    @pl.loop(0, groups)
    def _(j):
        for kv, (raw, cache) in enumerate(layer1):
            slot = 2 * lax.rem(j, 2) + kv
            raw_copy(raw, j, slot).wait()
            for i in range(cache_rows // crows):
                rows_at = pl.ds(pl.multiple_of(core * cache_rows + i * crows, 16), crows)
                vals = pltpu.einshape("thd->t(hd)", rawbuf[slot, i * crows:(i + 1) * crows])
                for part_i in range(WIDE // TILE):
                    piece = vals[:, part_i * TILE:(part_i + 1) * TILE]
                    block = 2 * j + part_i
                    owner = block // blocks
                    block = block - owner * blocks
                    to_at = pl.ds(pl.multiple_of(block * TILE, 128), TILE)

                    @pl.when(owner == core)
                    def _():
                        cache[rows_at, to_at] = piece

                    @pl.when(owner != core)
                    def _():
                        at = pl.ds(pl.multiple_of(((block * 2 + kv) * 2 + i) * TILE, 128), TILE)
                        ebuf[:, at] = piece
                        remote(ebuf.at[:, at], cache.at[rows_at, to_at], csem.at[2 * kv], csem.at[2 * kv + 1], partner).start()

            @pl.when(j < groups - 2)
            def _():
                raw_copy(raw, j + 2, slot).start()

    for slot, (raw, flat) in enumerate(layer2):
        raw_copy(raw, 0, slot).start()
    for s in range(3, SLOTS):
        start_tile(s, s, s + 1)
    for i, ref in enumerate((bq1, bk1, bq2, bk2)):
        bias32[i] = ref[...].astype(F32)
    x_loc.wait()
    x_rem.wait()

    def biased_rope(vals, bias_row, first_head, table_at, n):
        parts = []
        cos_t, sin_t = cos_ref[table_at, :], sin_ref[table_at, :]
        for i in range(n):
            seg = vals[:, i * HEAD:(i + 1) * HEAD] + bias32[bias_row, pl.ds(first_head + i, 1), :]
            seg = seg.astype(BF16).astype(F32)
            parts.append((seg * cos_t + pltpu.roll(seg, HEAD // 2, 1) * sin_t).astype(BF16))
        return jnp.concatenate(parts, axis=1)

    def norm(src, dst, first, count):
        step = 16

        @pl.loop(0, count // step)
        def _(i):
            at = pl.ds(pl.multiple_of(first + i * step, step), step)
            wide = src[at, :].astype(F32)
            dst[at, :] = (wide * lax.rsqrt(jnp.mean(wide * wide, axis=-1, keepdims=True) + NORM_EPS)).astype(BF16)

    row_i = lax.broadcasted_iota(jnp.int32, (2 * crows, crows), 0)
    col_i = lax.broadcasted_iota(jnp.int32, (2 * crows, crows), 1)
    far_lim = jnp.where(chip == 0, crows, -1)
    scale = HEAD ** -0.5 * math.log2(math.e)

    def attend(b):
        lane = lax.broadcasted_iota(jnp.int32, (2 * crows, HEAD), 1)
        visible = col_i <= jnp.where(row_i < crows, row_i, far_lim)
        stats = jnp.zeros((2 * crows, HEAD), F32)
        dims_t = (((1,), (1,)), ((), ()))
        for i in range(PER_BLOCK):
            at = pl.ds(i * HEAD, HEAD)
            cat = pl.ds(pl.multiple_of(b * TILE + i * HEAD, 128), HEAD)
            q = pre[b, :, at]
            s_old = lax.dot_general(q, kc[:, cat], dims_t, preferred_element_type=F32)
            s_new = lax.dot_general(q, pre[blocks + b, pl.ds(0, crows), at], dims_t, preferred_element_type=F32)
            s_new = jnp.where(visible, s_new, -jnp.inf)
            peak = jnp.maximum(jnp.max(s_old, axis=1, keepdims=True), jnp.max(s_new, axis=1, keepdims=True))
            p_old = jnp.exp2((s_old - peak) * scale)
            p_new = jnp.exp2((s_new - peak) * scale)
            total_p = jnp.sum(p_old, axis=1, keepdims=True) + jnp.sum(p_new, axis=1, keepdims=True)
            acc = jnp.dot(p_old.astype(BF16), vc[:, cat], preferred_element_type=F32)
            acc = acc + jnp.dot(p_new.astype(BF16), pre[blocks + b, pl.ds(crows, crows), at], preferred_element_type=F32)
            o_loc[b, :, at] = acc[:crows]
            o_send[b, :, at] = acc[crows:]
            stats = jnp.where(lane == 2 * i, peak, stats)
            stats = jnp.where(lane == 2 * i + 1, total_p, stats)
        st_loc[b] = stats[:crows]
        st_send[b] = stats[crows:].T[:8, :]

    def q_copy(b):
        return remote(pre.at[b, pl.ds(0, crows), :], pre.at[b, pl.ds(crows, crows), :], qsend.at[b], qrecv.at[b], peer)

    def o_copy(b):
        return remote(o_send.at[b], o_recv.at[b], osend.at[b], orecv.at[b], peer)

    def s_copy(b):
        return remote(st_send.at[b], st_recv.at[b], ssend.at[b], srecv.at[b], peer)

    def head_of(b):
        return core * (half // HEAD) + b * PER_BLOCK

    def attention(layer_in, base, bias_row, caches, k_out, v_out):
        def q_step(b, s, lo, hi):
            slot = wait_tile(s)
            raw = jnp.dot(layer_in[...], wring[slot], preferred_element_type=F32)
            start_tile(s + SLOTS, lo + SLOTS, hi + SLOTS)
            pre[b, pl.ds(0, crows), :] = biased_rope(raw, bias_row, head_of(b), pl.ds(chip_rows, crows), PER_BLOCK)
            q_copy(b).start()

        q_step(0, base, base, base + 1)

        @pl.loop(0, blocks)
        def _(b):
            has_q = (2 * blocks - 3 - b) // (blocks - 1)
            s = base + 1 + 3 * b

            @pl.when(b < blocks - 1)
            def _():
                q_step(b + 1, s, base + 1, base + loop_end)

            s = s + has_q
            slot = wait_tile(s)
            raw = jnp.dot(layer_in[...], wring[slot], preferred_element_type=F32)
            start_tile(s + SLOTS, base + 2 + SLOTS, base + loop_end + 2 + SLOTS)
            pre[blocks + b, pl.ds(0, crows), :] = biased_rope(raw, bias_row + 1, head_of(b), pl.ds(chip_rows, crows), PER_BLOCK)
            s = s + 1
            slot = wait_tile(s)
            vals = jnp.dot(layer_in[...], wring[slot], preferred_element_type=F32).astype(BF16)
            start_tile(s + SLOTS, base + 3 + SLOTS, base + loop_end + 2 + SLOTS)
            pre[blocks + b, pl.ds(crows, crows), :] = vals

            @pl.when(b == 0)
            def _():
                for c in caches:
                    c.wait()

            q_copy(b).wait_recv()
            attend(b)
            for part, dst, k in ((0, k_out, 0), (crows, v_out, 3)):
                pltpu.make_async_copy(pre.at[blocks + b, pl.ds(part + my_rows, rows), :], dst.at[:, pl.ds(col(b), TILE)], asem.at[k]).start()
                remote(pre.at[blocks + b, pl.ds(part + other_rows, rows), :], dst.at[:, pl.ds(col(b), TILE)], asem.at[k + 1],
                       asem.at[k + 2], partner).start()
            o_copy(b).start()
            s_copy(b).start()
            for slot, (raw, flat) in enumerate(layer2):
                raw_copy(raw, b, slot).wait()

                @pl.when(b > 0)
                def _():
                    flat_wait(flat, slot)

                flatten_heads(flat, b, slot)

                @pl.when(b < blocks - 1)
                def _():
                    raw_copy(raw, b + 1, slot).start()

        for slot, (raw, flat) in enumerate(layer2):
            flat_wait(flat, slot)

        @pl.loop(0, blocks)
        def _(b):
            o_copy(b).wait_recv()
            s_copy(b).wait_recv()
            far = jnp.concatenate([st_recv[b], jnp.zeros((HEAD - 8, HEAD), F32)], axis=0).T
            near = st_loc[b]
            for i in range(PER_BLOCK):
                at = pl.ds(i * HEAD, HEAD)
                m_a, l_a = near[:, 2 * i:2 * i + 1], near[:, 2 * i + 1:2 * i + 2]
                m_b, l_b = far[:, 2 * i:2 * i + 1], far[:, 2 * i + 1:2 * i + 2]
                peak = jnp.maximum(m_a, m_b)
                w_a, w_b = jnp.exp2((m_a - peak) * scale), jnp.exp2((m_b - peak) * scale)
                norm_l = 1.0 / (l_a * w_a + l_b * w_b)
                o = o_loc[b, :, at] * (w_a * norm_l) + o_recv[b, :, at] * (w_b * norm_l)
                obuf[:, pl.ds(pl.multiple_of(core * half + b * TILE + i * HEAD, 128), HEAD)] = o.astype(BF16)
            piece = obuf.at[:, pl.ds(col(b), TILE)]
            remote(piece, piece, dsend.at[0], drecv.at[0], partner).start()

        mine = obuf.at[:, pl.ds(my_cols, half)]
        theirs = obuf.at[:, pl.ds(other_cols, half)]
        remote(mine, theirs, dsend.at[0], drecv.at[0], partner).wait_send()
        remote(mine, theirs, dsend.at[0], drecv.at[0], partner).wait_recv()

        @pl.loop(0, blocks)
        def _(b):
            q_copy(b).wait_send()
            o_copy(b).wait_send()
            s_copy(b).wait_send()

        for dst, k in ((k_out, 0), (v_out, 3)):
            to_me = dst.at[:, pl.ds(my_cols, half)]
            to_me2 = dst.at[:, pl.ds(other_cols, half)]
            pltpu.make_async_copy(to_me, to_me, asem.at[k]).wait()
            remote(to_me, to_me2, asem.at[k + 1], asem.at[k + 2], partner).wait_send()
            remote(to_me, to_me2, asem.at[k + 1], asem.at[k + 2], partner).wait_recv()

    def both_wait(buf, sem, width, my_at, other_at):
        mine = buf.at[:, pl.ds(my_at, width)]
        theirs = buf.at[:, pl.ds(other_at, width)]
        remote(mine, theirs, dsend.at[sem], drecv.at[sem], partner).wait_send()
        remote(mine, theirs, dsend.at[sem], drecv.at[sem], partner).wait_recv()

    attention(xin, base1, 0, cache1, k1_out, v1_out)
    pl.semaphore_signal(yfree, inc=1, device_id={"dp": side_y}, device_id_type=MESH)

    PIECE = TILE // 2

    def cache2_copy(kv, kind, b=None):
        src, dst = ((ck2, kc), (cv2, vc))[kv]
        who, to_core, to_chip = ((None, core, chip), (partner, 1 - core, chip), (peer, core, 1 - chip),
                                 (diag, 1 - core, 1 - chip))[kind]
        off, width, sem = (0, quart, 0) if b is None else (b * PIECE, PIECE, 1 + b)
        side = 0 if kind < 2 else quart
        from_at = pl.ds(pl.multiple_of(to_core * half + to_chip * quart + off, 128), width)
        to = dst.at[pl.ds(pl.multiple_of(core * cache_rows, 16), cache_rows), pl.ds(pl.multiple_of(side + off, 128), width)]
        i = 4 * kv + kind
        if kind == 0:
            return pltpu.make_async_copy(src.at[:, from_at], to, c2send.at[i])
        return remote(src.at[:, from_at], to, c2send.at[i], c2recv.at[i, sem], who)

    def far_cache(b):
        for kv in range(2):
            for kind in (2, 3):
                cache2_copy(kv, kind, b).start()

    for b in range(3):
        far_cache(b)
    for kind in (1, 0):
        for kv in range(2):
            cache2_copy(kv, kind).start()

    pl.semaphore_wait(yfree, 1)

    def h_copy(b):
        return remote_y(hbuf.at[:, pl.ds(col(b), TILE)], pre.at[core * blocks + b, pl.ds(0, crows), :], hys.at[b], hyr.at[b])

    @pl.loop(0, blocks)
    def _(b):
        s = base1 + 3 * blocks + b
        slot = wait_tile(s)
        y = jnp.dot(obuf[...], wring[slot], preferred_element_type=F32).astype(BF16)
        start_tile(s + SLOTS, base1 + 3 * blocks + SLOTS, base_up + SLOTS)
        at = pl.ds(col(b), TILE)
        hbuf[:, at] = (xin[:, at].astype(F32) + y.astype(F32)).astype(BF16)
        h_copy(b).start()
        remote(hbuf.at[:, at], hbuf.at[:, at], dsend.at[1], drecv.at[1], partner).start()

    both_wait(hbuf, 1, half, my_cols, other_cols)
    norm(hbuf, nbuf, 0, crows)

    def glu(both):
        gate = both[:, :TILE // 2].astype(BF16).astype(F32)
        up = both[:, TILE // 2:].astype(BF16).astype(F32)
        return (jax.nn.silu(gate) * up).astype(BF16)

    @pl.loop(0, part)
    def _(n):
        s = base_up + n
        slot = wait_tile(s)
        both = jnp.dot(nbuf[pl.ds(0, crows), :], wring[slot], preferred_element_type=F32)
        start_tile(s + SLOTS, base_up + SLOTS, base_up + part + SLOTS)
        at = mlp_cols(n)
        ebuf[:, at] = glu(both)
        remote(ebuf.at[:, at], ebuf.at[:, at], dsend.at[2], drecv.at[2], partner).start()

    far_h = pre.at[pl.ds(core * blocks, blocks), pl.ds(0, crows), :]
    far_h_other = pre.at[pl.ds((1 - core) * blocks, blocks), pl.ds(0, crows), :]

    @pl.loop(0, blocks)
    def _(b):
        h_copy(b).wait_recv()
        h_copy(b).wait_send()

    remote(far_h, far_h, dsend.at[4], drecv.at[4], partner).start()
    remote(far_h, far_h, dsend.at[4], drecv.at[4], partner).wait_send()
    remote(far_h_other, far_h_other, dsend.at[4], drecv.at[4], partner).wait_recv()

    @pl.loop(0, crows // 16)
    def _(i):
        at = pl.ds(pl.multiple_of(i * 16, 16), 16)
        wide = [pre[j, at, :].astype(F32) for j in range(2 * blocks)]
        square = sum(jnp.sum(w * w, axis=-1, keepdims=True) for w in wide)
        inv = lax.rsqrt(square / d_model + NORM_EPS)
        for j in range(2 * blocks):
            nbuf[pl.ds(pl.multiple_of(crows + i * 16, 16), 16), pl.ds(j * TILE, TILE)] = (wide[j] * inv).astype(BF16)

    def e_return(n):
        return remote_y(pre.at[n, pl.ds(crows, crows), pl.ds(0, TILE // 2)], ebuf.at[:, mlp_cols(shared_tile(n))],
                        esem.at[0], esem.at[1])

    @pl.loop(0, part)
    def _(n):
        s = base_up + part + n
        slot = wait_tile(s)
        both = jnp.dot(nbuf[...], wring[slot], preferred_element_type=F32)
        start_tile(s + SLOTS, base_up + part + SLOTS, base_down + SLOTS)
        at = mlp_cols(shared_tile(n))
        mixed = glu(both)
        ebuf[:, at] = mixed[:crows]
        pre[n, pl.ds(crows, crows), pl.ds(0, TILE // 2)] = mixed[crows:]
        e_return(n).start()
        remote(ebuf.at[:, at], ebuf.at[:, at], dsend.at[2], drecv.at[2], partner).start()

    def returned(to_core):
        return ebuf.at[:, pl.ds(pl.multiple_of(to_core * ffh + (1 + side_y) * third, 128), third)]

    def partner_e_wait():
        some = ebuf.at[:, pl.ds(0, 2 * third)]
        remote(some, some, dsend.at[2], drecv.at[2], partner).wait_send()
        remote(some, some, dsend.at[2], drecv.at[2], partner).wait_recv()

    partner_e_wait()

    def down_dot(slot, chunk):
        out = None
        for i in range(2):
            at = pl.ds(pl.multiple_of(i * ffh + chunk * third, 128), third)
            term = jnp.dot(ebuf[:, at], wring[slot, i * third:(i + 1) * third, :], preferred_element_type=F32)
            out = term if out is None else out + term
        return out

    @pl.loop(0, blocks)
    def _(b):
        @pl.when(b == blocks - 2)
        def _():
            e_all = remote_y(returned(core), returned(core), esem.at[0], esem.at[1])
            e_all.wait_send()
            e_all.wait_recv()
            remote(returned(core), returned(core), dsend.at[1], drecv.at[1], partner).start()

        s = base_down + b
        slot = wait_tile(s, ffc)
        o_loc[b] = down_dot(slot, 0)
        start_tile(s + SLOTS, base_down + SLOTS, base_down + blocks + SLOTS)

    remote(returned(core), returned(core), dsend.at[1], drecv.at[1], partner).wait_send()
    remote(returned(1 - core), returned(1 - core), dsend.at[1], drecv.at[1], partner).wait_recv()

    def g_piece(b, first):
        return gbuf.at[pl.ds(first, crows), pl.ds(col(b), TILE)]

    @pl.loop(0, blocks)
    def _(b):
        at = pl.ds(col(b), TILE)
        down = o_loc[b]
        for k in range(2):
            s = base_down + blocks + 2 * b + k
            slot = wait_tile(s, ffc)
            down = down + down_dot(slot, 1 + k)
            start_tile(s + SLOTS, base_down + blocks + k + SLOTS, base_x - 1 + k + SLOTS)
        gbuf[pl.ds(chip_rows, crows), at] = (hbuf[:, at].astype(F32) + down).astype(BF16)
        piece = g_piece(b, chip_rows)
        remote(piece, piece, gxs.at[b], gxr.at[b], peer).start()
        remote(piece, piece, dsend.at[3], drecv.at[3], partner).start()

    def g_wait(first, sem):
        mine = gbuf.at[pl.ds(first, crows), pl.ds(my_cols, half)]
        theirs = gbuf.at[pl.ds(first, crows), pl.ds(other_cols, half)]
        remote(mine, theirs, dsend.at[sem], drecv.at[sem], partner).wait_send()
        remote(mine, theirs, dsend.at[sem], drecv.at[sem], partner).wait_recv()

    far_cache(3)
    far_cache(4)
    g_wait(chip_rows, 3)
    g_rows = pl.ds(pl.multiple_of(chip_rows + my_rows, 16), rows)
    g_copies = [pltpu.make_async_copy(gbuf.at[g_rows, :], g_out, gsem.at[0])]
    for c in g_copies:
        c.start()
    norm(gbuf, nbuf, chip_rows, crows)

    def g_forward(b):
        far = g_piece(b, far_rows)
        remote(far, far, gxs.at[b], gxr.at[b], peer).wait_recv()
        remote(far, far, dsend.at[0], drecv.at[0], partner).start()

    @pl.loop(0, blocks - 1)
    def _(b):
        g_forward(b)

    @pl.loop(0, blocks)
    def _(b):
        s = base_x + b
        slot = wait_tile(s)
        raw = jnp.dot(nbuf[pl.ds(chip_rows, crows), :], wring[slot], preferred_element_type=F32)
        start_tile(s + SLOTS, base_x + SLOTS, base2 + SLOTS)
        k_at = pl.ds(pl.multiple_of(b * TILE, 128), PAIR)
        v_at = pl.ds(pl.multiple_of(b * TILE + PAIR, 128), PAIR)
        ebuf[:, k_at] = biased_rope(raw[:, :PAIR], 3, other2 // HEAD + 2 * b, pl.ds(chip_rows, crows), 2)
        ebuf[:, v_at] = raw[:, PAIR:].astype(BF16)
        to_at = pl.ds(pl.multiple_of(other2 + b * PAIR, 128), PAIR)
        for kv, (at, dst) in enumerate(((k_at, k2_out), (v_at, v2_out))):
            pltpu.make_async_copy(ebuf.at[pl.ds(my_rows, rows), at], dst.at[:, to_at], a2send.at[2 * kv]).start()
            remote(ebuf.at[pl.ds(other_rows, rows), at], dst.at[:, to_at], a2send.at[2 * kv + 1], a2recv.at[kv], partner).start()

    g_forward(blocks - 1)
    g_wait(far_rows, 0)
    norm(gbuf, nbuf, far_rows, crows)

    heads2 = quart // HEAD
    row_2 = lax.broadcasted_iota(jnp.int32, (2 * crows, 2 * crows), 0)
    col_2 = lax.broadcasted_iota(jnp.int32, (2 * crows, 2 * crows), 1)

    def qk_tile(b):
        return b + 1 + b // 2

    def attend2(b):
        t = qk_tile(b)
        vt = 3 * (b // 2)
        dims_t = (((1,), (1,)), ((), ()))
        visible = col_2 <= row_2
        for i in range(2):
            near = pl.ds(pl.multiple_of(b * PAIR + i * HEAD, 128), HEAD)
            far = pl.ds(pl.multiple_of(quart + b * PAIR + i * HEAD, 128), HEAD)
            v_at = pl.ds(pl.multiple_of(lax.rem(b, 2) * PAIR + i * HEAD, 128), HEAD)
            q = pre[t, :, pl.ds(i * HEAD, HEAD)]
            s_a = lax.dot_general(q, kc[:, near], dims_t, preferred_element_type=F32)
            s_b = lax.dot_general(q, kc[:, far], dims_t, preferred_element_type=F32)
            s_n = lax.dot_general(q, pre[t, :, pl.ds(PAIR + i * HEAD, HEAD)], dims_t, preferred_element_type=F32)
            s_n = jnp.where(visible, s_n, -jnp.inf)
            peak = jnp.maximum(jnp.maximum(jnp.max(s_a, axis=1, keepdims=True), jnp.max(s_b, axis=1, keepdims=True)),
                               jnp.max(s_n, axis=1, keepdims=True))
            p_a, p_b, p_n = (jnp.exp2((s - peak) * scale) for s in (s_a, s_b, s_n))
            total_p = (jnp.sum(p_a, axis=1, keepdims=True) + jnp.sum(p_b, axis=1, keepdims=True)
                       + jnp.sum(p_n, axis=1, keepdims=True))
            acc = jnp.dot(p_a.astype(BF16), vc[:, near], preferred_element_type=F32)
            acc = acc + jnp.dot(p_b.astype(BF16), vc[:, far], preferred_element_type=F32)
            acc = acc + jnp.dot(p_n.astype(BF16), pre[vt, :, v_at], preferred_element_type=F32)
            opair[:, pl.ds(i * HEAD, HEAD)] = (acc * (1.0 / total_p)).astype(BF16)

    def o2_piece(b, from_chip):
        return obuf.at[:, pl.ds(pl.multiple_of(from_chip * quart + b * PAIR, 128), PAIR)]

    def o2_far(b):
        return obuf.at[:, pl.ds(pl.multiple_of(half + b * PAIR, 128), PAIR)]

    def o2_copy(b):
        return remote(o2_far(b), o2_piece(b, chip), osend.at[b], orecv.at[b], peer)

    def append2(b):
        to_at = pl.ds(pl.multiple_of(own2 + b * PAIR, 128), PAIR)
        v_at = pl.ds(pl.multiple_of(lax.rem(b, 2) * PAIR, 128), PAIR)
        mine = pl.ds(pl.multiple_of(chip_rows + my_rows, 16), rows)
        others = pl.ds(pl.multiple_of(chip_rows + other_rows, 16), rows)
        for kv, (t, at, dst) in enumerate(((qk_tile(b), pl.ds(PAIR, PAIR), k2_out), (3 * (b // 2), v_at, v2_out))):
            pltpu.make_async_copy(pre.at[t, mine, at], dst.at[:, to_at], a2send.at[2 * kv]).start()
            remote(pre.at[t, others, at], dst.at[:, to_at], a2send.at[2 * kv + 1], a2recv.at[kv], partner).start()

    @pl.loop(0, qkv2)
    def _(t):
        s = base2 + t

        @pl.when(t == qkv2 - 2)
        def _():
            at = wring.at[lax.rem(s, SLOTS), :, pl.ds(0, PAIR)]
            pltpu.make_async_copy(at, at, wsem.at[lax.rem(s, SLOTS)]).wait()

        @pl.when(t != qkv2 - 2)
        def _():
            wait_tile(s)

        raw = jnp.dot(nbuf[...], wring[lax.rem(s, SLOTS)], preferred_element_type=F32)
        start_tile(s + SLOTS, base2 + SLOTS, base2 + qkv2 + SLOTS)

        @pl.when(lax.rem(t, 3) == 0)
        def _():
            pre[t] = raw.astype(BF16)

        @pl.when(lax.rem(t, 3) != 0)
        def _():
            b = t - 1 - t // 3
            head = own2 // HEAD + 2 * b
            all_rows = pl.ds(0, 2 * crows)
            pre[t, :, pl.ds(0, PAIR)] = biased_rope(raw[:, :PAIR], 2, head, all_rows, 2)
            pre[t, :, pl.ds(PAIR, PAIR)] = biased_rope(raw[:, PAIR:], 3, head, all_rows, 2)

            @pl.when(b == 0)
            def _():
                for kv in range(2):
                    for kind in range(2):
                        cache2_copy(kv, kind).wait()

            for kv in range(2):
                for kind in (2, 3):
                    cache2_copy(kv, kind, b).wait_recv()
            attend2(b)
            obuf[:, pl.ds(pl.multiple_of(chip * quart + b * PAIR, 128), PAIR)] = opair[pl.ds(chip_rows, crows), :]
            obuf[:, pl.ds(pl.multiple_of(half + b * PAIR, 128), PAIR)] = opair[pl.ds(far_rows, crows), :]
            o2_copy(b).start()
            append2(b)

    @pl.loop(0, blocks)
    def _(b):
        remote(o2_far(b), o2_piece(b, 1 - chip), osend.at[b], orecv.at[b], peer).wait_recv()

    def y_copy(b):
        return remote(o_send.at[b], o_recv.at[b], qsend.at[b], qrecv.at[b], partner)

    @pl.loop(0, blocks)
    def _(b):
        slot = wait_tile(base2 + qkv2 + b)
        for i in range(2):
            y = jnp.dot(obuf[:, :half], wring[slot, i * half:(i + 1) * half, :], preferred_element_type=F32)
            at = pl.ds(i * rows, rows)
            for j in range(PER_BLOCK):
                lanes = pl.ds(j * HEAD, HEAD)
                st_loc[j] = y[:, j * HEAD:(j + 1) * HEAD]
                o_send[b, at, lanes] = st_loc[j, pl.ds(other_rows, rows), :]
                o_loc[b, at, lanes] = st_loc[j, pl.ds(my_rows, rows), :]
        y_copy(b).start()

    @pl.loop(0, blocks)
    def _(b):
        y_copy(b).wait_recv()
        for i in range(2):
            at = pl.ds(i * rows, rows)
            ybuf[:, pl.ds(pl.multiple_of(b * 2 * TILE + i * TILE, 128), TILE)] = (o_loc[b, at, :] + o_recv[b, at, :]).astype(BF16)

    y_copies = [pltpu.make_async_copy(ybuf, y_out, gsem.at[1])]
    for c in y_copies:
        c.start()

    @pl.loop(0, blocks)
    def _(b):
        y_copy(b).wait_send()
        o2_copy(b).wait_send()
        remote(g_piece(b, chip_rows), g_piece(b, chip_rows), gxs.at[b], gxr.at[b], peer).wait_send()

    for kv, dst in enumerate((k2_out, v2_out)):
        ref = dst.at[:, pl.ds(0, half)]
        pltpu.make_async_copy(ref, ref, a2send.at[2 * kv]).wait()
        remote(ref, ref, a2send.at[2 * kv + 1], a2recv.at[kv], partner).wait_send()
        remote(ref, ref, a2send.at[2 * kv + 1], a2recv.at[kv], partner).wait_recv()
        for kind in (2, 3):
            cache2_copy(kv, kind).wait_send()
    for ref, sem in ((y_out, 1), (g_out, 0)):
        pltpu.make_async_copy(ref, ref, gsem.at[sem]).wait()


def deliver(*refs):
    for i in range(6):
        src, dst = refs[i], refs[6 + i]
        dst[...] = src[...] if i < 2 else pltpu.einshape("t(hd)->thd", src[...], d=HEAD)


def solution(mesh):
    rows_spec = P(('dp', 'cp'), None)
    cache_spec = P(('dp', 'cp'), None, None)
    mat_spec = P(None, None)
    vec_spec = P(None)
    layer_specs = (cache_spec, cache_spec, mat_spec, vec_spec, mat_spec, vec_spec, mat_spec, mat_spec)
    in_specs = (rows_spec,) + layer_specs + (mat_spec, mat_spec, mat_spec) + layer_specs
    out_specs = (rows_spec, rows_spec, cache_spec, cache_spec, cache_spec, cache_spec)

    def forward(x_in, cache_k1, cache_v1, w_q1, b_q1, w_k1, b_k1, w_v1, w_o1, w_gate, w_up, w_down, cache_k2, cache_v2, w_q2, b_q2, w_k2, b_k2, w_v2, w_o2):
        rows, d_model = x_in.shape
        cache_rows, heads, head_dim = cache_k1.shape
        ff = w_gate.shape[1]
        half = d_model // 2
        blocks = half // TILE
        crows = 2 * rows
        cos_t, sin_t = rope_tables(4 * cache_rows + np.arange(2 * crows), head_dim)
        bias = [v.reshape(heads, head_dim) for v in (b_q1, b_k1, b_q2, b_k2)]

        any_spec = pl.BlockSpec(memory_space=pl.ANY)
        vmem_spec = pl.BlockSpec(memory_space=pltpu.VMEM)
        row_out = jax.ShapeDtypeStruct((rows, d_model), BF16)
        dma = pltpu.SemaphoreType.DMA
        out = pl.pallas_call(
            functools.partial(body, (d_model, ff, rows, cache_rows)),
            out_shape=[row_out] * 6 + [jax.ShapeDtypeStruct((cache_rows, d_model), BF16)] * 2,
            in_specs=[vmem_spec] * 6 + [any_spec] * 16,
            out_specs=[any_spec] * 8,
            scratch_shapes=[
                pltpu.VMEM((SLOTS, d_model, TILE), BF16),
                pltpu.VMEM((2 * crows, d_model), BF16),
                pltpu.VMEM((2 * crows, d_model), BF16),
                pltpu.VMEM((crows, ff), BF16),
                pltpu.VMEM((2 * blocks, 2 * crows, TILE), BF16),
                pltpu.VMEM((2 * cache_rows, half), BF16),
                pltpu.VMEM((2 * cache_rows, half), BF16),
                pltpu.VMEM((blocks, crows, TILE), F32),
                pltpu.VMEM((blocks, crows, TILE), F32),
                pltpu.VMEM((blocks, crows, TILE), F32),
                pltpu.VMEM((crows, d_model), BF16),
                pltpu.VMEM((2 * crows, TILE // 2), BF16),
                pltpu.VMEM((blocks, crows, HEAD), F32),
                pltpu.VMEM((blocks, 8, HEAD), F32),
                pltpu.VMEM((blocks, 8, HEAD), F32),
                pltpu.VMEM((4, heads, head_dim), F32),
                dma((SLOTS,)), dma((3,)), dma((4,)), dma((8,)), dma((8, 6)),
                dma((blocks,)), dma((blocks,)), dma((blocks,)), dma((blocks,)), dma((blocks,)), dma((blocks,)),
                dma((5,)), dma((5,)), dma((6,)), dma((2,)),
                dma((blocks,)), dma((blocks,)), dma((4,)), dma((2,)),
                dma((blocks,)), dma((blocks,)), dma((2,)), pltpu.SemaphoreType.REGULAR,
                pltpu.VMEM((4, cache_rows, 8, head_dim), BF16), dma((4,)), dma((2,)),
            ],
            compiler_params=pltpu.CompilerParams(
                collective_id=0, has_side_effects=True, vmem_limit_bytes=67043328),
        )(cos_t, sin_t, *bias, x_in, cache_k1, cache_v1, cache_k2, cache_v2,
          w_q1, w_k1, w_v1, w_o1, w_gate, w_up, w_down, w_q2, w_k2, w_v2, w_o2)
        steps = 4
        step_rows = pl.BlockSpec((rows // steps, d_model), lambda i: (i, 0))
        step_heads = pl.BlockSpec((rows // steps, heads, head_dim), lambda i: (i, 0, 0))
        head_out = jax.ShapeDtypeStruct((rows, heads, head_dim), BF16)
        return pl.pallas_call(
            deliver,
            grid=(steps,),
            out_shape=[row_out] * 2 + [head_out] * 4,
            in_specs=[step_rows] * 6,
            out_specs=[step_rows] * 2 + [step_heads] * 4,
        )(*out[:6])

    return jax.shard_map(forward, mesh=mesh, in_specs=in_specs, out_specs=out_specs, check_vma=False)
```

```python
import functools
import math

import jax
import jax.numpy as jnp
import numpy as np
from jax import lax
from jax.experimental import pallas as pl
from jax.experimental.pallas import tpu as pltpu
from jax.sharding import PartitionSpec as P

ROPE_THETA = 500000.0
NORM_EPS = 1e-5
MESH = pl.DeviceIdType.MESH
F32 = jnp.float32
BF16 = jnp.bfloat16

TILE = 512
HEAD = 128
PER_BLOCK = TILE // HEAD
SLOTS = 7


def rope_tables(positions, head_dim):
    half_dim = head_dim // 2
    inv_freq = (1.0 / (ROPE_THETA ** (np.arange(half_dim, dtype=np.float32) * np.float32(2.0 / head_dim)))).astype(np.float32)
    angles = positions.astype(np.float32)[:, None] * inv_freq[None, :]
    cos_t, sin_t = np.cos(angles), np.sin(angles)
    return np.concatenate([cos_t, cos_t], axis=1), np.concatenate([-sin_t, sin_t], axis=1)


def body(dims, cos_ref, sin_ref, bq1, bk1, bq2, bk2, x_hbm, raw_k1, raw_v1, raw_k2, raw_v2, wq1, wk1, wv1, wo1, w_gate, w_up, w_down,
         wq2, wk2, wv2, wo2, g_out, y_out, k1_out, v1_out, k2_out, v2_out, ck2, cv2,
         wring, nbuf, gbuf, ebuf, pre, kc, vc, o_loc, o_send, o_recv, obuf, opair,
         st_loc, st_send, st_recv, bias32,
         wsem, xsem, csem, c2send, c2recv, qsend, qrecv, osend, orecv, ssend, srecv, dsend, drecv, asem, gsem,
         gxs, gxr, a2send, a2recv, hys, hyr, esem, yfree, rawbuf, psem, fsem):
    d_model, ff, rows, cache_rows = dims
    half = d_model // 2
    ffh = ff // 2
    ffc = ff // 3
    third = ffc // 2
    part = third // (TILE // 2)
    blocks = half // TILE
    ffn = ffh // (TILE // 2)
    crows = 2 * rows
    quart = half // 2
    ybuf = nbuf.at[pl.ds(0, rows), :]
    me = lax.axis_index("cp")
    core = lax.rem(me, 2)
    chip = me // 2
    partner = me + 1 - 2 * core
    peer = lax.rem(me + 2, 4)
    diag = 3 - me
    dp = lax.axis_index("dp")
    side_y = 1 - dp
    chip_rows = pl.multiple_of(chip * crows, 16)
    xin = hbuf = gbuf.at[pl.ds(pl.multiple_of(chip * crows, 16), crows), :]
    far_rows = pl.multiple_of((1 - chip) * crows, 16)
    my_cols = pl.multiple_of(core * half, 128)
    my_rows = pl.multiple_of(core * rows, 16)
    other_rows = pl.multiple_of((1 - core) * rows, 16)
    other_cols = pl.multiple_of((1 - core) * half, 128)

    def col(b):
        return pl.multiple_of(core * half + b * TILE, 128)

    attn_tiles = 4 * blocks
    base1 = 0
    base_up = attn_tiles
    base_down = base_up + 2 * part
    base_x = base_down + 3 * blocks
    base2 = base_x + blocks
    qkv2 = 8

    def start_full(w, b, slot):
        pltpu.make_async_copy(w.at[:, pl.ds(col(b), TILE)], wring.at[slot], wsem.at[slot]).start()

    def mlp_cols(tile):
        return pl.ds(pl.multiple_of(core * ffh + tile * (TILE // 2), 128), TILE // 2)

    def shared_tile(n):
        return part + dp * part + n

    def start_mlp(tile, slot):
        at = mlp_cols(tile)
        pltpu.make_async_copy(w_gate.at[:, at], wring.at[slot, :, pl.ds(0, TILE // 2)], wsem.at[slot]).start()
        pltpu.make_async_copy(w_up.at[:, at], wring.at[slot, :, pl.ds(TILE // 2, TILE // 2)], wsem.at[slot]).start()

    def start_down(b, chunk, slot):
        for i in range(2):
            pltpu.make_async_copy(
                w_down.at[pl.ds(pl.multiple_of(i * ffh + chunk * third, 16), third), pl.ds(col(b), TILE)],
                wring.at[slot, pl.ds(i * third, third), :], wsem.at[slot]).start()

    loop_end = 3 * (blocks - 1) + 1

    def attn_segments(base, wq, wk, wv, wo):
        return [
            (base, base + 1, lambda r, slot: start_full(wq, 0, slot), None),
            (base + 1, base + loop_end, lambda r, slot: start_full(wq, r // 3 + 1, slot), 0),
            (base + 1, base + loop_end, lambda r, slot: start_full(wk, r // 3, slot), 1),
            (base + 1, base + loop_end, lambda r, slot: start_full(wv, r // 3, slot), 2),
            (base + loop_end, base + loop_end + 1, lambda r, slot: start_full(wk, blocks - 1, slot), None),
            (base + loop_end + 1, base + loop_end + 2, lambda r, slot: start_full(wv, blocks - 1, slot), None),
            (base + loop_end + 2, base + attn_tiles, lambda r, slot: start_full(wo, r, slot), None),
        ]

    PAIR = TILE // 2
    own2 = core * half + chip * quart

    def start_v2(t, slot):
        @pl.when(t < qkv2 - 2)
        def _():
            pltpu.make_async_copy(wv2.at[:, pl.ds(pl.multiple_of(own2 + (t // 3) * TILE, 128), TILE)], wring.at[slot],
                                  wsem.at[slot]).start()

        @pl.when(t >= qkv2 - 2)
        def _():
            pltpu.make_async_copy(wv2.at[:, pl.ds(pl.multiple_of(own2 + (t // 3) * TILE, 128), PAIR)],
                                  wring.at[slot, :, pl.ds(0, PAIR)], wsem.at[slot]).start()

    def start_qk2(t, slot):
        at = pl.ds(pl.multiple_of(own2 + (t - 1 - t // 3) * PAIR, 128), PAIR)
        pltpu.make_async_copy(wq2.at[:, at], wring.at[slot, :, pl.ds(0, PAIR)], wsem.at[slot]).start()
        pltpu.make_async_copy(wk2.at[:, at], wring.at[slot, :, pl.ds(PAIR, PAIR)], wsem.at[slot]).start()

    other2 = core * half + (1 - chip) * quart

    def start_kv_other(b, slot):
        at = pl.ds(pl.multiple_of(other2 + b * PAIR, 128), PAIR)
        pltpu.make_async_copy(wk2.at[:, at], wring.at[slot, :, pl.ds(0, PAIR)], wsem.at[slot]).start()
        pltpu.make_async_copy(wv2.at[:, at], wring.at[slot, :, pl.ds(PAIR, PAIR)], wsem.at[slot]).start()

    def start_wo2(b, slot):
        for i in range(2):
            pltpu.make_async_copy(
                wo2.at[pl.ds(my_cols, half), pl.ds(pl.multiple_of(b * 2 * TILE + i * TILE, 128), TILE)],
                wring.at[slot, pl.ds(i * half, half), :], wsem.at[slot]).start()

    segments = attn_segments(base1, wq1, wk1, wv1, wo1) + [
        (base_up, base_up + part, start_mlp, None),
        (base_up + part, base_down, lambda r, slot: start_mlp(shared_tile(r), slot), None),
        (base_down, base_down + blocks, lambda r, slot: start_down(r, 0, slot), None),
        (base_down + blocks, base_x, lambda r, slot: start_down(r // 2, 1 + r % 2 if isinstance(r, int) else 1 + lax.rem(r, 2), slot), None),
        (base_x, base2, start_kv_other, None),
        (base2, base2 + qkv2, start_v2, 0),
        (base2, base2 + qkv2, start_qk2, 1),
        (base2, base2 + qkv2, start_qk2, 2),
        (base2 + qkv2, base2 + qkv2 + blocks, start_wo2, None),
    ]

    def start_tile(s, lo, hi):
        slot = lax.rem(s, SLOTS) if not isinstance(s, int) else s % SLOTS
        for a, b, fn, phase in segments:
            if b <= lo or a >= hi:
                continue
            if isinstance(s, int):
                if a <= s < b and (phase is None or (s - a) % 3 == phase):
                    fn(s - a, slot)
                continue
            cond = (s >= a) & (s < b)
            if phase is not None:
                cond = cond & (lax.rem(s - a + 3, 3) == phase)

            @pl.when(cond)
            def _(a=a, fn=fn):
                fn(s - a, slot)

    def wait_tile(s, depth=None):
        slot = lax.rem(s, SLOTS) if not isinstance(s, int) else s % SLOTS
        ref = wring.at[slot] if depth is None else wring.at[slot, pl.ds(0, depth), :]
        pltpu.make_async_copy(ref, ref, wsem.at[slot]).wait()
        return slot

    def remote(src, dst, send, recv, who):
        return pltpu.make_async_remote_copy(src_ref=src, dst_ref=dst, send_sem=send, recv_sem=recv,
                                            device_id={"cp": who}, device_id_type=MESH)

    def remote_y(src, dst, send, recv):
        return pltpu.make_async_remote_copy(src_ref=src, dst_ref=dst, send_sem=send, recv_sem=recv,
                                            device_id={"dp": side_y}, device_id_type=MESH)

    HEADS8 = 8
    WIDE = HEADS8 * HEAD
    groups = d_model // WIDE

    def raw_copy(raw, j, slot):
        return pltpu.make_async_copy(raw.at[:, pl.ds(pl.multiple_of(j * HEADS8, HEADS8), HEADS8), :], rawbuf.at[slot],
                                     psem.at[slot])

    def flat_wait(flat, slot):
        ref = flat.at[:, pl.ds(0, WIDE)]
        pltpu.make_async_copy(ref, ref, fsem.at[slot]).wait()

    def flatten_heads(flat, j, slot):
        for i in range(cache_rows // crows):
            at = pl.ds((slot * 2 + i) * WIDE, WIDE)
            ebuf[:, at] = pltpu.einshape("thd->t(hd)", rawbuf[slot, i * crows:(i + 1) * crows])
            pltpu.make_async_copy(ebuf.at[:, at], flat.at[pl.ds(i * crows, crows), pl.ds(pl.multiple_of(j * WIDE, 128), WIDE)],
                                  fsem.at[slot]).start()

    layer1 = ((raw_k1, kc), (raw_v1, vc))
    layer2 = ((raw_k2, ck2), (raw_v2, cv2))
    for j in range(2):
        for kv in range(2):
            raw_copy(layer1[kv][0], j, 2 * j + kv).start()
    for s in range(3):
        start_tile(s, s, s + 1)

    barrier = pltpu.get_barrier_semaphore()
    for who in (partner, peer, diag):
        pl.semaphore_signal(barrier, inc=1, device_id={"cp": who}, device_id_type=MESH)
    pl.semaphore_signal(barrier, inc=1, device_id={"dp": side_y}, device_id_type=MESH)
    pl.semaphore_wait(barrier, 4)

    x_loc = pltpu.make_async_copy(x_hbm, xin.at[pl.ds(my_rows, rows)], xsem.at[0])
    x_rem = remote(x_hbm, xin.at[pl.ds(my_rows, rows)], xsem.at[1], xsem.at[2], partner)
    x_rem.start()
    x_loc.start()

    crow = pl.ds(pl.multiple_of(core * cache_rows, 16), cache_rows)
    cache1 = [remote(c.at[crow], c.at[crow], csem.at[2 * kv], csem.at[2 * kv + 1], partner) for kv, c in enumerate((kc, vc))]

    def place_cache1():
        start_tile(3, 3, 4)

        @pl.loop(0, groups)
        def _(j):
            for kv, (raw, cache) in enumerate(layer1):
                slot = 2 * lax.rem(j, 2) + kv
                raw_copy(raw, j, slot).wait()
                for i in range(cache_rows // crows):
                    rows_at = pl.ds(pl.multiple_of(core * cache_rows + i * crows, 16), crows)
                    vals = pltpu.einshape("thd->t(hd)", rawbuf[slot, i * crows:(i + 1) * crows])
                    for part_i in range(WIDE // TILE):
                        piece = vals[:, part_i * TILE:(part_i + 1) * TILE]
                        block = 2 * j + part_i
                        owner = block // blocks
                        block = block - owner * blocks
                        to_at = pl.ds(pl.multiple_of(block * TILE, 128), TILE)

                        @pl.when(owner == core)
                        def _():
                            cache[rows_at, to_at] = piece

                        @pl.when(owner != core)
                        def _():
                            at = pl.ds(pl.multiple_of(((block * 2 + kv) * 2 + i) * TILE, 128), TILE)
                            ebuf[:, at] = piece
                            remote(ebuf.at[:, at], cache.at[rows_at, to_at], csem.at[2 * kv], csem.at[2 * kv + 1], partner).start()

                @pl.when(j < groups - 2)
                def _():
                    raw_copy(raw, j + 2, slot).start()

        for slot, (raw, flat) in enumerate(layer2):
            raw_copy(raw, 0, slot).start()
        for s in range(4, SLOTS):
            start_tile(s, s, s + 1)

    for i, ref in enumerate((bq1, bk1, bq2, bk2)):
        bias32[i] = ref[...].astype(F32)
    x_loc.wait()
    x_rem.wait()

    def biased_rope(vals, bias_row, first_head, table_at, n):
        parts = []
        cos_t, sin_t = cos_ref[table_at, :], sin_ref[table_at, :]
        for i in range(n):
            seg = vals[:, i * HEAD:(i + 1) * HEAD] + bias32[bias_row, pl.ds(first_head + i, 1), :]
            seg = seg.astype(BF16).astype(F32)
            parts.append((seg * cos_t + pltpu.roll(seg, HEAD // 2, 1) * sin_t).astype(BF16))
        return jnp.concatenate(parts, axis=1)

    def norm(src, dst, first, count):
        step = 16

        @pl.loop(0, count // step)
        def _(i):
            at = pl.ds(pl.multiple_of(first + i * step, step), step)
            wide = src[at, :].astype(F32)
            dst[at, :] = (wide * lax.rsqrt(jnp.mean(wide * wide, axis=-1, keepdims=True) + NORM_EPS)).astype(BF16)

    row_i = lax.broadcasted_iota(jnp.int32, (2 * crows, crows), 0)
    col_i = lax.broadcasted_iota(jnp.int32, (2 * crows, crows), 1)
    far_lim = jnp.where(chip == 0, crows, -1)
    scale = HEAD ** -0.5 * math.log2(math.e)

    def attend(b):
        lane = lax.broadcasted_iota(jnp.int32, (2 * crows, HEAD), 1)
        visible = col_i <= jnp.where(row_i < crows, row_i, far_lim)
        stats = jnp.zeros((2 * crows, HEAD), F32)
        dims_t = (((1,), (1,)), ((), ()))
        for i in range(PER_BLOCK):
            at = pl.ds(i * HEAD, HEAD)
            cat = pl.ds(pl.multiple_of(b * TILE + i * HEAD, 128), HEAD)
            q = pre[b, :, at]
            s_old = lax.dot_general(q, kc[:, cat], dims_t, preferred_element_type=F32)
            s_new = lax.dot_general(q, pre[blocks + b, pl.ds(0, crows), at], dims_t, preferred_element_type=F32)
            s_new = jnp.where(visible, s_new, -jnp.inf)
            peak = jnp.maximum(jnp.max(s_old, axis=1, keepdims=True), jnp.max(s_new, axis=1, keepdims=True))
            p_old = jnp.exp2((s_old - peak) * scale)
            p_new = jnp.exp2((s_new - peak) * scale)
            total_p = jnp.sum(p_old, axis=1, keepdims=True) + jnp.sum(p_new, axis=1, keepdims=True)
            acc = jnp.dot(p_old.astype(BF16), vc[:, cat], preferred_element_type=F32)
            acc = acc + jnp.dot(p_new.astype(BF16), pre[blocks + b, pl.ds(crows, crows), at], preferred_element_type=F32)
            o_loc[b, :, at] = acc[:crows]
            o_send[b, :, at] = acc[crows:]
            stats = jnp.where(lane == 2 * i, peak, stats)
            stats = jnp.where(lane == 2 * i + 1, total_p, stats)
        st_loc[b] = stats[:crows]
        st_send[b] = stats[crows:].T[:8, :]

    def q_copy(b):
        return remote(pre.at[b, pl.ds(0, crows), :], pre.at[b, pl.ds(crows, crows), :], qsend.at[b], qrecv.at[b], peer)

    def o_copy(b):
        return remote(o_send.at[b], o_recv.at[b], osend.at[b], orecv.at[b], peer)

    def s_copy(b):
        return remote(st_send.at[b], st_recv.at[b], ssend.at[b], srecv.at[b], peer)

    PIECE = TILE // 2

    def cache2_copy(kv, kind, b=None):
        src, dst = ((ck2, kc), (cv2, vc))[kv]
        who, to_core, to_chip = ((None, core, chip), (partner, 1 - core, chip), (peer, core, 1 - chip),
                                 (diag, 1 - core, 1 - chip))[kind]
        off, width, sem = (0, quart, 0) if b is None else (b * PIECE, PIECE, 1 + b)
        side = 0 if kind < 2 else quart
        from_at = pl.ds(pl.multiple_of(to_core * half + to_chip * quart + off, 128), width)
        to = dst.at[pl.ds(pl.multiple_of(core * cache_rows, 16), cache_rows), pl.ds(pl.multiple_of(side + off, 128), width)]
        i = 4 * kv + kind
        if kind == 0:
            return pltpu.make_async_copy(src.at[:, from_at], to, c2send.at[i])
        return remote(src.at[:, from_at], to, c2send.at[i], c2recv.at[i, sem], who)

    def head_of(b):
        return core * (half // HEAD) + b * PER_BLOCK

    def attention(layer_in, base, bias_row, caches, k_out, v_out):
        def q_step(b, s, lo, hi):
            slot = wait_tile(s)
            raw = jnp.dot(layer_in[...], wring[slot], preferred_element_type=F32)
            start_tile(s + SLOTS, lo + SLOTS, hi + SLOTS)
            pre[b, pl.ds(0, crows), :] = biased_rope(raw, bias_row, head_of(b), pl.ds(chip_rows, crows), PER_BLOCK)
            q_copy(b).start()

        q_step(0, base, base, base + 1)
        place_cache1()

        @pl.loop(0, blocks)
        def _(b):
            has_q = (2 * blocks - 3 - b) // (blocks - 1)
            s = base + 1 + 3 * b

            @pl.when(b < blocks - 1)
            def _():
                q_step(b + 1, s, base + 1, base + loop_end)

            s = s + has_q
            slot = wait_tile(s)
            raw = jnp.dot(layer_in[...], wring[slot], preferred_element_type=F32)
            start_tile(s + SLOTS, base + 2 + SLOTS, base + loop_end + 2 + SLOTS)
            pre[blocks + b, pl.ds(0, crows), :] = biased_rope(raw, bias_row + 1, head_of(b), pl.ds(chip_rows, crows), PER_BLOCK)
            s = s + 1
            slot = wait_tile(s)
            vals = jnp.dot(layer_in[...], wring[slot], preferred_element_type=F32).astype(BF16)
            start_tile(s + SLOTS, base + 3 + SLOTS, base + loop_end + 2 + SLOTS)
            pre[blocks + b, pl.ds(crows, crows), :] = vals

            @pl.when(b == 0)
            def _():
                for c in caches:
                    c.wait()

            q_copy(b).wait_recv()
            attend(b)
            for part, dst, k in ((0, k_out, 0), (crows, v_out, 3)):
                pltpu.make_async_copy(pre.at[blocks + b, pl.ds(part + my_rows, rows), :], dst.at[:, pl.ds(col(b), TILE)], asem.at[k]).start()
                remote(pre.at[blocks + b, pl.ds(part + other_rows, rows), :], dst.at[:, pl.ds(col(b), TILE)], asem.at[k + 1],
                       asem.at[k + 2], partner).start()
            o_copy(b).start()
            s_copy(b).start()
            for slot, (raw, flat) in enumerate(layer2):
                raw_copy(raw, b, slot).wait()

                @pl.when(b > 0)
                def _():
                    flat_wait(flat, slot)

                flatten_heads(flat, b, slot)

                @pl.when(b < blocks - 1)
                def _():
                    raw_copy(raw, b + 1, slot).start()

        for slot, (raw, flat) in enumerate(layer2):
            flat_wait(flat, slot)

        @pl.loop(0, blocks)
        def _(b):
            o_copy(b).wait_recv()
            s_copy(b).wait_recv()

            @pl.when(b == blocks - 1)
            def _():
                for piece in range(3):
                    for kv in range(2):
                        cache2_copy(kv, 2, piece).start()

            far = jnp.concatenate([st_recv[b], jnp.zeros((HEAD - 8, HEAD), F32)], axis=0).T
            near = st_loc[b]
            for i in range(PER_BLOCK):
                at = pl.ds(i * HEAD, HEAD)
                m_a, l_a = near[:, 2 * i:2 * i + 1], near[:, 2 * i + 1:2 * i + 2]
                m_b, l_b = far[:, 2 * i:2 * i + 1], far[:, 2 * i + 1:2 * i + 2]
                peak = jnp.maximum(m_a, m_b)
                w_a, w_b = jnp.exp2((m_a - peak) * scale), jnp.exp2((m_b - peak) * scale)
                norm_l = 1.0 / (l_a * w_a + l_b * w_b)
                o = o_loc[b, :, at] * (w_a * norm_l) + o_recv[b, :, at] * (w_b * norm_l)
                obuf[:, pl.ds(pl.multiple_of(core * half + b * TILE + i * HEAD, 128), HEAD)] = o.astype(BF16)
            piece = obuf.at[:, pl.ds(col(b), TILE)]
            remote(piece, piece, dsend.at[0], drecv.at[0], partner).start()

        mine = obuf.at[:, pl.ds(my_cols, half)]
        theirs = obuf.at[:, pl.ds(other_cols, half)]
        remote(mine, theirs, dsend.at[0], drecv.at[0], partner).wait_send()
        remote(mine, theirs, dsend.at[0], drecv.at[0], partner).wait_recv()

        @pl.loop(0, blocks)
        def _(b):
            q_copy(b).wait_send()
            o_copy(b).wait_send()
            s_copy(b).wait_send()

        for dst, k in ((k_out, 0), (v_out, 3)):
            to_me = dst.at[:, pl.ds(my_cols, half)]
            to_me2 = dst.at[:, pl.ds(other_cols, half)]
            pltpu.make_async_copy(to_me, to_me, asem.at[k]).wait()
            remote(to_me, to_me2, asem.at[k + 1], asem.at[k + 2], partner).wait_send()
            remote(to_me, to_me2, asem.at[k + 1], asem.at[k + 2], partner).wait_recv()

    def both_wait(buf, sem, width, my_at, other_at):
        mine = buf.at[:, pl.ds(my_at, width)]
        theirs = buf.at[:, pl.ds(other_at, width)]
        remote(mine, theirs, dsend.at[sem], drecv.at[sem], partner).wait_send()
        remote(mine, theirs, dsend.at[sem], drecv.at[sem], partner).wait_recv()

    attention(xin, base1, 0, cache1, k1_out, v1_out)
    pl.semaphore_signal(yfree, inc=1, device_id={"dp": side_y}, device_id_type=MESH)

    def far_cache(b):
        for kv in range(2):
            for kind in (2, 3):
                cache2_copy(kv, kind, b).start()

    for b in range(3):
        for kv in range(2):
            cache2_copy(kv, 3, b).start()
    for kind in (1, 0):
        for kv in range(2):
            cache2_copy(kv, kind).start()

    pl.semaphore_wait(yfree, 1)

    def h_copy(b):
        return remote_y(hbuf.at[:, pl.ds(col(b), TILE)], pre.at[core * blocks + b, pl.ds(0, crows), :], hys.at[b], hyr.at[b])

    @pl.loop(0, blocks)
    def _(b):
        s = base1 + 3 * blocks + b
        slot = wait_tile(s)
        y = jnp.dot(obuf[...], wring[slot], preferred_element_type=F32).astype(BF16)
        start_tile(s + SLOTS, base1 + 3 * blocks + SLOTS, base_up + SLOTS)
        at = pl.ds(col(b), TILE)
        hbuf[:, at] = (xin[:, at].astype(F32) + y.astype(F32)).astype(BF16)
        h_copy(b).start()
        remote(hbuf.at[:, at], hbuf.at[:, at], dsend.at[1], drecv.at[1], partner).start()

    both_wait(hbuf, 1, half, my_cols, other_cols)
    norm(hbuf, nbuf, 0, crows)

    def glu(both):
        gate = both[:, :TILE // 2].astype(BF16).astype(F32)
        up = both[:, TILE // 2:].astype(BF16).astype(F32)
        return (jax.nn.silu(gate) * up).astype(BF16)

    @pl.loop(0, part)
    def _(n):
        s = base_up + n
        slot = wait_tile(s)
        both = jnp.dot(nbuf[pl.ds(0, crows), :], wring[slot], preferred_element_type=F32)
        start_tile(s + SLOTS, base_up + SLOTS, base_up + part + SLOTS)
        at = mlp_cols(n)
        ebuf[:, at] = glu(both)
        remote(ebuf.at[:, at], ebuf.at[:, at], dsend.at[2], drecv.at[2], partner).start()

    far_h = pre.at[pl.ds(core * blocks, blocks), pl.ds(0, crows), :]
    far_h_other = pre.at[pl.ds((1 - core) * blocks, blocks), pl.ds(0, crows), :]

    @pl.loop(0, blocks)
    def _(b):
        h_copy(b).wait_recv()
        h_copy(b).wait_send()

    remote(far_h, far_h, dsend.at[4], drecv.at[4], partner).start()
    remote(far_h, far_h, dsend.at[4], drecv.at[4], partner).wait_send()
    remote(far_h_other, far_h_other, dsend.at[4], drecv.at[4], partner).wait_recv()

    @pl.loop(0, crows // 16)
    def _(i):
        at = pl.ds(pl.multiple_of(i * 16, 16), 16)
        wide = [pre[j, at, :].astype(F32) for j in range(2 * blocks)]
        square = sum(jnp.sum(w * w, axis=-1, keepdims=True) for w in wide)
        inv = lax.rsqrt(square / d_model + NORM_EPS)
        for j in range(2 * blocks):
            nbuf[pl.ds(pl.multiple_of(crows + i * 16, 16), 16), pl.ds(j * TILE, TILE)] = (wide[j] * inv).astype(BF16)

    def e_return(n):
        return remote_y(pre.at[n, pl.ds(crows, crows), pl.ds(0, TILE // 2)], ebuf.at[:, mlp_cols(shared_tile(n))],
                        esem.at[0], esem.at[1])

    @pl.loop(0, part)
    def _(n):
        s = base_up + part + n
        slot = wait_tile(s)
        both = jnp.dot(nbuf[...], wring[slot], preferred_element_type=F32)
        start_tile(s + SLOTS, base_up + part + SLOTS, base_down + SLOTS)
        at = mlp_cols(shared_tile(n))
        mixed = glu(both)
        ebuf[:, at] = mixed[:crows]
        pre[n, pl.ds(crows, crows), pl.ds(0, TILE // 2)] = mixed[crows:]
        e_return(n).start()
        remote(ebuf.at[:, at], ebuf.at[:, at], dsend.at[2], drecv.at[2], partner).start()

    def returned(to_core):
        return ebuf.at[:, pl.ds(pl.multiple_of(to_core * ffh + (1 + side_y) * third, 128), third)]

    def partner_e_wait():
        some = ebuf.at[:, pl.ds(0, 2 * third)]
        remote(some, some, dsend.at[2], drecv.at[2], partner).wait_send()
        remote(some, some, dsend.at[2], drecv.at[2], partner).wait_recv()

    partner_e_wait()

    def down_dot(slot, chunk):
        out = None
        for i in range(2):
            at = pl.ds(pl.multiple_of(i * ffh + chunk * third, 128), third)
            term = jnp.dot(ebuf[:, at], wring[slot, i * third:(i + 1) * third, :], preferred_element_type=F32)
            out = term if out is None else out + term
        return out

    @pl.loop(0, blocks)
    def _(b):
        @pl.when(b == blocks - 2)
        def _():
            e_all = remote_y(returned(core), returned(core), esem.at[0], esem.at[1])
            e_all.wait_send()
            e_all.wait_recv()
            remote(returned(core), returned(core), dsend.at[1], drecv.at[1], partner).start()

        s = base_down + b
        slot = wait_tile(s, ffc)
        o_loc[b] = down_dot(slot, 0)
        start_tile(s + SLOTS, base_down + SLOTS, base_down + blocks + SLOTS)

    remote(returned(core), returned(core), dsend.at[1], drecv.at[1], partner).wait_send()
    remote(returned(1 - core), returned(1 - core), dsend.at[1], drecv.at[1], partner).wait_recv()

    def g_piece(b, first):
        return gbuf.at[pl.ds(first, crows), pl.ds(col(b), TILE)]

    @pl.loop(0, blocks)
    def _(b):
        at = pl.ds(col(b), TILE)
        down = o_loc[b]
        for k in range(2):
            s = base_down + blocks + 2 * b + k
            slot = wait_tile(s, ffc)
            down = down + down_dot(slot, 1 + k)
            start_tile(s + SLOTS, base_down + blocks + k + SLOTS, base_x - 1 + k + SLOTS)
        gbuf[pl.ds(chip_rows, crows), at] = (hbuf[:, at].astype(F32) + down).astype(BF16)
        piece = g_piece(b, chip_rows)
        remote(piece, piece, gxs.at[b], gxr.at[b], peer).start()
        remote(piece, piece, dsend.at[3], drecv.at[3], partner).start()

    def g_wait(first, sem):
        mine = gbuf.at[pl.ds(first, crows), pl.ds(my_cols, half)]
        theirs = gbuf.at[pl.ds(first, crows), pl.ds(other_cols, half)]
        remote(mine, theirs, dsend.at[sem], drecv.at[sem], partner).wait_send()
        remote(mine, theirs, dsend.at[sem], drecv.at[sem], partner).wait_recv()

    far_cache(3)
    far_cache(4)
    g_wait(chip_rows, 3)
    g_rows = pl.ds(pl.multiple_of(chip_rows + my_rows, 16), rows)
    g_copies = [pltpu.make_async_copy(gbuf.at[g_rows, :], g_out, gsem.at[0])]
    for c in g_copies:
        c.start()
    norm(gbuf, nbuf, chip_rows, crows)

    def g_forward(b):
        far = g_piece(b, far_rows)
        remote(far, far, gxs.at[b], gxr.at[b], peer).wait_recv()
        remote(far, far, dsend.at[0], drecv.at[0], partner).start()

    @pl.loop(0, blocks - 1)
    def _(b):
        g_forward(b)

    @pl.loop(0, blocks)
    def _(b):
        s = base_x + b
        slot = wait_tile(s)
        raw = jnp.dot(nbuf[pl.ds(chip_rows, crows), :], wring[slot], preferred_element_type=F32)
        start_tile(s + SLOTS, base_x + SLOTS, base2 + SLOTS)
        k_at = pl.ds(pl.multiple_of(b * TILE, 128), PAIR)
        v_at = pl.ds(pl.multiple_of(b * TILE + PAIR, 128), PAIR)
        ebuf[:, k_at] = biased_rope(raw[:, :PAIR], 3, other2 // HEAD + 2 * b, pl.ds(chip_rows, crows), 2)
        ebuf[:, v_at] = raw[:, PAIR:].astype(BF16)
        to_at = pl.ds(pl.multiple_of(other2 + b * PAIR, 128), PAIR)
        for kv, (at, dst) in enumerate(((k_at, k2_out), (v_at, v2_out))):
            pltpu.make_async_copy(ebuf.at[pl.ds(my_rows, rows), at], dst.at[:, to_at], a2send.at[2 * kv]).start()
            remote(ebuf.at[pl.ds(other_rows, rows), at], dst.at[:, to_at], a2send.at[2 * kv + 1], a2recv.at[kv], partner).start()

    g_forward(blocks - 1)
    g_wait(far_rows, 0)
    norm(gbuf, nbuf, far_rows, crows)

    heads2 = quart // HEAD
    row_2 = lax.broadcasted_iota(jnp.int32, (2 * crows, 2 * crows), 0)
    col_2 = lax.broadcasted_iota(jnp.int32, (2 * crows, 2 * crows), 1)

    def qk_tile(b):
        return b + 1 + b // 2

    def attend2(b):
        t = qk_tile(b)
        vt = 3 * (b // 2)
        dims_t = (((1,), (1,)), ((), ()))
        visible = col_2 <= row_2
        for i in range(2):
            near = pl.ds(pl.multiple_of(b * PAIR + i * HEAD, 128), HEAD)
            far = pl.ds(pl.multiple_of(quart + b * PAIR + i * HEAD, 128), HEAD)
            v_at = pl.ds(pl.multiple_of(lax.rem(b, 2) * PAIR + i * HEAD, 128), HEAD)
            q = pre[t, :, pl.ds(i * HEAD, HEAD)]
            s_a = lax.dot_general(q, kc[:, near], dims_t, preferred_element_type=F32)
            s_b = lax.dot_general(q, kc[:, far], dims_t, preferred_element_type=F32)
            s_n = lax.dot_general(q, pre[t, :, pl.ds(PAIR + i * HEAD, HEAD)], dims_t, preferred_element_type=F32)
            s_n = jnp.where(visible, s_n, -jnp.inf)
            peak = jnp.maximum(jnp.maximum(jnp.max(s_a, axis=1, keepdims=True), jnp.max(s_b, axis=1, keepdims=True)),
                               jnp.max(s_n, axis=1, keepdims=True))
            p_a, p_b, p_n = (jnp.exp2((s - peak) * scale) for s in (s_a, s_b, s_n))
            total_p = (jnp.sum(p_a, axis=1, keepdims=True) + jnp.sum(p_b, axis=1, keepdims=True)
                       + jnp.sum(p_n, axis=1, keepdims=True))
            acc = jnp.dot(p_a.astype(BF16), vc[:, near], preferred_element_type=F32)
            acc = acc + jnp.dot(p_b.astype(BF16), vc[:, far], preferred_element_type=F32)
            acc = acc + jnp.dot(p_n.astype(BF16), pre[vt, :, v_at], preferred_element_type=F32)
            opair[:, pl.ds(i * HEAD, HEAD)] = (acc * (1.0 / total_p)).astype(BF16)

    def o2_piece(b, from_chip):
        return obuf.at[:, pl.ds(pl.multiple_of(from_chip * quart + b * PAIR, 128), PAIR)]

    def o2_far(b):
        return obuf.at[:, pl.ds(pl.multiple_of(half + b * PAIR, 128), PAIR)]

    def o2_copy(b):
        return remote(o2_far(b), o2_piece(b, chip), osend.at[b], orecv.at[b], peer)

    def append2(b):
        to_at = pl.ds(pl.multiple_of(own2 + b * PAIR, 128), PAIR)
        v_at = pl.ds(pl.multiple_of(lax.rem(b, 2) * PAIR, 128), PAIR)
        mine = pl.ds(pl.multiple_of(chip_rows + my_rows, 16), rows)
        others = pl.ds(pl.multiple_of(chip_rows + other_rows, 16), rows)
        for kv, (t, at, dst) in enumerate(((qk_tile(b), pl.ds(PAIR, PAIR), k2_out), (3 * (b // 2), v_at, v2_out))):
            pltpu.make_async_copy(pre.at[t, mine, at], dst.at[:, to_at], a2send.at[2 * kv]).start()
            remote(pre.at[t, others, at], dst.at[:, to_at], a2send.at[2 * kv + 1], a2recv.at[kv], partner).start()

    @pl.loop(0, qkv2)
    def _(t):
        s = base2 + t

        @pl.when(t == qkv2 - 2)
        def _():
            at = wring.at[lax.rem(s, SLOTS), :, pl.ds(0, PAIR)]
            pltpu.make_async_copy(at, at, wsem.at[lax.rem(s, SLOTS)]).wait()

        @pl.when(t != qkv2 - 2)
        def _():
            wait_tile(s)

        raw = jnp.dot(nbuf[...], wring[lax.rem(s, SLOTS)], preferred_element_type=F32)
        start_tile(s + SLOTS, base2 + SLOTS, base2 + qkv2 + SLOTS)

        @pl.when(lax.rem(t, 3) == 0)
        def _():
            pre[t] = raw.astype(BF16)

        @pl.when(lax.rem(t, 3) != 0)
        def _():
            b = t - 1 - t // 3
            head = own2 // HEAD + 2 * b
            all_rows = pl.ds(0, 2 * crows)
            pre[t, :, pl.ds(0, PAIR)] = biased_rope(raw[:, :PAIR], 2, head, all_rows, 2)
            pre[t, :, pl.ds(PAIR, PAIR)] = biased_rope(raw[:, PAIR:], 3, head, all_rows, 2)

            @pl.when(b == 0)
            def _():
                for kv in range(2):
                    for kind in range(2):
                        cache2_copy(kv, kind).wait()

            for kv in range(2):
                for kind in (2, 3):
                    cache2_copy(kv, kind, b).wait_recv()
            attend2(b)
            obuf[:, pl.ds(pl.multiple_of(chip * quart + b * PAIR, 128), PAIR)] = opair[pl.ds(chip_rows, crows), :]
            obuf[:, pl.ds(pl.multiple_of(half + b * PAIR, 128), PAIR)] = opair[pl.ds(far_rows, crows), :]
            o2_copy(b).start()
            append2(b)

    @pl.loop(0, blocks)
    def _(b):
        remote(o2_far(b), o2_piece(b, 1 - chip), osend.at[b], orecv.at[b], peer).wait_recv()

    def y_copy(b):
        return remote(o_send.at[b], o_recv.at[b], qsend.at[b], qrecv.at[b], partner)

    @pl.loop(0, blocks)
    def _(b):
        slot = wait_tile(base2 + qkv2 + b)
        for i in range(2):
            y = jnp.dot(obuf[:, :half], wring[slot, i * half:(i + 1) * half, :], preferred_element_type=F32)
            at = pl.ds(i * rows, rows)
            for j in range(PER_BLOCK):
                lanes = pl.ds(j * HEAD, HEAD)
                st_loc[j] = y[:, j * HEAD:(j + 1) * HEAD]
                o_send[b, at, lanes] = st_loc[j, pl.ds(other_rows, rows), :]
                o_loc[b, at, lanes] = st_loc[j, pl.ds(my_rows, rows), :]
        y_copy(b).start()

    @pl.loop(0, blocks)
    def _(b):
        y_copy(b).wait_recv()
        for i in range(2):
            at = pl.ds(i * rows, rows)
            ybuf[:, pl.ds(pl.multiple_of(b * 2 * TILE + i * TILE, 128), TILE)] = (o_loc[b, at, :] + o_recv[b, at, :]).astype(BF16)

    y_copies = [pltpu.make_async_copy(ybuf, y_out, gsem.at[1])]
    for c in y_copies:
        c.start()

    @pl.loop(0, blocks)
    def _(b):
        y_copy(b).wait_send()
        o2_copy(b).wait_send()
        remote(g_piece(b, chip_rows), g_piece(b, chip_rows), gxs.at[b], gxr.at[b], peer).wait_send()

    for kv, dst in enumerate((k2_out, v2_out)):
        ref = dst.at[:, pl.ds(0, half)]
        pltpu.make_async_copy(ref, ref, a2send.at[2 * kv]).wait()
        remote(ref, ref, a2send.at[2 * kv + 1], a2recv.at[kv], partner).wait_send()
        remote(ref, ref, a2send.at[2 * kv + 1], a2recv.at[kv], partner).wait_recv()
        for kind in (2, 3):
            cache2_copy(kv, kind).wait_send()
    for ref, sem in ((y_out, 1), (g_out, 0)):
        pltpu.make_async_copy(ref, ref, gsem.at[sem]).wait()


def deliver(*refs):
    for i in range(6):
        src, dst = refs[i], refs[6 + i]
        dst[...] = src[...] if i < 2 else pltpu.einshape("t(hd)->thd", src[...], d=HEAD)


def solution(mesh):
    rows_spec = P(('dp', 'cp'), None)
    cache_spec = P(('dp', 'cp'), None, None)
    mat_spec = P(None, None)
    vec_spec = P(None)
    layer_specs = (cache_spec, cache_spec, mat_spec, vec_spec, mat_spec, vec_spec, mat_spec, mat_spec)
    in_specs = (rows_spec,) + layer_specs + (mat_spec, mat_spec, mat_spec) + layer_specs
    out_specs = (rows_spec, rows_spec, cache_spec, cache_spec, cache_spec, cache_spec)

    def forward(x_in, cache_k1, cache_v1, w_q1, b_q1, w_k1, b_k1, w_v1, w_o1, w_gate, w_up, w_down, cache_k2, cache_v2, w_q2, b_q2, w_k2, b_k2, w_v2, w_o2):
        rows, d_model = x_in.shape
        cache_rows, heads, head_dim = cache_k1.shape
        ff = w_gate.shape[1]
        half = d_model // 2
        blocks = half // TILE
        crows = 2 * rows
        cos_t, sin_t = rope_tables(4 * cache_rows + np.arange(2 * crows), head_dim)
        bias = [v.reshape(heads, head_dim) for v in (b_q1, b_k1, b_q2, b_k2)]

        any_spec = pl.BlockSpec(memory_space=pl.ANY)
        vmem_spec = pl.BlockSpec(memory_space=pltpu.VMEM)
        row_out = jax.ShapeDtypeStruct((rows, d_model), BF16)
        dma = pltpu.SemaphoreType.DMA
        out = pl.pallas_call(
            functools.partial(body, (d_model, ff, rows, cache_rows)),
            out_shape=[row_out] * 6 + [jax.ShapeDtypeStruct((cache_rows, d_model), BF16)] * 2,
            in_specs=[vmem_spec] * 6 + [any_spec] * 16,
            out_specs=[any_spec] * 8,
            scratch_shapes=[
                pltpu.VMEM((SLOTS, d_model, TILE), BF16),
                pltpu.VMEM((2 * crows, d_model), BF16),
                pltpu.VMEM((2 * crows, d_model), BF16),
                pltpu.VMEM((crows, ff), BF16),
                pltpu.VMEM((2 * blocks, 2 * crows, TILE), BF16),
                pltpu.VMEM((2 * cache_rows, half), BF16),
                pltpu.VMEM((2 * cache_rows, half), BF16),
                pltpu.VMEM((blocks, crows, TILE), F32),
                pltpu.VMEM((blocks, crows, TILE), F32),
                pltpu.VMEM((blocks, crows, TILE), F32),
                pltpu.VMEM((crows, d_model), BF16),
                pltpu.VMEM((2 * crows, TILE // 2), BF16),
                pltpu.VMEM((blocks, crows, HEAD), F32),
                pltpu.VMEM((blocks, 8, HEAD), F32),
                pltpu.VMEM((blocks, 8, HEAD), F32),
                pltpu.VMEM((4, heads, head_dim), F32),
                dma((SLOTS,)), dma((3,)), dma((4,)), dma((8,)), dma((8, 6)),
                dma((blocks,)), dma((blocks,)), dma((blocks,)), dma((blocks,)), dma((blocks,)), dma((blocks,)),
                dma((5,)), dma((5,)), dma((6,)), dma((2,)),
                dma((blocks,)), dma((blocks,)), dma((4,)), dma((2,)),
                dma((blocks,)), dma((blocks,)), dma((2,)), pltpu.SemaphoreType.REGULAR,
                pltpu.VMEM((4, cache_rows, 8, head_dim), BF16), dma((4,)), dma((2,)),
            ],
            compiler_params=pltpu.CompilerParams(
                collective_id=0, has_side_effects=True, vmem_limit_bytes=67043328),
        )(cos_t, sin_t, *bias, x_in, cache_k1, cache_v1, cache_k2, cache_v2,
          w_q1, w_k1, w_v1, w_o1, w_gate, w_up, w_down, w_q2, w_k2, w_v2, w_o2)
        steps = 4
        step_rows = pl.BlockSpec((rows // steps, d_model), lambda i: (i, 0))
        step_heads = pl.BlockSpec((rows // steps, heads, head_dim), lambda i: (i, 0, 0))
        head_out = jax.ShapeDtypeStruct((rows, heads, head_dim), BF16)
        return pl.pallas_call(
            deliver,
            grid=(steps,),
            out_shape=[row_out] * 2 + [head_out] * 4,
            in_specs=[step_rows] * 6,
            out_specs=[step_rows] * 2 + [step_heads] * 4,
        )(*out[:6])

    return jax.shard_map(forward, mesh=mesh, in_specs=in_specs, out_specs=out_specs, check_vma=False)
```
